256 devices in a mesh: slab: 256 (over x, z, y, core).
Axes of the slice: x: 4, y: 4, z: 8, core: 2. Of those that a mesh axis runs over, the one named last changes fastest.
Arguments:
- coords: float32 [3, 524288], P(None, 'slab'), may hold values from -18 to 2048, as said below
- charges: float32 [524288], P('slab'), may hold values from -3.6 to 3.6
- radii: float32 [524288], P('slab'), may hold values from 1.2 to 2
- screens: float32 [524288], P('slab'), may hold values from 0.6 to 0.9
- tile_lists: int32 [4096, 8], P('slab'), may hold values from 0 to 79, as said below
- tile_counts: int32 [4096], P('slab'), may hold values from 1 to 8, as said below
- slab_fill: int32 [256], P('slab'), may hold values from 1921 to 2048
Outputs:
- born_radii: float32 [524288], P('slab')
- energy: float32 [524288], P('slab')
- total: float32 [], replicated
The draws below stay inside these ranges and needn't reach their ends.
Inputs may be any that keep to these rules, and one draw needn't show every extreme that they name: `coords`: x and y lie within 18 of the fibre axis; z of atoms of slab s lies in [8 s, 8 s + 8]. `tile_lists`: entry 0 of tile g's list is its own tile, 32 + g % 16; the entries of a row are distinct; listed tiles lie in slabs that exist (the fibre does not close) and within 32 window tiles of the own tile. `tile_counts`: every slab has a tile whose count is 8.
All inputs are finite; a program needn't handle non-finite values.
Results may differ from the reference program's by a relative error of at most 0.0003.
Values sent between devices are 32-bit elements; how exact they have to be, the bound alone decides.
No kernel may reach another device: no remote copies, remote signals or barrier semaphores. Data moves between devices by JAX's collectives and lax.ppermute only.
A program may use at most 64 MiB of HBM per device.

```python
import math
import jax
import jax.numpy as jnp
from jax import lax

ATOM_DEV = 2048
MAXT = 8
TPD = 16
SLABS = 256
ATOMS = 524288


def draw_coords(key, part):
    key_list = jax.random.split(jax.random.fold_in(key, 11), 3)
    slot_ids = jnp.arange(ATOMS)
    slab_place = (slot_ids // ATOM_DEV).astype(jnp.float32)
    within = (slot_ids % ATOM_DEV).astype(jnp.float32)
    along = jax.random.uniform(key_list[0], (ATOMS,), jnp.float32)
    spread_draw = jax.random.uniform(key_list[1], (ATOMS,), jnp.float32)
    turning = jax.random.uniform(key_list[2], (ATOMS,), jnp.float32, -math.pi, math.pi)
    radial = 18.0 * jnp.sqrt(spread_draw)
    height = 8.0 * (slab_place + (within + along) / ATOM_DEV)
    height = jnp.clip(height, 8.0 * slab_place, 8.0 * slab_place + 8.0)
    return jnp.stack([radial * jnp.cos(turning), radial * jnp.sin(turning), height]).astype(jnp.float32)


def draw_charges(key, part):
    slab_place = (jnp.arange(ATOMS) // ATOM_DEV).astype(jnp.float32) / (SLABS - 1)
    values = jnp.clip(jax.random.normal(jax.random.fold_in(key, 12), (ATOMS,), jnp.float32), -3.0, 3.0)
    factor = 0.4 * (1.0 + 2.0 * slab_place)
    return (values * factor).astype(jnp.float32)


def draw_radii(key, part):
    key_list = jax.random.split(jax.random.fold_in(key, 15), 3)
    upper = jax.random.randint(key_list[0], (ATOMS,), 0, 2, jnp.int32) == 1
    high = jax.random.uniform(key_list[1], (ATOMS,), jnp.float32, 1.85, 2.0)
    broad = jax.random.uniform(key_list[2], (ATOMS,), jnp.float32, 1.2, 2.0)
    return jnp.where(upper, high, broad).astype(jnp.float32)


def draw_screens(key, part):
    key_list = jax.random.split(jax.random.fold_in(key, 16), 3)
    upper = jax.random.randint(key_list[0], (ATOMS,), 0, 2, jnp.int32) == 1
    high = jax.random.uniform(key_list[1], (ATOMS,), jnp.float32, 0.84, 0.9)
    broad = jax.random.uniform(key_list[2], (ATOMS,), jnp.float32, 0.6, 0.9)
    return jnp.where(upper, high, broad).astype(jnp.float32)


def draw_tile_lists(key, part):
    total_tiles = SLABS * TPD
    window_tiles = 5 * TPD
    tile_ids = jnp.arange(total_tiles, dtype=jnp.int32)
    slab_ids = tile_ids // TPD
    own_tiles = 2 * TPD + tile_ids % TPD
    window_ids = jnp.arange(window_tiles, dtype=jnp.int32)
    slab_offset = window_ids // TPD - 2
    target_slab = slab_ids[:, None] + slab_offset[None, :]
    separation = jnp.abs(window_ids[None, :] - own_tiles[:, None])
    usable = (target_slab >= 0) & (target_slab < SLABS) & (separation > 0) & (separation <= 2 * TPD)
    score = jax.random.randint(jax.random.fold_in(key, 13), (total_tiles, window_tiles), 0, 65536, jnp.int32)
    ranked = jnp.where(usable, score * 1024 + window_ids[None, :], -1 - window_ids[None, :])
    chosen = lax.top_k(ranked, MAXT - 1)[1].astype(jnp.int32)
    return jnp.concatenate([own_tiles[:, None], chosen], axis=1).astype(jnp.int32)


def draw_tile_counts(key, part):
    key_list = jax.random.split(jax.random.fold_in(key, 14), 3)
    ceiling = jax.random.randint(key_list[0], (SLABS,), max(1, MAXT // 2), MAXT + 1, jnp.int32)
    per_tile = jnp.repeat(ceiling, TPD)
    floor_tile = jnp.maximum(per_tile // 2, 1)
    counts = jax.random.randint(key_list[1], (SLABS * TPD,), floor_tile, per_tile + 1, jnp.int32)
    heaviest = jax.random.randint(key_list[2], (SLABS,), 0, TPD, jnp.int32)
    position = jnp.arange(SLABS * TPD, dtype=jnp.int32) % TPD
    return jnp.where(position == jnp.repeat(heaviest, TPD), MAXT, counts).astype(jnp.int32)


def plant(drawn, own_key, smallest, high):
    longest = drawn.shape.index(max(drawn.shape))
    spots = []
    for shift in (0, 1):
        where = [jax.random.randint(jax.random.fold_in(own_key, axis), (), 0, length) for axis, length in enumerate(drawn.shape)]
        where[longest] = (where[longest] + shift) % drawn.shape[longest]
        spots.append(tuple(where))
    return drawn.at[spots[0]].set(smallest).at[spots[1]].set(high)


def setup_inputs(seed: int = 0) -> dict:
    seeds = jax.random.split(jax.random.key(seed), 8)
    return {
        "coords": draw_coords(jax.random.fold_in(seeds[7], 71), 0),
        "charges": draw_charges(jax.random.fold_in(seeds[7], 71), 0),
        "radii": draw_radii(jax.random.fold_in(seeds[7], 71), 0),
        "screens": draw_screens(jax.random.fold_in(seeds[7], 71), 0),
        "tile_lists": draw_tile_lists(jax.random.fold_in(seeds[7], 71), 0),
        "tile_counts": draw_tile_counts(jax.random.fold_in(seeds[7], 71), 0),
        "slab_fill": plant(jax.random.randint(seeds[6], (SLABS,), ATOM_DEV - 127, ATOM_DEV + 1), jax.random.fold_in(seeds[6], 1), ATOM_DEV - 127, ATOM_DEV).astype(jnp.int32),
    }


OFFSET = 0.09
SOFTEN = 1.0
group_tiles = 4

def pair_geometry(own_atoms, partner_atoms, list_block, count_block, first_block):
    squared = jnp.zeros((own_atoms.shape[1], 128, partner_atoms.shape[2], 128), jnp.float32)
    for component in range(3):
        offsets = own_atoms[component][:, :, None, None] - partner_atoms[component][:, None, :, :]
        squared = squared + offsets * offsets
    slot_ids = jnp.arange(partner_atoms.shape[2], dtype=jnp.int32)
    used_slot = (slot_ids[None, :] < count_block[:, None])[:, None, :, None]
    partner_mask = used_slot & (partner_atoms[6] > 0.5)[:, None, :, :] & (own_atoms[6] > 0.5)[:, :, None, None]
    lanes = jnp.arange(128, dtype=jnp.int32)
    own_ids = first_block[:, None] * 128 + lanes[None, :]
    partner_ids = list_block[:, :, None] * 128 + lanes[None, None, :]
    distinct = own_ids[:, :, None, None] != partner_ids[:, None, :, :]
    return (squared, partner_mask, distinct)

def born_block(own_atoms, partner_atoms, list_block, count_block, first_block):
    squared, partner_mask, distinct = pair_geometry(own_atoms, partner_atoms, list_block, count_block, first_block)
    own_live = own_atoms[6] > 0.5
    radius_own = jnp.where(own_live, own_atoms[4], 1.5)
    radius_partner = jnp.where(partner_atoms[6] > 0.5, partner_atoms[4], 1.5)[:, None, :, :]
    screen_partner = jnp.where(partner_atoms[6] > 0.5, partner_atoms[5], 0.8)[:, None, :, :]
    offset_radius = (radius_own - OFFSET)[:, :, None, None]
    scaled_radius = screen_partner * (radius_partner - OFFSET)
    distance = jnp.sqrt(squared + SOFTEN)
    upper_end = distance + scaled_radius
    lower_end = jnp.maximum(offset_radius, jnp.abs(distance - scaled_radius))
    pair_term = 0.5 * (1.0 / lower_end - 1.0 / upper_end + 0.25 * (distance - scaled_radius * scaled_radius / distance) * (1.0 / (upper_end * upper_end) - 1.0 / (lower_end * lower_end)) + 0.5 * jnp.log(lower_end / upper_end) / distance)
    pair_term = pair_term + jnp.where(offset_radius < scaled_radius - distance, 2.0 * (1.0 / offset_radius - 1.0 / lower_end), 0.0)
    counted = partner_mask & distinct & (offset_radius < upper_end)
    integral = lax.optimization_barrier(jnp.sum(jnp.where(counted, pair_term, 0.0), axis=(2, 3)))
    inner_radius = radius_own - OFFSET
    psi_value = integral * inner_radius
    bending = jnp.tanh(psi_value - 0.8 * psi_value * psi_value + 4.85 * psi_value * psi_value * psi_value)
    result = 1.0 / (1.0 / inner_radius - bending / radius_own)
    return jnp.where(own_live, result, 0.0)

def energy_block(own_atoms, partner_atoms, radius_own, radius_partner, list_block, count_block, first_block):
    squared, partner_mask, distinct = pair_geometry(own_atoms, partner_atoms, list_block, count_block, first_block)
    own_live = own_atoms[6] > 0.5
    born_own = jnp.where(own_live, radius_own, 1.0)[:, :, None, None]
    born_partner = jnp.where(partner_atoms[6] > 0.5, radius_partner, 1.0)[:, None, :, :]
    product = born_own * born_partner
    screened = jnp.sqrt(squared + product * jnp.exp(-squared / (4.0 * product)))
    pair_term = jnp.where(partner_mask, partner_atoms[3][:, None, :, :] / screened, 0.0)
    result = -0.5 * own_atoms[3] * lax.optimization_barrier(jnp.sum(pair_term, axis=(2, 3)))
    return jnp.where(own_live, result, 0.0)

def tile_setup(window, lists, counts):
    width = window.shape[1]
    tiles = width // 640
    blocks = tiles // group_tiles
    tiled = window.reshape(window.shape[0], width // 128, 128)
    own_atoms = tiled[:, 2 * tiles:3 * tiles].reshape(window.shape[0], blocks, group_tiles, 128).transpose(1, 0, 2, 3)
    list_groups = lists.reshape(blocks, group_tiles, lists.shape[1])
    count_groups = counts.reshape(blocks, group_tiles)
    first_tiles = (2 * tiles + jnp.arange(tiles, dtype=jnp.int32)).reshape(blocks, group_tiles)
    return (tiled, own_atoms, list_groups, count_groups, first_tiles)

def slab_born(window, lists, counts):
    tiled, own_atoms, list_groups, count_groups, first_tiles = tile_setup(window, lists, counts)

    def one_block(inputs):
        own_block, list_block, count_block, first_block = inputs
        partner_atoms = jnp.take(tiled, list_block, axis=1)
        return born_block(own_block, partner_atoms, list_block, count_block, first_block)
    result = lax.map(one_block, (own_atoms, list_groups, count_groups, first_tiles))
    return result.reshape(-1)

def slab_energy(window, radius_window, lists, counts):
    tiled, own_atoms, list_groups, count_groups, first_tiles = tile_setup(window, lists, counts)
    radius_tiled = radius_window.reshape(-1, 128)
    tiles = radius_tiled.shape[0] // 5
    radius_groups = radius_tiled[2 * tiles:3 * tiles].reshape(-1, group_tiles, 128)

    def one_block(inputs):
        own_block, radius_block, list_block, count_block, first_block = inputs
        partner_atoms = jnp.take(tiled, list_block, axis=1)
        partner_radii = jnp.take(radius_tiled, list_block, axis=0)
        return energy_block(own_block, partner_atoms, radius_block, partner_radii, list_block, count_block, first_block)
    result = lax.map(one_block, (own_atoms, radius_groups, list_groups, count_groups, first_tiles))
    return result.reshape(-1)

def reference(coords, charges, radii, screens, tile_lists, tile_counts, slab_fill):
    slot_index = jnp.arange(ATOMS, dtype=jnp.int32)
    live_flag = (slot_index % ATOM_DEV < slab_fill[slot_index // ATOM_DEV]).astype(jnp.float32)
    packed = jnp.concatenate([coords, charges[None], radii[None], screens[None], live_flag[None]], axis=0)
    padded = jnp.pad(packed, ((0, 0), (2 * ATOM_DEV, 2 * ATOM_DEV)))
    lists = tile_lists.reshape(SLABS, TPD, MAXT)
    counts = tile_counts.reshape(SLABS, TPD)
    slab_ids = jnp.arange(SLABS, dtype=jnp.int32)

    def born_of(inputs):
        slab_id, slab_lists, slab_counts = inputs
        start = (slab_id * ATOM_DEV).astype(jnp.int32)
        window = lax.dynamic_slice(padded, (jnp.zeros((), jnp.int32), start), (7, 5 * ATOM_DEV))
        return slab_born(window, slab_lists, slab_counts)
    born_radii = lax.map(born_of, (slab_ids, lists, counts)).reshape(ATOMS)
    radius_padded = jnp.pad(born_radii, (2 * ATOM_DEV, 2 * ATOM_DEV))

    def energy_of(inputs):
        slab_id, slab_lists, slab_counts = inputs
        start = (slab_id * ATOM_DEV).astype(jnp.int32)
        window = lax.dynamic_slice(padded, (jnp.zeros((), jnp.int32), start), (7, 5 * ATOM_DEV))
        radius_window = lax.dynamic_slice(radius_padded, (start,), (5 * ATOM_DEV,))
        return slab_energy(window, radius_window, slab_lists, slab_counts)
    energy = lax.map(energy_of, (slab_ids, lists, counts)).reshape(ATOMS)
    return (born_radii, energy, jnp.sum(energy))
```

```python
import jax
import jax.numpy as jnp
from jax import lax
from jax.experimental import pallas as pl
from jax.experimental.pallas import tpu as pltpu
from jax.sharding import Mesh
from jax.sharding import PartitionSpec as P

SLAB = ("slab_0", "slab_1", "slab_2", "slab_3")
OFFSET = 0.09
LOG2E = 1.4426950408889634
TILES = 16
UNROLL = 4
FAR_GAP = 3.5
ROWS = 88


def swaps(count):
    def chip_swap(odd):
        pairs = []
        for chip in range(count // 2):
            other = ((chip + odd) ^ 1) - odd
            for core in (0, 1):
                if 0 <= other < count // 2:
                    pairs.append((2 * chip + core, 2 * other + core))
                else:
                    pairs.append((2 * chip + core, 2 * chip + 1 - core))
        return pairs

    inner = [(i, i ^ 1) for i in range(count)]
    outer = [(i, (((i + 1) ^ 1) - 1) % count) for i in range(count)]
    return inner, outer, chip_swap(0), chip_swap(1)


def neighbours(value):
    return [lax.ppermute(value, SLAB, pairs) for pairs in swaps(lax.axis_size(SLAB))]


def slots(slab):
    inner = jnp.where(slab % 2 == 0, 3, 1)
    chip = jnp.where((slab // 2) % 2 == 0, 4, 0)
    return inner, 4 - inner, chip, 4 - chip


def rows_of(shape, axis=0):
    return lax.broadcasted_iota(jnp.int32, shape, axis)


def prep_kernel(slab_ref, fill_ref, coords_ref, charges_ref, radii_ref, screens_ref, out_ref):
    fill = fill_ref[0]
    middle = (8 * slab_ref[0] + 4).astype(jnp.float32)
    slot = rows_of((TILES, 128)) * 128 + rows_of((TILES, 128), 1)
    live = slot < fill
    scaled = jnp.where(live, screens_ref[...] * (radii_ref[...] - OFFSET), 0.0)
    charge = jnp.where(live, charges_ref[...], 0.0)
    home = jnp.where(rows_of((3, 128)) == 2, middle, 0.0)
    lane = rows_of((3, 128), 1)
    column = rows_of((1, 128), 1)
    low = jnp.zeros((1, 128), jnp.float32)
    high = jnp.zeros((1, 128), jnp.float32)
    for t in range(TILES):
        xyz = jnp.where(lane + t * 128 < fill, coords_ref[:, t * 128 : (t + 1) * 128], home)
        out_ref[5 * t : 5 * t + 3, :] = xyz
        out_ref[5 * t + 3 : 5 * t + 4, :] = scaled[t : t + 1]
        out_ref[5 * t + 4 : 5 * t + 5, :] = charge[t : t + 1]
        low = jnp.where(column == t, jnp.min(xyz[2:3], axis=1, keepdims=True), low)
        high = jnp.where(column == t, jnp.max(xyz[2:3], axis=1, keepdims=True), high)
    out_ref[80:81, :] = low
    out_ref[81:82, :] = high
    out_ref[82:88, :] = jnp.zeros((6, 128), jnp.float32)


def fill_blocks(blocks_ref, packed_ref, base, centre):
    row = rows_of((8, 128))
    shift = jnp.where(row == 2, centre, 0.0)
    tail = jnp.where(row == 6, 1.0, 0.0)
    for t in range(TILES):
        block = packed_ref[5 * t : 5 * t + 8, :] - shift
        square = block * block
        norm = square[0:1] + square[1:2] + square[2:3]
        blocks_ref[base + t] = jnp.where(row < 5, block, jnp.where(row == 5, norm, tail))


def parts_of(rows):
    first = rows.astype(jnp.bfloat16).astype(jnp.float32)
    rest = rows - first
    second = rest.astype(jnp.bfloat16).astype(jnp.float32)
    third = (rest - second).astype(jnp.bfloat16).astype(jnp.float32)
    return first, second, third


def fill_left(left_ref, blocks_ref):
    row = rows_of((8, 128))
    for g in range(TILES):
        block = blocks_ref[2 * TILES + g]
        norm = block[5:6] + 1.0
        left = jnp.where(
            row < 3,
            -2.0 * block,
            jnp.where(row == 5, 1.0, jnp.where(row == 6, jnp.broadcast_to(norm, (8, 128)), 0.0)),
        )
        a1, a2, a3 = parts_of(left)
        stack = jnp.concatenate([a1, a1, a1, a2, a2, a3], axis=0)
        left_ref[g] = stack.T.astype(jnp.bfloat16)


def column_of(row):
    return jnp.broadcast_to(row, (128, 128)).T


def softened(left_ref, blocks_ref, g, w):
    b1, b2, b3 = parts_of(blocks_ref[w])
    right = jnp.concatenate([b1, b2, b3, b1, b2, b1], axis=0).astype(jnp.bfloat16)
    return jnp.dot(left_ref[g], right, preferred_element_type=jnp.float32)


def run_list(count, entry_of, buffers, produce, consume):
    def fetch(base):
        for u in range(UNROLL):
            w, slot = entry_of(base + u)
            buffers[u][...] = produce(w, jnp.minimum(slot, TILES - 1))

    fetch(0)

    @pl.loop(0, (count + UNROLL - 1) // UNROLL)
    def _(step):
        base = step * UNROLL
        for u in range(UNROLL):
            w, slot = entry_of(base + u)
            consume(w, slot, buffers[u])
        fetch(base + UNROLL)


def pad_list(list_ref, count):
    for u in range(2 * UNROLL):
        list_ref[count + u] = 2 * TILES * 32 + TILES


def entry_in(list_ref):
    def entry_of(index):
        entry = list_ref[index]
        return entry >> 5, entry & 31

    return entry_of


def born_kernel(
    slab_ref, fill_ref, lists_ref, counts_ref, own_ref, p0_ref, p1_ref, p2_ref, p3_ref, radii_ref,
    blocks_ref, left_ref, born_ref, send_ref,
    offsets_ref, acc_ref, buf0, buf1, buf2, buf3, near_ref, far_ref, range_ref, sums_ref, sem,
):
    slab = slab_ref[0]
    places = (2,) + slots(slab)
    packed = (own_ref, p0_ref, p1_ref, p2_ref, p3_ref)
    copies = [
        pltpu.make_async_copy(ref.at[pl.ds(80, 8), :], range_ref.at[place], sem.at[i])
        for i, (ref, place) in enumerate(zip(packed, places))
    ]
    for copy in copies:
        copy.start()
    centre = (8 * slab + 4).astype(jnp.float32)
    for ref, place in zip(packed, places):
        fill_blocks(blocks_ref, ref, place * TILES, centre)
    fill_left(left_ref, blocks_ref)
    offset = radii_ref[...] - OFFSET
    for g in range(TILES):
        offsets_ref[g] = column_of(offset[g : g + 1])
    offsets_ref[TILES] = offsets_ref[0]
    for copy in copies:
        copy.wait()

    near = jnp.int32(0)
    far = jnp.int32(0)
    for g in range(TILES):
        low = range_ref[2, 0, g]
        high = range_ref[2, 1, g]
        for k in range(1, 8):
            w = lists_ref[g, k]
            used = (k < counts_ref[g]).astype(jnp.int32)
            gap = jnp.maximum(
                range_ref[w >> 4, 0, w & 15] - high, low - range_ref[w >> 4, 1, w & 15]
            )
            apart = (gap >= FAR_GAP).astype(jnp.int32) * used
            near_ref[near] = w * 32 + g
            far_ref[far] = w * 32 + g
            far = far + apart
            near = near + used - apart
    pad_list(near_ref, near)
    pad_list(far_ref, far)

    buffers = (buf0, buf1, buf2, buf3)

    def produce(w, g):
        return softened(left_ref, blocks_ref, g, w)

    def near_term(soft, scaled, offset):
        inverse = lax.rsqrt(soft)
        distance = soft * inverse
        upper = distance + scaled
        gap = distance - scaled
        lower = jnp.minimum(jnp.maximum(offset, jnp.abs(gap)), upper)
        ratio = 1.0 / (lower * upper)
        difference = (upper - lower) * ratio
        total = (upper + lower) * ratio
        weight = gap * upper * inverse
        logs = jnp.log(lower * lower * ratio)
        term = difference * (4.0 - weight * total) + (inverse + inverse) * logs
        inside = jnp.where(offset < -gap, 16.0 * (1.0 / offset - 1.0 / lower), 0.0)
        return term + inside

    def consume_near(w, slot, buffer, diagonal=False):
        scaled = blocks_ref[w, 3:4, :]
        for v in range(8):
            rows = slice(16 * v, 16 * v + 16)
            c = jnp.broadcast_to(scaled, (16, 128))
            if diagonal:
                same = rows_of((16, 128)) + 16 * v == rows_of((16, 128), 1)
                c = jnp.where(same, 0.0, c)
            term = near_term(buffer[rows, :], c, offsets_ref[slot, rows, :])
            if diagonal:
                acc_ref[slot, rows, :] = term
            else:
                acc_ref[slot, rows, :] += term

    def consume_far(w, slot, buffer):
        scaled = blocks_ref[w, 3:4, :]
        for v in range(8):
            rows = slice(16 * v, 16 * v + 16)
            soft = buffer[rows, :]
            inverse = lax.rsqrt(soft)
            gap = soft * inverse - scaled
            ratio = 1.0 / (soft - scaled * scaled)
            logs = jnp.log(gap * gap * ratio)
            acc_ref[slot, rows, :] += (4.0 * scaled) * ratio + (inverse + inverse) * logs

    run_list(
        TILES,
        lambda index: (2 * TILES + jnp.minimum(index, TILES - 1), index),
        buffers,
        produce,
        lambda w, slot, buffer: consume_near(w, slot, buffer, True),
    )
    run_list(near, entry_in(near_ref), buffers, produce, consume_near)
    run_list(far, entry_in(far_ref), buffers, produce, consume_far)

    for g in range(TILES):
        sums_ref[g : g + 1, :] = jnp.sum(acc_ref[g].T, axis=0, keepdims=True)
    slot = rows_of((TILES, 128)) * 128 + rows_of((TILES, 128), 1)
    live = slot < fill_ref[0]
    radius = jnp.where(live, radii_ref[...], 1.5)
    inner = radius - OFFSET
    psi = 0.125 * sums_ref[...] * inner
    bending = jnp.tanh(psi - 0.8 * psi * psi + 4.85 * psi * psi * psi)
    born = 1.0 / (1.0 / inner - bending / radius)
    born_ref[...] = jnp.where(live, born, 0.0)
    send_ref[...] = jnp.where(live, born, 1.0)


def energy_kernel(
    slab_ref, lists_ref, counts_ref, blocks_ref, left_ref, own_ref, r0_ref, r1_ref, r2_ref, r3_ref,
    energy_ref, share_ref,
    born_ref, column_ref, inverse_ref, acc_ref, buf0, buf1, buf2, buf3, list_ref, charge_ref,
):
    places = (2,) + slots(slab_ref[0])
    for ref, place in zip((own_ref, r0_ref, r1_ref, r2_ref, r3_ref), places):
        born_ref[pl.ds(place * TILES, TILES), :] = ref[...]
    count = jnp.int32(0)
    for g in range(TILES):
        for k in range(1, 8):
            list_ref[count] = lists_ref[g, k] * 32 + g
            count = count + (k < counts_ref[g]).astype(jnp.int32)
    pad_list(list_ref, count)
    for g in range(TILES):
        column = column_of(own_ref[g : g + 1, :])
        column_ref[g] = column
        inverse_ref[g] = (-0.25 * LOG2E) / column
    column_ref[TILES] = column_ref[0]
    inverse_ref[TILES] = inverse_ref[0]

    buffers = (buf0, buf1, buf2, buf3)

    def produce(w, g):
        return softened(left_ref, blocks_ref, g, w)

    def consume(w, slot, buffer, first=False):
        charge = blocks_ref[w, 4:5, :]
        partner = born_ref[pl.ds(w, 1), :]
        backward = 1.0 / partner
        for v in range(8):
            rows = slice(16 * v, 16 * v + 16)
            squared = buffer[rows, :] - 1.0
            product = column_ref[slot, rows, :] * partner
            decay = jnp.exp2(squared * (inverse_ref[slot, rows, :] * backward))
            term = charge * lax.rsqrt(squared + product * decay)
            if first:
                acc_ref[slot, rows, :] = term
            else:
                acc_ref[slot, rows, :] += term

    run_list(
        TILES,
        lambda index: (2 * TILES + jnp.minimum(index, TILES - 1), index),
        buffers,
        produce,
        lambda w, slot, buffer: consume(w, slot, buffer, True),
    )
    run_list(count, entry_in(list_ref), buffers, produce, consume)
    for g in range(TILES):
        energy_ref[g : g + 1, :] = jnp.sum(acc_ref[g].T, axis=0, keepdims=True)
        charge_ref[g : g + 1, :] = blocks_ref[2 * TILES + g, 4:5, :]
    energy = -0.5 * charge_ref[...] * energy_ref[...]
    energy_ref[...] = energy
    share = jnp.sum(jnp.sum(energy, axis=0, keepdims=True), axis=1, keepdims=True)
    share_ref[...] = jnp.broadcast_to(share[None], share_ref.shape)


def shards(coords, charges, radii, screens, tile_lists, tile_counts, slab_fill):
    f32 = jnp.float32
    count = lax.axis_size(SLAB)
    smem = pl.BlockSpec(memory_space=pltpu.SMEM)
    vmem = pl.BlockSpec(memory_space=pltpu.VMEM)
    slab = lax.axis_index(SLAB).astype(jnp.int32)[None]
    charges, radii, screens = (v.reshape(TILES, 128) for v in (charges, radii, screens))
    packed = pl.pallas_call(
        prep_kernel,
        out_shape=jax.ShapeDtypeStruct((ROWS, 128), f32),
        in_specs=[smem, smem] + [vmem] * 4,
        out_specs=vmem,
        name="prep",
    )(slab, slab_fill, coords, charges, radii, screens)
    around = neighbours(packed)
    square = pltpu.VMEM((128, 128), f32)
    stack = pltpu.VMEM((TILES + 1, 128, 128), f32)
    blocks, left, born, send = pl.pallas_call(
        born_kernel,
        out_shape=(
            jax.ShapeDtypeStruct((5 * TILES, 8, 128), f32),
            jax.ShapeDtypeStruct((TILES, 128, 48), jnp.bfloat16),
            jax.ShapeDtypeStruct((TILES, 128), f32),
            jax.ShapeDtypeStruct((TILES, 128), f32),
        ),
        in_specs=[smem] * 4 + [vmem] * 6,
        out_specs=(vmem,) * 4,
        scratch_shapes=[stack, stack, square, square, square, square]
        + [pltpu.SMEM((144,), jnp.int32)] * 2
        + [pltpu.SMEM((5, 8, 128), f32), pltpu.VMEM((TILES, 128), f32), pltpu.SemaphoreType.DMA((5,))],
        name="born",
    )(slab, slab_fill, tile_lists, tile_counts, packed, *around, radii)
    far_born = neighbours(send)
    energy, share = pl.pallas_call(
        energy_kernel,
        out_shape=(
            jax.ShapeDtypeStruct((TILES, 128), f32),
            jax.ShapeDtypeStruct((count, 1, 128), f32),
        ),
        in_specs=[smem] * 3 + [vmem] * 7,
        out_specs=(vmem,) * 2,
        scratch_shapes=[pltpu.VMEM((5 * TILES, 128), f32), stack, stack, stack, square, square, square, square]
        + [pltpu.SMEM((144,), jnp.int32), pltpu.VMEM((TILES, 128), f32)],
        name="energy",
    )(slab, tile_lists, tile_counts, blocks, left, send, *far_born)
    shares = lax.all_to_all(share, SLAB, 0, 0, tiled=True)
    total = jnp.sum(shares[:, 0, 0])
    return (born.reshape(-1), energy.reshape(-1), total)


def solution(mesh):
    torus = Mesh(mesh.devices.reshape(4, 8, 4, 2), SLAB)
    placed = (P(None, SLAB), P(SLAB), P(SLAB), P(SLAB), P(SLAB, None), P(SLAB), P(SLAB))
    return jax.shard_map(
        shards, mesh=torus, in_specs=placed, out_specs=(P(SLAB), P(SLAB), P()), check_vma=False
    )
```

```python
import jax
import jax.numpy as jnp
from jax import lax
from jax.experimental import pallas as pl
from jax.experimental.pallas import tpu as pltpu
from jax.sharding import Mesh
from jax.sharding import PartitionSpec as P

SLAB = ("slab_0", "slab_1", "slab_2", "slab_3")
OFFSET = 0.09
LOG2E = 1.4426950408889634
TILES = 16
UNROLL = 8
FAR_GAP = 3.5
ROWS = 88


def swaps(count):
    def chip_swap(odd):
        pairs = []
        for chip in range(count // 2):
            other = ((chip + odd) ^ 1) - odd
            for core in (0, 1):
                if 0 <= other < count // 2:
                    pairs.append((2 * chip + core, 2 * other + core))
                else:
                    pairs.append((2 * chip + core, 2 * chip + 1 - core))
        return pairs

    inner = [(i, i ^ 1) for i in range(count)]
    outer = [(i, (((i + 1) ^ 1) - 1) % count) for i in range(count)]
    return inner, outer, chip_swap(0), chip_swap(1)


def neighbours(value):
    return [lax.ppermute(value, SLAB, pairs) for pairs in swaps(lax.axis_size(SLAB))]


def slots(slab):
    inner = jnp.where(slab % 2 == 0, 3, 1)
    chip = jnp.where((slab // 2) % 2 == 0, 4, 0)
    return inner, 4 - inner, chip, 4 - chip


def rows_of(shape, axis=0):
    return lax.broadcasted_iota(jnp.int32, shape, axis)


def prep_kernel(slab_ref, fill_ref, coords_ref, charges_ref, radii_ref, screens_ref, out_ref):
    fill = fill_ref[0]
    middle = (8 * slab_ref[0] + 4).astype(jnp.float32)
    slot = rows_of((TILES, 128)) * 128 + rows_of((TILES, 128), 1)
    live = slot < fill
    scaled = jnp.where(live, screens_ref[...] * (radii_ref[...] - OFFSET), 0.0)
    charge = jnp.where(live, charges_ref[...], 0.0)
    home = jnp.where(rows_of((3, 128)) == 2, middle, 0.0)
    lane = rows_of((3, 128), 1)
    column = rows_of((1, 128), 1) % TILES
    low = jnp.zeros((1, 128), jnp.float32)
    high = jnp.zeros((1, 128), jnp.float32)
    for t in range(TILES):
        xyz = jnp.where(lane + t * 128 < fill, coords_ref[:, t * 128 : (t + 1) * 128], home)
        out_ref[5 * t : 5 * t + 3, :] = xyz
        out_ref[5 * t + 3 : 5 * t + 4, :] = scaled[t : t + 1]
        out_ref[5 * t + 4 : 5 * t + 5, :] = charge[t : t + 1]
        low = jnp.where(column == t, jnp.min(xyz[2:3], axis=1, keepdims=True), low)
        high = jnp.where(column == t, jnp.max(xyz[2:3], axis=1, keepdims=True), high)
    top = jnp.max(jnp.max(scaled, axis=0, keepdims=True), axis=1, keepdims=True)
    out_ref[80:81, :] = low
    out_ref[81:82, :] = high
    out_ref[82:83, :] = jnp.broadcast_to(top, (1, 128))
    out_ref[83:88, :] = jnp.zeros((5, 128), jnp.float32)


def parts_of(rows):
    first = rows.astype(jnp.bfloat16).astype(jnp.float32)
    rest = rows - first
    second = rest.astype(jnp.bfloat16).astype(jnp.float32)
    third = (rest - second).astype(jnp.bfloat16).astype(jnp.float32)
    return first, second, third


def fill_blocks(blocks_ref, right_ref, packed_ref, base, centre):
    row = rows_of((8, 128))
    shift = jnp.where(row == 2, centre, 0.0)
    tail = jnp.where(row == 6, 1.0, 0.0)
    last = jnp.where(rows_of((16, 128)) == 0, 1.0, 0.0)
    for t in range(TILES):
        block = packed_ref[5 * t : 5 * t + 8, :] - shift
        square = block * block
        norm = square[0:1] + square[1:2] + square[2:3]
        block = jnp.where(row < 5, block, jnp.where(row == 5, norm, tail))
        blocks_ref[base + t] = block
        b1, b2, b3 = parts_of(block)
        stack = jnp.concatenate([b1, b2, b3, b1, b2, b1, last], axis=0)
        right_ref[base + t] = stack.astype(jnp.bfloat16)


def fill_left(left_ref, blocks_ref):
    row = rows_of((8, 128))
    last = jnp.where(rows_of((16, 128)) == 0, 1.0, 0.0)
    for g in range(TILES):
        block = blocks_ref[2 * TILES + g]
        norm = jnp.broadcast_to(block[5:6], (8, 128))
        left = jnp.where(
            row < 3, -2.0 * block, jnp.where(row == 5, 1.0, jnp.where(row == 6, norm, 0.0))
        )
        a1, a2, a3 = parts_of(left)
        stack = jnp.concatenate([a1, a1, a1, a2, a2, a3, last], axis=0)
        left_ref[g] = stack.T.astype(jnp.bfloat16)


def column_of(row):
    return jnp.broadcast_to(row, (128, 128)).T


def squares(left_ref, right_ref, g, w, depth):
    return jnp.dot(
        left_ref[g, :, :depth], right_ref[w, :depth, :], preferred_element_type=jnp.float32
    )


def run_list(count, entry_of, buffers, produce, consume):
    unroll = len(buffers)

    def fetch(base):
        for u, buffer in enumerate(buffers):
            w, slot = entry_of(base + u)
            buffer[...] = produce(w, jnp.minimum(slot, TILES - 1))

    fetch(0)

    @pl.loop(0, (count + unroll - 1) // unroll)
    def _(step):
        base = step * unroll
        for u, buffer in enumerate(buffers):
            w, slot = entry_of(base + u)
            consume(w, slot, buffer)
        fetch(base + unroll)


def own_entry(index):
    return 2 * TILES + jnp.minimum(index, TILES - 1), index


def pad_list(list_ref, count):
    for u in range(2 * UNROLL):
        list_ref[count + u] = 2 * TILES * 32 + TILES


def entry_in(list_ref):
    def entry_of(index):
        entry = list_ref[index]
        return (entry >> 5) & 127, entry & 31

    return entry_of


def plan_of(lists_ref, counts_ref, offset, packed, places, index_ref, plan_ref):
    lane = rows_of((1, 128), 1)
    low = jnp.zeros((1, 128), jnp.float32)
    high = jnp.zeros((1, 128), jnp.float32)
    top = packed[0][82:83, :]
    for ref, place in zip(packed, places):
        low = jnp.where(lane >> 4 == place, ref[80:81, :], low)
        high = jnp.where(lane >> 4 == place, ref[81:82, :], high)
        top = jnp.maximum(top, ref[82:83, :])
    index_ref[...] = jnp.zeros((16, 128), jnp.int32)
    index_ref[0:8, 0:TILES] = lists_ref[...]
    index_ref[8:9, 0:TILES] = counts_ref[...]
    tile = index_ref[0:8, :]
    used = (rows_of((8, 128)) > 0) & (rows_of((8, 128)) < index_ref[8:9, :])

    def picked(row):
        return jnp.take_along_axis(
            jnp.broadcast_to(row, (8, 128)), tile, axis=1, mode="promise_in_bounds"
        )

    gap = jnp.maximum(picked(low) - packed[0][81:82, :], packed[0][80:81, :] - picked(high))
    kind = jnp.where(used, jnp.where(gap >= FAR_GAP, 1 << 17, 1 << 16), 0)
    plan_ref[0:8, :] = tile * 32 + (lane & 15) + kind
    least = jnp.min(jnp.min(offset, axis=0, keepdims=True), axis=1, keepdims=True)
    plan_ref[8:16, :] = jnp.broadcast_to(jnp.where(top - 0.99 >= least, 1, 0), (8, 128))


def born_kernel(
    slab_ref, fill_ref, lists_ref, counts_ref, own_ref, p0_ref, p1_ref, p2_ref, p3_ref, radii_ref,
    blocks_ref, left_ref, right_ref, plan_ref, born_ref, send_ref,
    offsets_ref, acc_ref, buf0, buf1, buf2, buf3, buf4, buf5, buf6, buf7,
    near_ref, far_ref, index_ref, steps_ref, sums_ref, sem,
):
    slab = slab_ref[0]
    places = (2,) + slots(slab)
    packed = (own_ref, p0_ref, p1_ref, p2_ref, p3_ref)
    offset = radii_ref[...] - OFFSET
    plan_of(lists_ref, counts_ref, offset, packed, places, index_ref, plan_ref)
    copy = pltpu.make_async_copy(plan_ref, steps_ref, sem)
    copy.start()
    centre = (8 * slab + 4).astype(jnp.float32)
    for ref, place in zip(packed, places):
        fill_blocks(blocks_ref, right_ref, ref, place * TILES, centre)
    copy.wait()
    near = jnp.int32(0)
    far = jnp.int32(0)
    for g in range(TILES):
        for k in range(1, 8):
            entry = steps_ref[k, g]
            near_ref[near] = entry
            far_ref[far] = entry
            near = near + ((entry >> 16) & 1)
            far = far + (entry >> 17)
    pad_list(near_ref, near)
    pad_list(far_ref, far)
    fill_left(left_ref, blocks_ref)
    for g in range(TILES):
        offsets_ref[g] = column_of(offset[g : g + 1])
    offsets_ref[TILES] = offsets_ref[0]

    buffers = (buf0, buf1, buf2, buf3, buf4, buf5, buf6, buf7)

    def produce(w, g):
        return squares(left_ref, right_ref, g, w, 64)

    def near_term(soft, scaled, offset, inside):
        inverse = lax.rsqrt(soft)
        distance = soft * inverse
        upper = distance + scaled
        gap = distance - scaled
        lower = jnp.minimum(jnp.maximum(offset, jnp.abs(gap)), upper)
        ratio = 1.0 / (lower * upper)
        difference = (upper - lower) * ratio
        total = (upper + lower) * ratio
        weight = gap * upper * inverse
        logs = jnp.log(lower * lower * ratio)
        term = difference * (4.0 - weight * total) + (inverse + inverse) * logs
        if inside:
            term += jnp.where(offset < -gap, 16.0 * (1.0 / offset - 1.0 / lower), 0.0)
        return term

    def consume_near(inside, diagonal):
        def consume(w, slot, buffer):
            scaled = blocks_ref[w, 3:4, :]
            for v in range(8):
                rows = slice(16 * v, 16 * v + 16)
                c = jnp.broadcast_to(scaled, (16, 128))
                if diagonal:
                    same = rows_of((16, 128)) + 16 * v == rows_of((16, 128), 1)
                    c = jnp.where(same, 0.0, c)
                term = near_term(buffer[rows, :], c, offsets_ref[slot, rows, :], inside)
                if diagonal:
                    acc_ref[slot, rows, :] = term
                else:
                    acc_ref[slot, rows, :] += term

        return consume

    def consume_far(w, slot, buffer):
        scaled = blocks_ref[w, 3:4, :]
        for v in range(8):
            rows = slice(16 * v, 16 * v + 16)
            soft = buffer[rows, :]
            inverse = lax.rsqrt(soft)
            gap = soft * inverse - scaled
            ratio = 1.0 / (soft - scaled * scaled)
            logs = jnp.log(gap * gap * ratio)
            acc_ref[slot, rows, :] += (4.0 * scaled) * ratio + (inverse + inverse) * logs

    def near_lists(inside):
        run_list(TILES, own_entry, buffers[:4], produce, consume_near(inside, True))
        run_list(near, entry_in(near_ref), buffers[:4], produce, consume_near(inside, False))

    within = steps_ref[8, 0]
    pl.when(within == 0)(lambda: near_lists(False))
    pl.when(within != 0)(lambda: near_lists(True))
    run_list(far, entry_in(far_ref), buffers, produce, consume_far)

    for g in range(TILES):
        sums_ref[g : g + 1, :] = jnp.sum(acc_ref[g].T, axis=0, keepdims=True)
    slot = rows_of((TILES, 128)) * 128 + rows_of((TILES, 128), 1)
    live = slot < fill_ref[0]
    radius = jnp.where(live, radii_ref[...], 1.5)
    inner = radius - OFFSET
    psi = 0.125 * sums_ref[...] * inner
    bending = jnp.tanh(psi - 0.8 * psi * psi + 4.85 * psi * psi * psi)
    born = 1.0 / (1.0 / inner - bending / radius)
    born_ref[...] = jnp.where(live, born, 0.0)
    send_ref[...] = jnp.where(live, born, 1.0)


def energy_kernel(
    slab_ref, plan_ref, blocks_ref, left_ref, right_ref, own_ref, r0_ref, r1_ref, r2_ref, r3_ref,
    energy_ref, share_ref,
    born_ref, column_ref, inverse_ref, acc_ref, buf0, buf1, buf2, buf3, buf4, buf5, buf6, buf7,
    list_ref, steps_ref, charge_ref, sem,
):
    copy = pltpu.make_async_copy(plan_ref, steps_ref, sem)
    copy.start()
    places = (2,) + slots(slab_ref[0])
    for ref, place in zip((own_ref, r0_ref, r1_ref, r2_ref, r3_ref), places):
        born_ref[pl.ds(place * TILES, TILES), :] = ref[...]
    copy.wait()
    count = jnp.int32(0)
    for g in range(TILES):
        for k in range(1, 8):
            entry = steps_ref[k, g]
            list_ref[count] = entry
            count = count + jnp.minimum(entry >> 16, 1)
    pad_list(list_ref, count)
    for g in range(TILES):
        column = column_of(own_ref[g : g + 1, :])
        column_ref[g] = column
        inverse_ref[g] = (-0.25 * LOG2E) / column
    column_ref[TILES] = column_ref[0]
    inverse_ref[TILES] = inverse_ref[0]

    buffers = (buf0, buf1, buf2, buf3, buf4, buf5, buf6, buf7)

    def produce(w, g):
        return squares(left_ref, right_ref, g, w, 48)

    def consume(first):
        def body(w, slot, buffer):
            charge = blocks_ref[w, 4:5, :]
            partner = born_ref[pl.ds(w, 1), :]
            backward = 1.0 / partner
            for v in range(8):
                rows = slice(16 * v, 16 * v + 16)
                squared = buffer[rows, :]
                product = column_ref[slot, rows, :] * partner
                decay = jnp.exp2(squared * (inverse_ref[slot, rows, :] * backward))
                term = charge * lax.rsqrt(squared + product * decay)
                if first:
                    acc_ref[slot, rows, :] = term
                else:
                    acc_ref[slot, rows, :] += term

        return body

    run_list(TILES, own_entry, buffers, produce, consume(True))
    run_list(count, entry_in(list_ref), buffers, produce, consume(False))
    for g in range(TILES):
        energy_ref[g : g + 1, :] = jnp.sum(acc_ref[g].T, axis=0, keepdims=True)
        charge_ref[g : g + 1, :] = blocks_ref[2 * TILES + g, 4:5, :]
    energy = -0.5 * charge_ref[...] * energy_ref[...]
    energy_ref[...] = energy
    share = jnp.sum(jnp.sum(energy, axis=0, keepdims=True), axis=1, keepdims=True)
    share_ref[...] = jnp.broadcast_to(share[None], share_ref.shape)


def total_kernel(shares_ref, total_ref):
    total = shares_ref[0]
    for i in range(1, shares_ref.shape[0]):
        total = total + shares_ref[i]
    total_ref[0] = total[0, 0]


def shards(coords, charges, radii, screens, tile_lists, tile_counts, slab_fill):
    f32 = jnp.float32
    count = lax.axis_size(SLAB)
    smem = pl.BlockSpec(memory_space=pltpu.SMEM)
    vmem = pl.BlockSpec(memory_space=pltpu.VMEM)

    def near(value):
        return pltpu.with_memory_space_constraint(value, pltpu.VMEM)

    slab = lax.axis_index(SLAB).astype(jnp.int32)[None]
    charges, radii, screens = (v.reshape(TILES, 128) for v in (charges, radii, screens))
    packed = pl.pallas_call(
        prep_kernel,
        out_shape=pltpu.VMEM((ROWS, 128), f32),
        in_specs=[smem, smem] + [vmem] * 4,
        out_specs=vmem,
        name="prep",
    )(slab, slab_fill, coords, charges, radii, screens)
    around = neighbours(packed)
    squares = [pltpu.VMEM((128, 128), f32)] * 8
    stack = pltpu.VMEM((TILES + 1, 128, 128), f32)
    steps = pltpu.SMEM((16, 128), jnp.int32)
    blocks, left, right, plan, born, send = pl.pallas_call(
        born_kernel,
        out_shape=(
            pltpu.VMEM((5 * TILES, 8, 128), f32),
            pltpu.VMEM((TILES, 128, 64), jnp.bfloat16),
            pltpu.VMEM((5 * TILES, 64, 128), jnp.bfloat16),
            pltpu.VMEM((16, 128), jnp.int32),
            jax.ShapeDtypeStruct((TILES, 128), f32),
            pltpu.VMEM((TILES, 128), f32),
        ),
        in_specs=[smem] * 2 + [vmem] * 8,
        out_specs=(vmem,) * 6,
        scratch_shapes=[stack, stack]
        + squares
        + [pltpu.SMEM((144,), jnp.int32)] * 2
        + [pltpu.VMEM((16, 128), jnp.int32), steps, pltpu.VMEM((TILES, 128), f32), pltpu.SemaphoreType.DMA],
        name="born",
    )(
        slab, slab_fill, tile_lists.T, tile_counts.reshape(1, TILES),
        near(packed), *(near(value) for value in around), radii,
    )
    far_born = neighbours(send)
    energy, share = pl.pallas_call(
        energy_kernel,
        out_shape=(jax.ShapeDtypeStruct((TILES, 128), f32), pltpu.VMEM((count, 1, 128), f32)),
        in_specs=[smem] + [vmem] * 9,
        out_specs=(vmem,) * 2,
        scratch_shapes=[pltpu.VMEM((5 * TILES, 128), f32), stack, stack, stack]
        + squares
        + [pltpu.SMEM((144,), jnp.int32), steps, pltpu.VMEM((TILES, 128), f32), pltpu.SemaphoreType.DMA],
        name="energy",
    )(slab, *(near(value) for value in (plan, blocks, left, right, send, *far_born)))
    shares = lax.all_to_all(share, SLAB, 0, 0, tiled=True)
    total = pl.pallas_call(
        total_kernel,
        out_shape=jax.ShapeDtypeStruct((1,), f32),
        in_specs=[vmem],
        out_specs=smem,
        name="total",
    )(near(shares))
    return (born.reshape(-1), energy.reshape(-1), total[0])


def solution(mesh):
    torus = Mesh(mesh.devices.reshape(4, 8, 4, 2), SLAB)
    placed = (P(None, SLAB), P(SLAB), P(SLAB), P(SLAB), P(SLAB, None), P(SLAB), P(SLAB))
    return jax.shard_map(
        shards, mesh=torus, in_specs=placed, out_specs=(P(SLAB), P(SLAB), P()), check_vma=False
    )
```

```python
import jax
import jax.numpy as jnp
from jax import lax
from jax.experimental import pallas as pl
from jax.experimental.pallas import tpu as pltpu
from jax.sharding import Mesh
from jax.sharding import PartitionSpec as P

SLAB = ("slab_0", "slab_1", "slab_2", "slab_3")
OFFSET = 0.09
LOG2E = 1.4426950408889634
TILES = 16
UNROLL = 8
FAR_GAP = 3.5
ROWS = 88


def chip_swap(count, odd):
    pairs = []
    for chip in range(count // 2):
        other = ((chip + odd) ^ 1) - odd
        for core in (0, 1):
            if 0 <= other < count // 2:
                pairs.append((2 * chip + core, 2 * other + core))
            else:
                pairs.append((2 * chip + core, 2 * chip + 1 - core))
    return pairs


def neighbours(value):
    count = lax.axis_size(SLAB)
    other = lax.ppermute(value, SLAB, [(i, i ^ 1) for i in range(count)])
    both = jnp.concatenate([value, other], axis=0)
    return [other] + [lax.ppermute(both, SLAB, chip_swap(count, odd)) for odd in (0, 1)]


class Window:
    def __init__(self, slab, own, other, even, odd):
        core = slab % 2
        ahead = (slab // 2) % 2 == 0
        height = own.shape[0]
        near = jnp.where(core == 0, 3, 1)
        far = jnp.where(ahead, 4, 0)
        from_even = ahead == (core == 1)

        def crossed(start, size):
            rows = pl.ds(height + start, size)
            return jnp.where(from_even, even[rows, :], odd[rows, :])

        def reader(ref):
            return lambda start, size: ref[pl.ds(start, size), :]

        self.slabs = (
            (2, reader(own)),
            (near, reader(other)),
            (4 - near, crossed),
            (far, reader(even)),
            (4 - far, reader(odd)),
        )


def rows_of(shape, axis=0):
    return lax.broadcasted_iota(jnp.int32, shape, axis)


def prep_kernel(slab_ref, fill_ref, coords_ref, charges_ref, radii_ref, screens_ref, out_ref):
    fill = fill_ref[0]
    middle = (8 * slab_ref[0] + 4).astype(jnp.float32)
    slot = rows_of((TILES, 128)) * 128 + rows_of((TILES, 128), 1)
    live = slot < fill
    scaled = jnp.where(live, screens_ref[...] * (radii_ref[...] - OFFSET), 0.0)
    charge = jnp.where(live, charges_ref[...], 0.0)
    home = jnp.where(rows_of((3, 128)) == 2, middle, 0.0)
    lane = rows_of((3, 128), 1)
    column = rows_of((1, 128), 1) % TILES
    low = jnp.zeros((1, 128), jnp.float32)
    high = jnp.zeros((1, 128), jnp.float32)
    for t in range(TILES):
        xyz = jnp.where(lane + t * 128 < fill, coords_ref[:, t * 128 : (t + 1) * 128], home)
        out_ref[5 * t : 5 * t + 3, :] = xyz
        out_ref[5 * t + 3 : 5 * t + 4, :] = scaled[t : t + 1]
        out_ref[5 * t + 4 : 5 * t + 5, :] = charge[t : t + 1]
        low = jnp.where(column == t, jnp.min(xyz[2:3], axis=1, keepdims=True), low)
        high = jnp.where(column == t, jnp.max(xyz[2:3], axis=1, keepdims=True), high)
    top = jnp.max(jnp.max(scaled, axis=0, keepdims=True), axis=1, keepdims=True)
    out_ref[80:81, :] = low
    out_ref[81:82, :] = high
    out_ref[82:83, :] = jnp.broadcast_to(top, (1, 128))
    out_ref[83:88, :] = jnp.zeros((5, 128), jnp.float32)


def parts_of(rows):
    first = rows.astype(jnp.bfloat16).astype(jnp.float32)
    rest = rows - first
    second = rest.astype(jnp.bfloat16).astype(jnp.float32)
    third = (rest - second).astype(jnp.bfloat16).astype(jnp.float32)
    return first, second, third


def fill_blocks(blocks_ref, read, base, centre):
    row = rows_of((8, 128))
    shift = jnp.where(row == 2, centre, 0.0)
    tail = jnp.where(row == 6, 1.0, 0.0)
    for t in range(TILES):
        block = read(5 * t, 8) - shift
        square = block * block
        norm = square[0:1] + square[1:2] + square[2:3]
        blocks_ref[base + t] = jnp.where(row < 5, block, jnp.where(row == 5, norm, tail))


def fill_right(right_ref, blocks_ref):
    last = jnp.where(rows_of((16, 128)) == 0, 1.0, 0.0)
    for w in range(5 * TILES):
        b1, b2, b3 = parts_of(blocks_ref[w])
        stack = jnp.concatenate([b1, b2, b3, b1, b2, b1, last], axis=0)
        right_ref[w] = stack.astype(jnp.bfloat16)


def fill_left(left_ref, blocks_ref):
    row = rows_of((8, 128))
    last = jnp.where(rows_of((16, 128)) == 0, 1.0, 0.0)
    for g in range(TILES):
        block = blocks_ref[2 * TILES + g]
        norm = jnp.broadcast_to(block[5:6], (8, 128))
        left = jnp.where(
            row < 3, -2.0 * block, jnp.where(row == 5, 1.0, jnp.where(row == 6, norm, 0.0))
        )
        a1, a2, a3 = parts_of(left)
        stack = jnp.concatenate([a1, a1, a1, a2, a2, a3, last], axis=0)
        left_ref[g] = stack.T.astype(jnp.bfloat16)


def column_of(row):
    return jnp.broadcast_to(row, (128, 128)).T


def squares(left_ref, right_ref, g, w, depth):
    return jnp.dot(
        left_ref[g, :, :depth], right_ref[w, :depth, :], preferred_element_type=jnp.float32
    )


def run_list(count, entry_of, buffers, produce, consume):
    unroll = len(buffers)

    def fetch(base):
        for u, buffer in enumerate(buffers):
            w, slot = entry_of(base + u)
            buffer[...] = produce(w, jnp.minimum(slot, TILES - 1))

    fetch(0)

    @pl.loop(0, (count + unroll - 1) // unroll)
    def _(step):
        base = step * unroll
        for u, buffer in enumerate(buffers):
            w, slot = entry_of(base + u)
            consume(w, slot, buffer)
        fetch(base + unroll)


def own_entry(index):
    return 2 * TILES + jnp.minimum(index, TILES - 1), index


def pad_list(list_ref, count):
    for u in range(2 * UNROLL):
        list_ref[count + u] = 2 * TILES * 32 + TILES


def entry_in(list_ref):
    def entry_of(index):
        entry = list_ref[index]
        return (entry >> 5) & 127, entry & 31

    return entry_of


def plan_of(lists_ref, counts_ref, offset, window, index_ref, plan_ref):
    lane = rows_of((1, 128), 1)
    low = jnp.zeros((1, 128), jnp.float32)
    high = jnp.zeros((1, 128), jnp.float32)
    top = jnp.zeros((1, 128), jnp.float32)
    for place, read in window.slabs:
        ranges = read(80, 8)
        low = jnp.where(lane >> 4 == place, ranges[0:1], low)
        high = jnp.where(lane >> 4 == place, ranges[1:2], high)
        top = jnp.maximum(top, ranges[2:3])
    own = window.slabs[0][1](80, 8)
    index_ref[...] = jnp.zeros((16, 128), jnp.int32)
    index_ref[0:8, 0:TILES] = lists_ref[...]
    index_ref[8:9, 0:TILES] = counts_ref[...]
    tile = index_ref[0:8, :]
    used = (rows_of((8, 128)) > 0) & (rows_of((8, 128)) < index_ref[8:9, :])

    def picked(row):
        return jnp.take_along_axis(
            jnp.broadcast_to(row, (8, 128)), tile, axis=1, mode="promise_in_bounds"
        )

    gap = jnp.maximum(picked(low) - own[1:2], own[0:1] - picked(high))
    kind = jnp.where(used, jnp.where(gap >= FAR_GAP, 1 << 17, 1 << 16), 0)
    plan_ref[0:8, :] = tile * 32 + (lane & 15) + kind
    least = jnp.min(jnp.min(offset, axis=0, keepdims=True), axis=1, keepdims=True)
    plan_ref[8:16, :] = jnp.broadcast_to(jnp.where(top - 0.99 >= least, 1, 0), (8, 128))


def born_kernel(
    slab_ref, fill_ref, lists_ref, counts_ref, own_ref, other_ref, even_ref, odd_ref, radii_ref,
    blocks_ref, left_ref, plan_ref, born_ref, send_ref,
    right_ref, offsets_ref, acc_ref, buf0, buf1, buf2, buf3, buf4, buf5, buf6, buf7,
    near_ref, far_ref, index_ref, steps_ref, sums_ref, sem,
):
    slab = slab_ref[0]
    window = Window(slab, own_ref, other_ref, even_ref, odd_ref)
    offset = radii_ref[...] - OFFSET
    plan_of(lists_ref, counts_ref, offset, window, index_ref, plan_ref)
    copy = pltpu.make_async_copy(plan_ref, steps_ref, sem)
    copy.start()
    centre = (8 * slab + 4).astype(jnp.float32)
    for place, read in window.slabs:
        fill_blocks(blocks_ref, read, place * TILES, centre)
    fill_right(right_ref, blocks_ref)
    copy.wait()
    near = jnp.int32(0)
    far = jnp.int32(0)
    for g in range(TILES):
        for k in range(1, 8):
            entry = steps_ref[k, g]
            near_ref[near] = entry
            far_ref[far] = entry
            near = near + ((entry >> 16) & 1)
            far = far + (entry >> 17)
    pad_list(near_ref, near)
    pad_list(far_ref, far)
    fill_left(left_ref, blocks_ref)
    for g in range(TILES):
        offsets_ref[g] = column_of(offset[g : g + 1])
    offsets_ref[TILES] = offsets_ref[0]

    buffers = (buf0, buf1, buf2, buf3, buf4, buf5, buf6, buf7)

    def produce(w, g):
        return squares(left_ref, right_ref, g, w, 64)

    def near_term(soft, scaled, offset, inside):
        inverse = lax.rsqrt(soft)
        distance = soft * inverse
        upper = distance + scaled
        gap = distance - scaled
        lower = jnp.minimum(jnp.maximum(offset, jnp.abs(gap)), upper)
        ratio = 1.0 / (lower * upper)
        difference = (upper - lower) * ratio
        total = (upper + lower) * ratio
        weight = gap * upper * inverse
        logs = jnp.log(lower * lower * ratio)
        term = difference * (4.0 - weight * total) + (inverse + inverse) * logs
        if inside:
            term += jnp.where(offset < -gap, 16.0 * (1.0 / offset - 1.0 / lower), 0.0)
        return term

    def consume_near(inside, diagonal):
        def consume(w, slot, buffer):
            scaled = blocks_ref[w, 3:4, :]
            for v in range(8):
                rows = slice(16 * v, 16 * v + 16)
                c = jnp.broadcast_to(scaled, (16, 128))
                if diagonal:
                    same = rows_of((16, 128)) + 16 * v == rows_of((16, 128), 1)
                    c = jnp.where(same, 0.0, c)
                term = near_term(buffer[rows, :], c, offsets_ref[slot, rows, :], inside)
                if diagonal:
                    acc_ref[slot, rows, :] = term
                else:
                    acc_ref[slot, rows, :] += term

        return consume

    def consume_far(w, slot, buffer):
        scaled = blocks_ref[w, 3:4, :]
        for v in range(8):
            rows = slice(16 * v, 16 * v + 16)
            soft = buffer[rows, :]
            inverse = lax.rsqrt(soft)
            gap = soft * inverse - scaled
            ratio = 1.0 / (soft - scaled * scaled)
            logs = jnp.log(gap * gap * ratio)
            acc_ref[slot, rows, :] += (4.0 * scaled) * ratio + (inverse + inverse) * logs

    def near_lists(inside):
        run_list(TILES, own_entry, buffers[:4], produce, consume_near(inside, True))
        run_list(near, entry_in(near_ref), buffers[:4], produce, consume_near(inside, False))

    within = steps_ref[8, 0]
    pl.when(within == 0)(lambda: near_lists(False))
    pl.when(within != 0)(lambda: near_lists(True))
    run_list(far, entry_in(far_ref), buffers, produce, consume_far)

    for g in range(TILES):
        sums_ref[g : g + 1, :] = jnp.sum(acc_ref[g].T, axis=0, keepdims=True)
    slot = rows_of((TILES, 128)) * 128 + rows_of((TILES, 128), 1)
    live = slot < fill_ref[0]
    radius = jnp.where(live, radii_ref[...], 1.5)
    inner = radius - OFFSET
    psi = 0.125 * sums_ref[...] * inner
    bending = jnp.tanh(psi - 0.8 * psi * psi + 4.85 * psi * psi * psi)
    born = 1.0 / (1.0 / inner - bending / radius)
    born_ref[...] = jnp.where(live, born, 0.0)
    send_ref[...] = jnp.where(live, born, 1.0)


def energy_kernel(
    slab_ref, plan_ref, blocks_ref, left_ref, own_ref, other_ref, even_ref, odd_ref,
    energy_ref, share_ref,
    right_ref, born_ref, column_ref, inverse_ref, acc_ref, buf0, buf1, buf2, buf3, buf4, buf5, buf6, buf7,
    list_ref, steps_ref, charge_ref, sem,
):
    copy = pltpu.make_async_copy(plan_ref, steps_ref, sem)
    copy.start()
    window = Window(slab_ref[0], own_ref, other_ref, even_ref, odd_ref)
    for place, read in window.slabs:
        born_ref[pl.ds(place * TILES, TILES), :] = read(0, TILES)
    fill_right(right_ref, blocks_ref)
    copy.wait()
    count = jnp.int32(0)
    for g in range(TILES):
        for k in range(1, 8):
            entry = steps_ref[k, g]
            list_ref[count] = entry
            count = count + jnp.minimum(entry >> 16, 1)
    pad_list(list_ref, count)
    for g in range(TILES):
        column = column_of(own_ref[g : g + 1, :])
        column_ref[g] = column
        inverse_ref[g] = (-0.25 * LOG2E) / column
    column_ref[TILES] = column_ref[0]
    inverse_ref[TILES] = inverse_ref[0]

    buffers = (buf0, buf1, buf2, buf3, buf4, buf5, buf6, buf7)

    def produce(w, g):
        return squares(left_ref, right_ref, g, w, 48)

    def consume(first):
        def body(w, slot, buffer):
            charge = blocks_ref[w, 4:5, :]
            partner = born_ref[pl.ds(w, 1), :]
            backward = 1.0 / partner
            for v in range(8):
                rows = slice(16 * v, 16 * v + 16)
                squared = buffer[rows, :]
                product = column_ref[slot, rows, :] * partner
                decay = jnp.exp2(squared * (inverse_ref[slot, rows, :] * backward))
                term = charge * lax.rsqrt(squared + product * decay)
                if first:
                    acc_ref[slot, rows, :] = term
                else:
                    acc_ref[slot, rows, :] += term

        return body

    run_list(TILES, own_entry, buffers, produce, consume(True))
    run_list(count, entry_in(list_ref), buffers, produce, consume(False))
    for g in range(TILES):
        energy_ref[g : g + 1, :] = jnp.sum(acc_ref[g].T, axis=0, keepdims=True)
        charge_ref[g : g + 1, :] = blocks_ref[2 * TILES + g, 4:5, :]
    energy = -0.5 * charge_ref[...] * energy_ref[...]
    energy_ref[...] = energy
    share = jnp.sum(jnp.sum(energy, axis=0, keepdims=True), axis=1, keepdims=True)
    share_ref[...] = jnp.broadcast_to(share[None], share_ref.shape)


def total_kernel(shares_ref, total_ref):
    total = shares_ref[0]
    for i in range(1, shares_ref.shape[0]):
        total = total + shares_ref[i]
    total_ref[0] = total[0, 0]


def shards(coords, charges, radii, screens, tile_lists, tile_counts, slab_fill):
    f32 = jnp.float32
    count = lax.axis_size(SLAB)
    smem = pl.BlockSpec(memory_space=pltpu.SMEM)
    vmem = pl.BlockSpec(memory_space=pltpu.VMEM)

    def near(value):
        return pltpu.with_memory_space_constraint(value, pltpu.VMEM)

    slab = lax.axis_index(SLAB).astype(jnp.int32)[None]
    charges, radii, screens = (v.reshape(TILES, 128) for v in (charges, radii, screens))
    packed = pl.pallas_call(
        prep_kernel,
        out_shape=pltpu.VMEM((ROWS, 128), f32),
        in_specs=[smem, smem] + [vmem] * 4,
        out_specs=vmem,
        name="prep",
    )(slab, slab_fill, coords, charges, radii, screens)
    around = neighbours(packed)
    squares = [pltpu.VMEM((128, 128), f32)] * 8
    stack = pltpu.VMEM((TILES + 1, 128, 128), f32)
    right = pltpu.VMEM((5 * TILES, 64, 128), jnp.bfloat16)
    steps = pltpu.SMEM((16, 128), jnp.int32)
    blocks, left, plan, born, send = pl.pallas_call(
        born_kernel,
        out_shape=(
            pltpu.VMEM((5 * TILES, 8, 128), f32),
            pltpu.VMEM((TILES, 128, 64), jnp.bfloat16),
            pltpu.VMEM((16, 128), jnp.int32),
            jax.ShapeDtypeStruct((TILES, 128), f32),
            pltpu.VMEM((TILES, 128), f32),
        ),
        in_specs=[smem] * 2 + [vmem] * 7,
        out_specs=(vmem,) * 5,
        scratch_shapes=[right, stack, stack]
        + squares
        + [pltpu.SMEM((144,), jnp.int32)] * 2
        + [pltpu.VMEM((16, 128), jnp.int32), steps, pltpu.VMEM((TILES, 128), f32), pltpu.SemaphoreType.DMA],
        name="born",
    )(
        slab, slab_fill, tile_lists.T, tile_counts.reshape(1, TILES),
        near(packed), *(near(value) for value in around), radii,
    )
    far_born = neighbours(send)
    energy, share = pl.pallas_call(
        energy_kernel,
        out_shape=(jax.ShapeDtypeStruct((TILES, 128), f32), pltpu.VMEM((count, 1, 128), f32)),
        in_specs=[smem] + [vmem] * 7,
        out_specs=(vmem,) * 2,
        scratch_shapes=[right, pltpu.VMEM((5 * TILES, 128), f32), stack, stack, stack]
        + squares
        + [pltpu.SMEM((144,), jnp.int32), steps, pltpu.VMEM((TILES, 128), f32), pltpu.SemaphoreType.DMA],
        name="energy",
    )(slab, *(near(value) for value in (plan, blocks, left, send, *far_born)))
    shares = lax.all_to_all(share, SLAB, 0, 0, tiled=True)
    total = pl.pallas_call(
        total_kernel,
        out_shape=jax.ShapeDtypeStruct((1,), f32),
        in_specs=[vmem],
        out_specs=smem,
        name="total",
    )(near(shares))
    return (born.reshape(-1), energy.reshape(-1), total[0])


def solution(mesh):
    torus = Mesh(mesh.devices.reshape(4, 8, 4, 2), SLAB)
    placed = (P(None, SLAB), P(SLAB), P(SLAB), P(SLAB), P(SLAB, None), P(SLAB), P(SLAB))
    return jax.shard_map(
        shards, mesh=torus, in_specs=placed, out_specs=(P(SLAB), P(SLAB), P()), check_vma=False
    )
```

```python
import jax
import jax.numpy as jnp
from jax import lax
from jax.experimental import pallas as pl
from jax.experimental.pallas import tpu as pltpu
from jax.sharding import Mesh
from jax.sharding import PartitionSpec as P

SLAB = ("slab_0", "slab_1", "slab_2", "slab_3")
OFFSET = 0.09
LOG2E = 1.4426950408889634
TILES = 16
UNROLL = 8
FAR_GAP = 3.5
ROWS = 88


def swaps(count):
    def chip_swap(odd):
        pairs = []
        for chip in range(count // 2):
            other = ((chip + odd) ^ 1) - odd
            for core in (0, 1):
                if 0 <= other < count // 2:
                    pairs.append((2 * chip + core, 2 * other + core))
                else:
                    pairs.append((2 * chip + core, 2 * chip + 1 - core))
        return pairs

    inner = [(i, i ^ 1) for i in range(count)]
    outer = [(i, (((i + 1) ^ 1) - 1) % count) for i in range(count)]
    return inner, outer, chip_swap(0), chip_swap(1)


def neighbours(value):
    return [lax.ppermute(value, SLAB, pairs) for pairs in swaps(lax.axis_size(SLAB))]


def slots(slab):
    inner = jnp.where(slab % 2 == 0, 3, 1)
    chip = jnp.where((slab // 2) % 2 == 0, 4, 0)
    return inner, 4 - inner, chip, 4 - chip


def rows_of(shape, axis=0):
    return lax.broadcasted_iota(jnp.int32, shape, axis)


def prep_kernel(slab_ref, fill_ref, coords_ref, charges_ref, radii_ref, screens_ref, out_ref):
    fill = fill_ref[0]
    middle = (8 * slab_ref[0] + 4).astype(jnp.float32)
    slot = rows_of((TILES, 128)) * 128 + rows_of((TILES, 128), 1)
    live = slot < fill
    scaled = jnp.where(live, screens_ref[...] * (radii_ref[...] - OFFSET), 0.0)
    charge = jnp.where(live, charges_ref[...], 0.0)
    home = jnp.where(rows_of((3, 128)) == 2, middle, 0.0)
    lane = rows_of((3, 128), 1)
    column = rows_of((1, 128), 1) % TILES
    low = jnp.zeros((1, 128), jnp.float32)
    high = jnp.zeros((1, 128), jnp.float32)
    for t in range(TILES):
        xyz = jnp.where(lane + t * 128 < fill, coords_ref[:, t * 128 : (t + 1) * 128], home)
        out_ref[5 * t : 5 * t + 3, :] = xyz
        out_ref[5 * t + 3 : 5 * t + 4, :] = scaled[t : t + 1]
        out_ref[5 * t + 4 : 5 * t + 5, :] = charge[t : t + 1]
        low = jnp.where(column == t, jnp.min(xyz[2:3], axis=1, keepdims=True), low)
        high = jnp.where(column == t, jnp.max(xyz[2:3], axis=1, keepdims=True), high)
    top = jnp.max(jnp.max(scaled, axis=0, keepdims=True), axis=1, keepdims=True)
    out_ref[80:81, :] = low
    out_ref[81:82, :] = high
    out_ref[82:83, :] = jnp.broadcast_to(top, (1, 128))
    out_ref[83:88, :] = jnp.zeros((5, 128), jnp.float32)


def parts_of(rows):
    first = rows.astype(jnp.bfloat16).astype(jnp.float32)
    rest = rows - first
    second = rest.astype(jnp.bfloat16).astype(jnp.float32)
    third = (rest - second).astype(jnp.bfloat16).astype(jnp.float32)
    return first, second, third


def fill_blocks(blocks_ref, packed_ref, base, centre):
    row = rows_of((8, 128))
    shift = jnp.where(row == 2, centre, 0.0)
    tail = jnp.where(row == 6, 1.0, 0.0)
    for t in range(TILES):
        block = packed_ref[5 * t : 5 * t + 8, :] - shift
        square = block * block
        norm = square[0:1] + square[1:2] + square[2:3]
        blocks_ref[base + t] = jnp.where(row < 5, block, jnp.where(row == 5, norm, tail))


def fill_right(right_ref, blocks_ref, base):
    last = jnp.where(rows_of((16, 128)) == 0, 1.0, 0.0)
    for t in range(TILES):
        b1, b2, b3 = parts_of(blocks_ref[base + t])
        stack = jnp.concatenate([b1, b2, b3, b1, b2, b1, last], axis=0)
        right_ref[base + t] = stack.astype(jnp.bfloat16)


def fill_left(left_ref, blocks_ref):
    row = rows_of((8, 128))
    last = jnp.where(rows_of((16, 128)) == 0, 1.0, 0.0)
    for g in range(TILES):
        block = blocks_ref[2 * TILES + g]
        norm = jnp.broadcast_to(block[5:6], (8, 128))
        left = jnp.where(
            row < 3, -2.0 * block, jnp.where(row == 5, 1.0, jnp.where(row == 6, norm, 0.0))
        )
        a1, a2, a3 = parts_of(left)
        stack = jnp.concatenate([a1, a1, a1, a2, a2, a3, last], axis=0)
        left_ref[g] = stack.T.astype(jnp.bfloat16)


def column_of(row):
    return jnp.broadcast_to(row, (128, 128)).T


def squares(left_ref, right_ref, g, w, depth):
    return jnp.dot(
        left_ref[g, :, :depth], right_ref[w, :depth, :], preferred_element_type=jnp.float32
    )


def run_list(count, entry_of, buffers, produce, consume):
    unroll = len(buffers)

    def fetch(base):
        for u, buffer in enumerate(buffers):
            w, slot = entry_of(base + u)
            buffer[...] = produce(w, jnp.minimum(slot, TILES - 1))

    fetch(0)

    @pl.loop(0, (count + unroll - 1) // unroll)
    def _(step):
        base = step * unroll
        for u, buffer in enumerate(buffers):
            w, slot = entry_of(base + u)
            consume(w, slot, buffer)
        fetch(base + unroll)


def own_entry(index):
    return 2 * TILES + jnp.minimum(index, TILES - 1), index


def pad_list(list_ref, count):
    for u in range(2 * UNROLL):
        list_ref[count + u] = 2 * TILES * 32 + TILES


def entry_in(list_ref):
    def entry_of(index):
        entry = list_ref[index]
        return (entry >> 5) & 127, entry & 31

    return entry_of


def plan_of(lists_ref, counts_ref, least, sources, index_ref, plan_ref, own_ref):
    lane = rows_of((1, 128), 1)
    low = jnp.zeros((1, 128), jnp.float32)
    high = jnp.zeros((1, 128), jnp.float32)
    top = jnp.zeros((1, 128), jnp.float32)
    index_ref[...] = jnp.zeros((16, 128), jnp.int32)
    index_ref[0:8, 0:TILES] = lists_ref[...]
    index_ref[8:9, 0:TILES] = counts_ref[...]
    tile = index_ref[0:8, :]
    here = jnp.zeros((8, 128), jnp.int32)
    for place, ref in sources:
        low = jnp.where(lane >> 4 == place, ref[80:81, :], low)
        high = jnp.where(lane >> 4 == place, ref[81:82, :], high)
        top = jnp.maximum(top, ref[82:83, :])
        here = jnp.where(tile >> 4 == place, 1, here)
    used = (rows_of((8, 128)) > 0) & (rows_of((8, 128)) < index_ref[8:9, :]) & (here > 0)

    def picked(row):
        return jnp.take_along_axis(
            jnp.broadcast_to(row, (8, 128)), tile, axis=1, mode="promise_in_bounds"
        )

    gap = jnp.maximum(picked(low) - own_ref[81:82, :], own_ref[80:81, :] - picked(high))
    kind = jnp.where(used, jnp.where(gap >= FAR_GAP, 1 << 17, 1 << 16), 0)
    plan_ref[0:8, :] = tile * 32 + (lane & 15) + kind
    plan_ref[8:16, :] = jnp.broadcast_to(jnp.where(top - 0.99 >= least, 1, 0), (8, 128))


def near_term(soft, scaled, offset, inside):
    inverse = lax.rsqrt(soft)
    distance = soft * inverse
    upper = distance + scaled
    gap = distance - scaled
    lower = jnp.minimum(jnp.maximum(offset, jnp.abs(gap)), upper)
    ratio = 1.0 / (lower * upper)
    difference = (upper - lower) * ratio
    total = (upper + lower) * ratio
    weight = gap * upper * inverse
    logs = jnp.log(lower * lower * ratio)
    term = difference * (4.0 - weight * total) + (inverse + inverse) * logs
    if inside:
        term += jnp.where(offset < -gap, 16.0 * (1.0 / offset - 1.0 / lower), 0.0)
    return term


def split_lists(steps_ref, near_ref, far_ref):
    near = jnp.int32(0)
    far = jnp.int32(0)
    for g in range(TILES):
        for k in range(1, 8):
            entry = steps_ref[k, g]
            near_ref[near] = entry
            far_ref[far] = entry
            near = near + ((entry >> 16) & 1)
            far = far + (entry >> 17)
    pad_list(near_ref, near)
    pad_list(far_ref, far)
    return near, far


def sum_pairs(left_ref, right_ref, blocks_ref, offsets_ref, acc_ref, buffers, lists, counts, within, own):
    def produce(w, g):
        return squares(left_ref, right_ref, g, w, 64)

    def consume_near(inside, diagonal):
        def consume(w, slot, buffer):
            scaled = blocks_ref[w, 3:4, :]
            for v in range(8):
                rows = slice(16 * v, 16 * v + 16)
                c = jnp.broadcast_to(scaled, (16, 128))
                if diagonal:
                    same = rows_of((16, 128)) + 16 * v == rows_of((16, 128), 1)
                    c = jnp.where(same, 0.0, c)
                term = near_term(buffer[rows, :], c, offsets_ref[slot, rows, :], inside)
                if diagonal:
                    acc_ref[slot, rows, :] = term
                else:
                    acc_ref[slot, rows, :] += term

        return consume

    def consume_far(w, slot, buffer):
        scaled = blocks_ref[w, 3:4, :]
        for v in range(8):
            rows = slice(16 * v, 16 * v + 16)
            soft = buffer[rows, :]
            inverse = lax.rsqrt(soft)
            gap = soft * inverse - scaled
            ratio = 1.0 / (soft - scaled * scaled)
            logs = jnp.log(gap * gap * ratio)
            acc_ref[slot, rows, :] += (4.0 * scaled) * ratio + (inverse + inverse) * logs

    def near_lists(inside):
        if own:
            run_list(TILES, own_entry, buffers[:4], produce, consume_near(inside, True))
        run_list(counts[0], entry_in(lists[0]), buffers[:4], produce, consume_near(inside, False))

    pl.when(within == 0)(lambda: near_lists(False))
    pl.when(within != 0)(lambda: near_lists(True))
    run_list(counts[1], entry_in(lists[1]), buffers[:4] if own else buffers, produce, consume_far)


def least_of(offset):
    return jnp.min(jnp.min(offset, axis=0, keepdims=True), axis=1, keepdims=True)


def born_own_kernel(
    slab_ref, lists_ref, counts_ref, own_ref, radii_ref,
    blocks_ref, left_ref, right_ref, offsets_ref, acc_ref, plan_ref,
    near_ref, far_ref, index_ref, steps_ref, sem, *buffers,
):
    offset = radii_ref[...] - OFFSET
    plan_of(lists_ref, counts_ref, least_of(offset), ((2, own_ref),), index_ref, plan_ref, own_ref)
    copy = pltpu.make_async_copy(plan_ref, steps_ref, sem)
    copy.start()
    centre = (8 * slab_ref[0] + 4).astype(jnp.float32)
    fill_blocks(blocks_ref, own_ref, 2 * TILES, centre)
    fill_right(right_ref, blocks_ref, 2 * TILES)
    fill_left(left_ref, blocks_ref)
    for g in range(TILES):
        offsets_ref[g] = column_of(offset[g : g + 1])
    offsets_ref[TILES] = offsets_ref[0]
    copy.wait()
    counts = split_lists(steps_ref, near_ref, far_ref)
    sum_pairs(
        left_ref, right_ref, blocks_ref, offsets_ref, acc_ref, buffers,
        (near_ref, far_ref), counts, steps_ref[8, 0], True,
    )


def born_rest_kernel(
    slab_ref, fill_ref, lists_ref, counts_ref, own_ref, p0_ref, p1_ref, p2_ref, p3_ref, radii_ref,
    left_ref, offsets_ref, blocks_in, right_in, acc_in,
    plan_ref, born_ref, send_ref, blocks_ref, right_ref, acc_ref,
    near_ref, far_ref, index_ref, steps_ref, sem, sums_ref, *buffers,
):
    slab = slab_ref[0]
    sources = tuple(zip(slots(slab), (p0_ref, p1_ref, p2_ref, p3_ref)))
    offset = radii_ref[...] - OFFSET
    plan_of(lists_ref, counts_ref, least_of(offset), sources, index_ref, plan_ref, own_ref)
    copy = pltpu.make_async_copy(plan_ref, steps_ref, sem)
    copy.start()
    centre = (8 * slab + 4).astype(jnp.float32)
    for place, ref in sources:
        fill_blocks(blocks_ref, ref, place * TILES, centre)
        fill_right(right_ref, blocks_ref, place * TILES)
    copy.wait()
    counts = split_lists(steps_ref, near_ref, far_ref)
    sum_pairs(
        left_ref, right_ref, blocks_ref, offsets_ref, acc_ref, buffers,
        (near_ref, far_ref), counts, steps_ref[8, 0], False,
    )
    for g in range(TILES):
        sums_ref[g : g + 1, :] = jnp.sum(acc_ref[g].T, axis=0, keepdims=True)
    slot = rows_of((TILES, 128)) * 128 + rows_of((TILES, 128), 1)
    live = slot < fill_ref[0]
    radius = jnp.where(live, radii_ref[...], 1.5)
    inner = radius - OFFSET
    psi = 0.125 * sums_ref[...] * inner
    bending = jnp.tanh(psi - 0.8 * psi * psi + 4.85 * psi * psi * psi)
    born = 1.0 / (1.0 / inner - bending / radius)
    born_ref[...] = jnp.where(live, born, 0.0)
    send_ref[...] = jnp.where(live, born, 1.0)


def energy_list(plan_ref, steps_ref, list_ref, sem):
    copy = pltpu.make_async_copy(plan_ref, steps_ref, sem)
    copy.start()
    copy.wait()
    count = jnp.int32(0)
    for g in range(TILES):
        for k in range(1, 8):
            entry = steps_ref[k, g]
            list_ref[count] = entry
            count = count + jnp.minimum(entry >> 16, 1)
    pad_list(list_ref, count)
    return count


def sum_energy(left_ref, right_ref, blocks_ref, born_ref, column_ref, inverse_ref, acc_ref, buffers, entries, count, first):
    def produce(w, g):
        return squares(left_ref, right_ref, g, w, 48)

    def consume(w, slot, buffer):
        charge = blocks_ref[w, 4:5, :]
        partner = born_ref[pl.ds(w, 1), :]
        backward = 1.0 / partner
        for v in range(8):
            rows = slice(16 * v, 16 * v + 16)
            squared = buffer[rows, :]
            product = column_ref[slot, rows, :] * partner
            decay = jnp.exp2(squared * (inverse_ref[slot, rows, :] * backward))
            term = charge * lax.rsqrt(squared + product * decay)
            if first:
                acc_ref[slot, rows, :] = term
            else:
                acc_ref[slot, rows, :] += term

    run_list(count, entries, buffers, produce, consume)


def energy_own_kernel(
    plan_ref, blocks_ref, left_ref, right_ref, own_ref,
    column_ref, inverse_ref, acc_ref,
    list_ref, steps_ref, born_ref, sem, *buffers,
):
    count = energy_list(plan_ref, steps_ref, list_ref, sem)
    born_ref[2 * TILES : 3 * TILES, :] = own_ref[...]
    for g in range(TILES):
        column = column_of(own_ref[g : g + 1, :])
        column_ref[g] = column
        inverse_ref[g] = (-0.25 * LOG2E) / column
    column_ref[TILES] = column_ref[0]
    inverse_ref[TILES] = inverse_ref[0]
    shared = (left_ref, right_ref, blocks_ref, born_ref, column_ref, inverse_ref, acc_ref)
    sum_energy(*shared, buffers, own_entry, TILES, True)
    sum_energy(*shared, buffers[:4], entry_in(list_ref), count, False)


def energy_rest_kernel(
    slab_ref, plan_ref, blocks_ref, left_ref, right_ref, r0_ref, r1_ref, r2_ref, r3_ref,
    column_ref, inverse_ref, acc_in,
    energy_ref, share_ref, acc_ref,
    list_ref, steps_ref, born_ref, sem, charge_ref, *buffers,
):
    count = energy_list(plan_ref, steps_ref, list_ref, sem)
    for place, ref in zip(slots(slab_ref[0]), (r0_ref, r1_ref, r2_ref, r3_ref)):
        born_ref[pl.ds(place * TILES, TILES), :] = ref[...]
    born_ref[2 * TILES : 3 * TILES, :] = jnp.ones((TILES, 128), jnp.float32)
    sum_energy(
        left_ref, right_ref, blocks_ref, born_ref, column_ref, inverse_ref, acc_ref, buffers,
        entry_in(list_ref), count, False,
    )
    for g in range(TILES):
        energy_ref[g : g + 1, :] = jnp.sum(acc_ref[g].T, axis=0, keepdims=True)
        charge_ref[g : g + 1, :] = blocks_ref[2 * TILES + g, 4:5, :]
    energy = -0.5 * charge_ref[...] * energy_ref[...]
    energy_ref[...] = energy
    share = jnp.sum(jnp.sum(energy, axis=0, keepdims=True), axis=1, keepdims=True)
    share_ref[...] = jnp.broadcast_to(share[None], share_ref.shape)


def total_kernel(shares_ref, total_ref):
    total = shares_ref[0]
    for i in range(1, shares_ref.shape[0]):
        total = total + shares_ref[i]
    total_ref[0] = total[0, 0]


def shards(coords, charges, radii, screens, tile_lists, tile_counts, slab_fill):
    f32 = jnp.float32
    count = lax.axis_size(SLAB)
    smem = pl.BlockSpec(memory_space=pltpu.SMEM)
    vmem = pl.BlockSpec(memory_space=pltpu.VMEM)

    def near(*values):
        return tuple(pltpu.with_memory_space_constraint(value, pltpu.VMEM) for value in values)

    def call(kernel, name, outs, scalars, arrays, scratch, aliases=None, out_specs=None, flops=0):
        return pl.pallas_call(
            kernel,
            out_shape=outs,
            in_specs=[smem] * len(scalars) + [vmem] * len(arrays),
            out_specs=out_specs or (vmem,) * len(outs),
            scratch_shapes=scratch,
            input_output_aliases=aliases or {},
            cost_estimate=pl.CostEstimate(flops=flops, transcendentals=0, bytes_accessed=0),
            compiler_params=pltpu.CompilerParams(vmem_limit_bytes=20 << 20),
            name=name,
        )(*scalars, *arrays)

    stack = pltpu.VMEM((TILES + 1, 128, 128), f32)
    blocks_type = pltpu.VMEM((5 * TILES, 8, 128), f32)
    right_type = pltpu.VMEM((5 * TILES, 64, 128), jnp.bfloat16)
    left_type = pltpu.VMEM((TILES, 128, 64), jnp.bfloat16)
    plan_type = pltpu.VMEM((16, 128), jnp.int32)
    slab_type = pltpu.VMEM((TILES, 128), f32)
    entries = pltpu.SMEM((144,), jnp.int32)
    steps = pltpu.SMEM((16, 128), jnp.int32)
    squares = [pltpu.VMEM((128, 128), f32)] * 8
    sem = pltpu.SemaphoreType.DMA

    slab = lax.axis_index(SLAB).astype(jnp.int32)[None]
    charges, radii, screens = (v.reshape(TILES, 128) for v in (charges, radii, screens))
    lists, counts = tile_lists.T, tile_counts.reshape(1, TILES)
    coords, charges, radii, screens, lists, counts = (
        pltpu.with_memory_space_constraint(value, pltpu.HBM)
        for value in (coords, charges, radii, screens, lists, counts)
    )
    (packed,) = call(
        prep_kernel, "prep", (pltpu.VMEM((ROWS, 128), f32),),
        (slab, slab_fill), (coords, charges, radii, screens), [],
    )
    around = neighbours(packed)
    (packed,) = near(packed)
    blocks, left, right, offsets, acc, own_plan = call(
        born_own_kernel, "born_own",
        (blocks_type, left_type, right_type, stack, stack, plan_type),
        (slab,), (lists, counts, packed, radii),
        [entries, entries, plan_type, steps, sem] + squares, flops=1 << 27,
    )
    plan, born, send, blocks, right, acc = call(
        born_rest_kernel, "born_rest",
        (plan_type, jax.ShapeDtypeStruct((TILES, 128), f32), slab_type, blocks_type, right_type, stack),
        (slab, slab_fill),
        (lists, counts, packed, *near(*around), radii, *near(left, offsets, blocks, right, acc)),
        [entries, entries, plan_type, steps, sem, slab_type] + squares,
        aliases={12: 3, 13: 4, 14: 5},
    )
    far_born = neighbours(send)
    column, inverse, acc = call(
        energy_own_kernel, "energy_own", (stack,) * 3,
        (), near(own_plan, blocks, left, right, send),
        [entries, steps, pltpu.VMEM((5 * TILES, 128), f32), sem] + squares, flops=1 << 27,
    )
    energy, share, acc = call(
        energy_rest_kernel, "energy_rest",
        (jax.ShapeDtypeStruct((TILES, 128), f32), pltpu.VMEM((count, 1, 128), f32), stack),
        (slab,), near(plan, blocks, left, right, *far_born, column, inverse, acc),
        [entries, steps, pltpu.VMEM((5 * TILES, 128), f32), sem, slab_type] + squares,
        aliases={11: 2},
    )
    shares = lax.all_to_all(share, SLAB, 0, 0, tiled=True)
    (total,) = call(
        total_kernel, "total", (jax.ShapeDtypeStruct((1,), f32),), (), near(shares), [], out_specs=(smem,)
    )
    return (born.reshape(-1), energy.reshape(-1), total[0])


def solution(mesh):
    torus = Mesh(mesh.devices.reshape(4, 8, 4, 2), SLAB)
    placed = (P(None, SLAB), P(SLAB), P(SLAB), P(SLAB), P(SLAB, None), P(SLAB), P(SLAB))
    return jax.shard_map(
        shards, mesh=torus, in_specs=placed, out_specs=(P(SLAB), P(SLAB), P()), check_vma=False
    )
```

```python
import jax
import jax.numpy as jnp
from jax import lax
from jax.experimental import pallas as pl
from jax.experimental.pallas import tpu as pltpu
from jax.sharding import Mesh
from jax.sharding import PartitionSpec as P

SLAB = ("slab_0", "slab_1", "slab_2", "slab_3")
OFFSET = 0.09
LOG2E = 1.4426950408889634
TILES = 16
UNROLL = 8
FAR_GAP = 3.5
ROWS = 88


def chip_swap(count, odd):
    pairs = []
    for chip in range(count // 2):
        other = ((chip + odd) ^ 1) - odd
        for core in (0, 1):
            if 0 <= other < count // 2:
                pairs.append((2 * chip + core, 2 * other + core))
            else:
                pairs.append((2 * chip + core, 2 * chip + 1 - core))
    return pairs


def neighbours(value):
    count = lax.axis_size(SLAB)
    other = lax.ppermute(value, SLAB, [(i, i ^ 1) for i in range(count)])
    both = jnp.concatenate([value, other], axis=0)
    return [other] + [lax.ppermute(both, SLAB, chip_swap(count, odd)) for odd in (0, 1)]


def rows_in(ref):
    return lambda start, size: ref[pl.ds(start, size), :]


def inner_slot(slab):
    return jnp.where(slab % 2 == 0, 3, 1)


def outer_slabs(slab, even, odd, height):
    ahead = (slab // 2) % 2 == 0
    far = jnp.where(ahead, 4, 0)
    from_even = ahead == (slab % 2 == 1)

    def crossed(start, size):
        rows = pl.ds(height + start, size)
        return jnp.where(from_even, even[rows, :], odd[rows, :])

    return ((4 - inner_slot(slab), crossed), (far, rows_in(even)), (4 - far, rows_in(odd)))


def rows_of(shape, axis=0):
    return lax.broadcasted_iota(jnp.int32, shape, axis)


def prep_kernel(slab_ref, fill_ref, coords_ref, charges_ref, radii_ref, screens_ref, out_ref):
    fill = fill_ref[0]
    middle = (8 * slab_ref[0] + 4).astype(jnp.float32)
    slot = rows_of((TILES, 128)) * 128 + rows_of((TILES, 128), 1)
    live = slot < fill
    scaled = jnp.where(live, screens_ref[...] * (radii_ref[...] - OFFSET), 0.0)
    charge = jnp.where(live, charges_ref[...], 0.0)
    home = jnp.where(rows_of((3, 128)) == 2, middle, 0.0)
    lane = rows_of((3, 128), 1)
    column = rows_of((1, 128), 1) % TILES
    low = jnp.zeros((1, 128), jnp.float32)
    high = jnp.zeros((1, 128), jnp.float32)
    for t in range(TILES):
        xyz = jnp.where(lane + t * 128 < fill, coords_ref[:, t * 128 : (t + 1) * 128], home)
        out_ref[5 * t : 5 * t + 3, :] = xyz
        out_ref[5 * t + 3 : 5 * t + 4, :] = scaled[t : t + 1]
        out_ref[5 * t + 4 : 5 * t + 5, :] = charge[t : t + 1]
        low = jnp.where(column == t, jnp.min(xyz[2:3], axis=1, keepdims=True), low)
        high = jnp.where(column == t, jnp.max(xyz[2:3], axis=1, keepdims=True), high)
    top = jnp.max(jnp.max(scaled, axis=0, keepdims=True), axis=1, keepdims=True)
    out_ref[80:81, :] = low
    out_ref[81:82, :] = high
    out_ref[82:83, :] = jnp.broadcast_to(top, (1, 128))
    out_ref[83:88, :] = jnp.zeros((5, 128), jnp.float32)


def parts_of(rows):
    first = rows.astype(jnp.bfloat16).astype(jnp.float32)
    rest = rows - first
    second = rest.astype(jnp.bfloat16).astype(jnp.float32)
    third = (rest - second).astype(jnp.bfloat16).astype(jnp.float32)
    return first, second, third


def fill_blocks(blocks_ref, read, base, centre):
    row = rows_of((8, 128))
    shift = jnp.where(row == 2, centre, 0.0)
    tail = jnp.where(row == 6, 1.0, 0.0)
    for t in range(TILES):
        block = read(5 * t, 8) - shift
        square = block * block
        norm = square[0:1] + square[1:2] + square[2:3]
        blocks_ref[base + t] = jnp.where(row < 5, block, jnp.where(row == 5, norm, tail))


def fill_right(right_ref, blocks_ref, base):
    last = jnp.where(rows_of((16, 128)) == 0, 1.0, 0.0)
    for t in range(TILES):
        b1, b2, b3 = parts_of(blocks_ref[base + t])
        stack = jnp.concatenate([b1, b2, b3, b1, b2, b1, last], axis=0)
        right_ref[base + t] = stack.astype(jnp.bfloat16)


def fill_left(left_ref, blocks_ref):
    row = rows_of((8, 128))
    last = jnp.where(rows_of((16, 128)) == 0, 1.0, 0.0)
    for g in range(TILES):
        block = blocks_ref[2 * TILES + g]
        norm = jnp.broadcast_to(block[5:6], (8, 128))
        left = jnp.where(
            row < 3, -2.0 * block, jnp.where(row == 5, 1.0, jnp.where(row == 6, norm, 0.0))
        )
        a1, a2, a3 = parts_of(left)
        stack = jnp.concatenate([a1, a1, a1, a2, a2, a3, last], axis=0)
        left_ref[g] = stack.T.astype(jnp.bfloat16)


def column_of(row):
    return jnp.broadcast_to(row, (128, 128)).T


def squares(left_ref, right_ref, g, w, depth):
    return jnp.dot(
        left_ref[g, :, :depth], right_ref[w, :depth, :], preferred_element_type=jnp.float32
    )


def run_list(count, entry_of, buffers, produce, consume):
    unroll = len(buffers)

    def fetch(base):
        for u, buffer in enumerate(buffers):
            w, slot = entry_of(base + u)
            buffer[...] = produce(w, jnp.minimum(slot, TILES - 1))

    fetch(0)

    @pl.loop(0, (count + unroll - 1) // unroll)
    def _(step):
        base = step * unroll
        for u, buffer in enumerate(buffers):
            w, slot = entry_of(base + u)
            consume(w, slot, buffer)
        fetch(base + unroll)


def own_entry(index):
    return 2 * TILES + jnp.minimum(index, TILES - 1), index


def pad_list(list_ref, count):
    for u in range(2 * UNROLL):
        list_ref[count + u] = 2 * TILES * 32 + TILES


def entry_in(list_ref):
    def entry_of(index):
        entry = list_ref[index]
        return (entry >> 5) & 127, entry & 31

    return entry_of


def plan_of(lists_ref, counts_ref, least, sources, index_ref, plan_ref, own_ref):
    lane = rows_of((1, 128), 1)
    low = jnp.zeros((1, 128), jnp.float32)
    high = jnp.zeros((1, 128), jnp.float32)
    top = jnp.zeros((1, 128), jnp.float32)
    index_ref[...] = jnp.zeros((16, 128), jnp.int32)
    index_ref[0:8, 0:TILES] = lists_ref[...]
    index_ref[8:9, 0:TILES] = counts_ref[...]
    tile = index_ref[0:8, :]
    here = jnp.zeros((8, 128), jnp.int32)
    for place, read in sources:
        ranges = read(80, 8)
        low = jnp.where(lane >> 4 == place, ranges[0:1], low)
        high = jnp.where(lane >> 4 == place, ranges[1:2], high)
        top = jnp.maximum(top, ranges[2:3])
        here = jnp.where(tile >> 4 == place, 1, here)
    used = (rows_of((8, 128)) > 0) & (rows_of((8, 128)) < index_ref[8:9, :]) & (here > 0)

    def picked(row):
        return jnp.take_along_axis(
            jnp.broadcast_to(row, (8, 128)), tile, axis=1, mode="promise_in_bounds"
        )

    gap = jnp.maximum(picked(low) - own_ref[81:82, :], own_ref[80:81, :] - picked(high))
    kind = jnp.where(used, jnp.where(gap >= FAR_GAP, 1 << 17, 1 << 16), 0)
    plan_ref[0:8, :] = tile * 32 + (lane & 15) + kind
    plan_ref[8:16, :] = jnp.broadcast_to(jnp.where(top - 0.99 >= least, 1, 0), (8, 128))


def near_term(soft, scaled, offset, inside):
    inverse = lax.rsqrt(soft)
    distance = soft * inverse
    upper = distance + scaled
    gap = distance - scaled
    lower = jnp.minimum(jnp.maximum(offset, jnp.abs(gap)), upper)
    ratio = 1.0 / (lower * upper)
    difference = (upper - lower) * ratio
    total = (upper + lower) * ratio
    weight = gap * upper * inverse
    logs = jnp.log(lower * lower * ratio)
    term = difference * (4.0 - weight * total) + (inverse + inverse) * logs
    if inside:
        term += jnp.where(offset < -gap, 16.0 * (1.0 / offset - 1.0 / lower), 0.0)
    return term


def split_lists(steps_ref, near_ref, far_ref):
    near = jnp.int32(0)
    far = jnp.int32(0)
    for g in range(TILES):
        for k in range(1, 8):
            entry = steps_ref[k, g]
            near_ref[near] = entry
            far_ref[far] = entry
            near = near + ((entry >> 16) & 1)
            far = far + (entry >> 17)
    pad_list(near_ref, near)
    pad_list(far_ref, far)
    return near, far


def sum_pairs(left_ref, right_ref, blocks_ref, offsets_ref, acc_ref, buffers, lists, counts, within, own):
    def produce(w, g):
        return squares(left_ref, right_ref, g, w, 64)

    def consume_near(inside, diagonal):
        def consume(w, slot, buffer):
            scaled = blocks_ref[w, 3:4, :]
            for v in range(8):
                rows = slice(16 * v, 16 * v + 16)
                c = jnp.broadcast_to(scaled, (16, 128))
                if diagonal:
                    same = rows_of((16, 128)) + 16 * v == rows_of((16, 128), 1)
                    c = jnp.where(same, 0.0, c)
                term = near_term(buffer[rows, :], c, offsets_ref[slot, rows, :], inside)
                if diagonal:
                    acc_ref[slot, rows, :] = term
                else:
                    acc_ref[slot, rows, :] += term

        return consume

    def consume_far(w, slot, buffer):
        scaled = blocks_ref[w, 3:4, :]
        for v in range(8):
            rows = slice(16 * v, 16 * v + 16)
            soft = buffer[rows, :]
            inverse = lax.rsqrt(soft)
            gap = soft * inverse - scaled
            ratio = 1.0 / (soft - scaled * scaled)
            logs = jnp.log(gap * gap * ratio)
            acc_ref[slot, rows, :] += (4.0 * scaled) * ratio + (inverse + inverse) * logs

    def near_lists(inside):
        if own:
            run_list(TILES, own_entry, buffers[:4], produce, consume_near(inside, True))
        run_list(counts[0], entry_in(lists[0]), buffers[:4], produce, consume_near(inside, False))

    pl.when(within == 0)(lambda: near_lists(False))
    pl.when(within != 0)(lambda: near_lists(True))
    run_list(counts[1], entry_in(lists[1]), buffers, produce, consume_far)


def least_of(offset):
    return jnp.min(jnp.min(offset, axis=0, keepdims=True), axis=1, keepdims=True)


def born_own_kernel(
    slab_ref, lists_ref, counts_ref, own_ref, other_ref, radii_ref,
    blocks_ref, left_ref, right_ref, offsets_ref, acc_ref, plan_ref,
    near_ref, far_ref, index_ref, steps_ref, sem, *buffers,
):
    offset = radii_ref[...] - OFFSET
    sources = ((2, rows_in(own_ref)), (inner_slot(slab_ref[0]), rows_in(other_ref)))
    plan_of(lists_ref, counts_ref, least_of(offset), sources, index_ref, plan_ref, own_ref)
    copy = pltpu.make_async_copy(plan_ref, steps_ref, sem)
    copy.start()
    centre = (8 * slab_ref[0] + 4).astype(jnp.float32)
    for place, read in sources:
        fill_blocks(blocks_ref, read, place * TILES, centre)
        fill_right(right_ref, blocks_ref, place * TILES)
    fill_left(left_ref, blocks_ref)
    for g in range(TILES):
        offsets_ref[g] = column_of(offset[g : g + 1])
    offsets_ref[TILES] = offsets_ref[0]
    copy.wait()
    counts = split_lists(steps_ref, near_ref, far_ref)
    sum_pairs(
        left_ref, right_ref, blocks_ref, offsets_ref, acc_ref, buffers,
        (near_ref, far_ref), counts, steps_ref[8, 0], True,
    )


def born_rest_kernel(
    slab_ref, fill_ref, lists_ref, counts_ref, own_ref, even_ref, odd_ref, radii_ref,
    left_ref, offsets_ref, blocks_in, right_in, acc_in,
    plan_ref, born_ref, send_ref, blocks_ref, right_ref, acc_ref,
    near_ref, far_ref, index_ref, steps_ref, sem, sums_ref, *buffers,
):
    slab = slab_ref[0]
    sources = outer_slabs(slab, even_ref, odd_ref, ROWS)
    offset = radii_ref[...] - OFFSET
    plan_of(lists_ref, counts_ref, least_of(offset), sources, index_ref, plan_ref, own_ref)
    copy = pltpu.make_async_copy(plan_ref, steps_ref, sem)
    copy.start()
    centre = (8 * slab + 4).astype(jnp.float32)
    for place, read in sources:
        fill_blocks(blocks_ref, read, place * TILES, centre)
        fill_right(right_ref, blocks_ref, place * TILES)
    copy.wait()
    counts = split_lists(steps_ref, near_ref, far_ref)
    sum_pairs(
        left_ref, right_ref, blocks_ref, offsets_ref, acc_ref, buffers,
        (near_ref, far_ref), counts, steps_ref[8, 0], False,
    )
    for g in range(TILES):
        sums_ref[g : g + 1, :] = jnp.sum(acc_ref[g].T, axis=0, keepdims=True)
    slot = rows_of((TILES, 128)) * 128 + rows_of((TILES, 128), 1)
    live = slot < fill_ref[0]
    radius = jnp.where(live, radii_ref[...], 1.5)
    inner = radius - OFFSET
    psi = 0.125 * sums_ref[...] * inner
    bending = jnp.tanh(psi - 0.8 * psi * psi + 4.85 * psi * psi * psi)
    born = 1.0 / (1.0 / inner - bending / radius)
    born_ref[...] = jnp.where(live, born, 0.0)
    send_ref[...] = jnp.where(live, born, 1.0)


def energy_list(plan_ref, steps_ref, list_ref, sem):
    copy = pltpu.make_async_copy(plan_ref, steps_ref, sem)
    copy.start()
    copy.wait()
    count = jnp.int32(0)
    for g in range(TILES):
        for k in range(1, 8):
            entry = steps_ref[k, g]
            list_ref[count] = entry
            count = count + jnp.minimum(entry >> 16, 1)
    pad_list(list_ref, count)
    return count


def sum_energy(left_ref, right_ref, blocks_ref, born_ref, column_ref, inverse_ref, acc_ref, buffers, entries, count, first):
    def produce(w, g):
        return squares(left_ref, right_ref, g, w, 48)

    def consume(w, slot, buffer):
        charge = blocks_ref[w, 4:5, :]
        partner = born_ref[pl.ds(w, 1), :]
        backward = 1.0 / partner
        for v in range(8):
            rows = slice(16 * v, 16 * v + 16)
            squared = buffer[rows, :]
            product = column_ref[slot, rows, :] * partner
            decay = jnp.exp2(squared * (inverse_ref[slot, rows, :] * backward))
            term = charge * lax.rsqrt(squared + product * decay)
            if first:
                acc_ref[slot, rows, :] = term
            else:
                acc_ref[slot, rows, :] += term

    run_list(count, entries, buffers, produce, consume)


def energy_own_kernel(
    slab_ref, plan_ref, blocks_ref, left_ref, right_ref, own_ref, other_ref,
    column_ref, inverse_ref, acc_ref,
    list_ref, steps_ref, born_ref, sem, *buffers,
):
    count = energy_list(plan_ref, steps_ref, list_ref, sem)
    born_ref[2 * TILES : 3 * TILES, :] = own_ref[...]
    born_ref[pl.ds(inner_slot(slab_ref[0]) * TILES, TILES), :] = other_ref[...]
    for g in range(TILES):
        column = column_of(own_ref[g : g + 1, :])
        column_ref[g] = column
        inverse_ref[g] = (-0.25 * LOG2E) / column
    column_ref[TILES] = column_ref[0]
    inverse_ref[TILES] = inverse_ref[0]
    shared = (left_ref, right_ref, blocks_ref, born_ref, column_ref, inverse_ref, acc_ref)
    sum_energy(*shared, buffers, own_entry, TILES, True)
    sum_energy(*shared, buffers, entry_in(list_ref), count, False)


def energy_rest_kernel(
    slab_ref, plan_ref, blocks_ref, left_ref, right_ref, even_ref, odd_ref,
    column_ref, inverse_ref, acc_in,
    energy_ref, share_ref, acc_ref,
    list_ref, steps_ref, born_ref, sem, charge_ref, *buffers,
):
    count = energy_list(plan_ref, steps_ref, list_ref, sem)
    for place, read in outer_slabs(slab_ref[0], even_ref, odd_ref, TILES):
        born_ref[pl.ds(place * TILES, TILES), :] = read(0, TILES)
    born_ref[2 * TILES : 3 * TILES, :] = jnp.ones((TILES, 128), jnp.float32)
    sum_energy(
        left_ref, right_ref, blocks_ref, born_ref, column_ref, inverse_ref, acc_ref, buffers,
        entry_in(list_ref), count, False,
    )
    for g in range(TILES):
        energy_ref[g : g + 1, :] = jnp.sum(acc_ref[g].T, axis=0, keepdims=True)
        charge_ref[g : g + 1, :] = blocks_ref[2 * TILES + g, 4:5, :]
    energy = -0.5 * charge_ref[...] * energy_ref[...]
    energy_ref[...] = energy
    share = jnp.sum(jnp.sum(energy, axis=0, keepdims=True), axis=1, keepdims=True)
    share_ref[...] = jnp.broadcast_to(share[None], share_ref.shape)


def total_kernel(shares_ref, total_ref):
    total = shares_ref[0]
    for i in range(1, shares_ref.shape[0]):
        total = total + shares_ref[i]
    total_ref[0] = total[0, 0]


def shards(coords, charges, radii, screens, tile_lists, tile_counts, slab_fill):
    f32 = jnp.float32
    count = lax.axis_size(SLAB)
    smem = pl.BlockSpec(memory_space=pltpu.SMEM)
    vmem = pl.BlockSpec(memory_space=pltpu.VMEM)

    def near(*values):
        return tuple(pltpu.with_memory_space_constraint(value, pltpu.VMEM) for value in values)

    def call(kernel, name, outs, scalars, arrays, scratch, aliases=None, out_specs=None, flops=0):
        return pl.pallas_call(
            kernel,
            out_shape=outs,
            in_specs=[smem] * len(scalars) + [vmem] * len(arrays),
            out_specs=out_specs or (vmem,) * len(outs),
            scratch_shapes=scratch,
            input_output_aliases=aliases or {},
            cost_estimate=pl.CostEstimate(flops=flops, transcendentals=0, bytes_accessed=0),
            compiler_params=pltpu.CompilerParams(vmem_limit_bytes=20 << 20),
            name=name,
        )(*scalars, *arrays)

    stack = pltpu.VMEM((TILES + 1, 128, 128), f32)
    blocks_type = pltpu.VMEM((5 * TILES, 8, 128), f32)
    right_type = pltpu.VMEM((5 * TILES, 64, 128), jnp.bfloat16)
    left_type = pltpu.VMEM((TILES, 128, 64), jnp.bfloat16)
    plan_type = pltpu.VMEM((16, 128), jnp.int32)
    slab_type = pltpu.VMEM((TILES, 128), f32)
    entries = pltpu.SMEM((144,), jnp.int32)
    steps = pltpu.SMEM((16, 128), jnp.int32)
    squares = [pltpu.VMEM((128, 128), f32)] * 8
    sem = pltpu.SemaphoreType.DMA

    slab = lax.axis_index(SLAB).astype(jnp.int32)[None]
    charges, radii, screens = (v.reshape(TILES, 128) for v in (charges, radii, screens))
    lists, counts = tile_lists.T, tile_counts.reshape(1, TILES)
    coords, charges, radii, screens, lists, counts = (
        pltpu.with_memory_space_constraint(value, pltpu.HBM)
        for value in (coords, charges, radii, screens, lists, counts)
    )
    (packed,) = call(
        prep_kernel, "prep", (pltpu.VMEM((ROWS, 128), f32),),
        (slab, slab_fill), (coords, charges, radii, screens), [],
    )
    other, even, odd = neighbours(packed)
    packed, other, even, odd = near(packed, other, even, odd)
    blocks, left, right, offsets, acc, own_plan = call(
        born_own_kernel, "born_own",
        (blocks_type, left_type, right_type, stack, stack, plan_type),
        (slab,), (lists, counts, packed, other, radii),
        [entries, entries, plan_type, steps, sem] + squares, flops=1 << 27,
    )
    plan, born, send, blocks, right, acc = call(
        born_rest_kernel, "born_rest",
        (plan_type, jax.ShapeDtypeStruct((TILES, 128), f32), slab_type, blocks_type, right_type, stack),
        (slab, slab_fill),
        (lists, counts, packed, even, odd, radii, *near(left, offsets, blocks, right, acc)),
        [entries, entries, plan_type, steps, sem, slab_type] + squares,
        aliases={10: 3, 11: 4, 12: 5},
    )
    born_other, born_even, born_odd = neighbours(send)
    column, inverse, acc = call(
        energy_own_kernel, "energy_own", (stack,) * 3,
        (slab,), near(own_plan, blocks, left, right, send, born_other),
        [entries, steps, pltpu.VMEM((5 * TILES, 128), f32), sem] + squares, flops=1 << 27,
    )
    energy, share, acc = call(
        energy_rest_kernel, "energy_rest",
        (jax.ShapeDtypeStruct((TILES, 128), f32), pltpu.VMEM((count, 1, 128), f32), stack),
        (slab,), near(plan, blocks, left, right, born_even, born_odd, column, inverse, acc),
        [entries, steps, pltpu.VMEM((5 * TILES, 128), f32), sem, slab_type] + squares,
        aliases={9: 2},
    )
    shares = lax.all_to_all(share, SLAB, 0, 0, tiled=True)
    (total,) = call(
        total_kernel, "total", (jax.ShapeDtypeStruct((1,), f32),), (), near(shares), [], out_specs=(smem,)
    )
    return (born.reshape(-1), energy.reshape(-1), total[0])


def solution(mesh):
    torus = Mesh(mesh.devices.reshape(4, 8, 4, 2), SLAB)
    placed = (P(None, SLAB), P(SLAB), P(SLAB), P(SLAB), P(SLAB, None), P(SLAB), P(SLAB))
    return jax.shard_map(
        shards, mesh=torus, in_specs=placed, out_specs=(P(SLAB), P(SLAB), P()), check_vma=False
    )
```

```python
import jax
import jax.numpy as jnp
from jax import lax
from jax.experimental import pallas as pl
from jax.experimental.pallas import tpu as pltpu
from jax.sharding import Mesh
from jax.sharding import PartitionSpec as P

SLAB = ("slab_0", "slab_1", "slab_2", "slab_3")
OFFSET = 0.09
LOG2E = 1.4426950408889634
TILES = 16
UNROLL = 8
FAR_GAP = 3.5
ROWS = 88


def chip_swap(count, odd):
    pairs = []
    for chip in range(count // 2):
        other = ((chip + odd) ^ 1) - odd
        for core in (0, 1):
            if 0 <= other < count // 2:
                pairs.append((2 * chip + core, 2 * other + core))
            else:
                pairs.append((2 * chip + core, 2 * chip + 1 - core))
    return pairs


def neighbours(value):
    count = lax.axis_size(SLAB)
    other = lax.ppermute(value, SLAB, [(i, i ^ 1) for i in range(count)])
    both = jnp.concatenate([value, other], axis=0)
    return [other] + [lax.ppermute(both, SLAB, chip_swap(count, odd)) for odd in (0, 1)]


def rows_in(ref):
    return lambda start, size: ref[pl.ds(start, size), :]


def inner_slot(slab):
    return jnp.where(slab % 2 == 0, 3, 1)


def outer_slabs(slab, even, odd, height):
    ahead = (slab // 2) % 2 == 0
    far = jnp.where(ahead, 4, 0)
    from_even = ahead == (slab % 2 == 1)

    def crossed(start, size):
        rows = pl.ds(height + start, size)
        return jnp.where(from_even, even[rows, :], odd[rows, :])

    return ((4 - inner_slot(slab), crossed), (far, rows_in(even)), (4 - far, rows_in(odd)))


def rows_of(shape, axis=0):
    return lax.broadcasted_iota(jnp.int32, shape, axis)


def prep_kernel(
    slab_ref, fill_ref, coords_ref, charges_ref, radii_ref, screens_ref, lists_ref, counts_ref,
    out_ref, index_ref, kept_ref,
):
    index_ref[...] = jnp.zeros((8, 128), jnp.int32)
    for k in range(8):
        lanes = slice(TILES * k, TILES * k + TILES)
        index_ref[0:1, lanes] = lists_ref[k : k + 1, :]
        index_ref[1:2, lanes] = counts_ref[...]
    kept_ref[...] = radii_ref[...]
    fill = fill_ref[0]
    middle = (8 * slab_ref[0] + 4).astype(jnp.float32)
    slot = rows_of((TILES, 128)) * 128 + rows_of((TILES, 128), 1)
    live = slot < fill
    scaled = jnp.where(live, screens_ref[...] * (radii_ref[...] - OFFSET), 0.0)
    charge = jnp.where(live, charges_ref[...], 0.0)
    home = jnp.where(rows_of((3, 128)) == 2, middle, 0.0)
    lane = rows_of((3, 128), 1)
    column = rows_of((1, 128), 1) % TILES
    low = jnp.zeros((1, 128), jnp.float32)
    high = jnp.zeros((1, 128), jnp.float32)
    for t in range(TILES):
        xyz = jnp.where(lane + t * 128 < fill, coords_ref[:, t * 128 : (t + 1) * 128], home)
        out_ref[5 * t : 5 * t + 3, :] = xyz
        out_ref[5 * t + 3 : 5 * t + 4, :] = scaled[t : t + 1]
        out_ref[5 * t + 4 : 5 * t + 5, :] = charge[t : t + 1]
        low = jnp.where(column == t, jnp.min(xyz[2:3], axis=1, keepdims=True), low)
        high = jnp.where(column == t, jnp.max(xyz[2:3], axis=1, keepdims=True), high)
    top = jnp.max(jnp.max(scaled, axis=0, keepdims=True), axis=1, keepdims=True)
    out_ref[80:81, :] = low
    out_ref[81:82, :] = high
    out_ref[82:83, :] = jnp.broadcast_to(top, (1, 128))
    out_ref[83:88, :] = jnp.zeros((5, 128), jnp.float32)


def parts_of(rows):
    first = rows.astype(jnp.bfloat16).astype(jnp.float32)
    rest = rows - first
    second = rest.astype(jnp.bfloat16).astype(jnp.float32)
    third = (rest - second).astype(jnp.bfloat16).astype(jnp.float32)
    return first, second, third


def fill_blocks(blocks_ref, read, base, centre):
    row = rows_of((8, 128))
    shift = jnp.where(row == 2, centre, 0.0)
    tail = jnp.where(row == 6, 1.0, 0.0)
    for t in range(TILES):
        block = read(5 * t, 8) - shift
        square = block * block
        norm = square[0:1] + square[1:2] + square[2:3]
        blocks_ref[base + t] = jnp.where(row < 5, block, jnp.where(row == 5, norm, tail))


def fill_right(right_ref, blocks_ref, base):
    last = jnp.where(rows_of((16, 128)) == 0, 1.0, 0.0)
    for t in range(TILES):
        b1, b2, b3 = parts_of(blocks_ref[base + t])
        stack = jnp.concatenate([b1, b2, b3, b1, b2, b1, last], axis=0)
        right_ref[base + t] = stack.astype(jnp.bfloat16)


def fill_left(left_ref, blocks_ref):
    row = rows_of((8, 128))
    last = jnp.where(rows_of((16, 128)) == 0, 1.0, 0.0)
    for g in range(TILES):
        block = blocks_ref[2 * TILES + g]
        norm = jnp.broadcast_to(block[5:6], (8, 128))
        left = jnp.where(
            row < 3, -2.0 * block, jnp.where(row == 5, 1.0, jnp.where(row == 6, norm, 0.0))
        )
        a1, a2, a3 = parts_of(left)
        stack = jnp.concatenate([a1, a1, a1, a2, a2, a3, last], axis=0)
        left_ref[g] = stack.T.astype(jnp.bfloat16)


def column_of(row):
    return jnp.broadcast_to(row, (128, 128)).T


def squares(left_ref, right_ref, g, w, depth):
    return jnp.dot(
        left_ref[g, :, :depth], right_ref[w, :depth, :], preferred_element_type=jnp.float32
    )


def run_list(count, entry_of, buffers, produce, consume):
    unroll = len(buffers)

    def fetch(base):
        for u, buffer in enumerate(buffers):
            w, slot = entry_of(base + u)
            buffer[...] = produce(w, jnp.minimum(slot, TILES - 1))

    fetch(0)

    @pl.loop(0, (count + unroll - 1) // unroll)
    def _(step):
        base = step * unroll
        for u, buffer in enumerate(buffers):
            w, slot = entry_of(base + u)
            consume(w, slot, buffer)
        fetch(base + unroll)


def own_entry(index):
    return 2 * TILES + jnp.minimum(index, TILES - 1), index


def pad_list(list_ref, count):
    for u in range(2 * UNROLL):
        list_ref[count + u] = 2 * TILES * 32 + TILES


def entry_in(list_ref):
    def entry_of(index):
        entry = list_ref[index]
        return (entry >> 5) & 127, entry & 31

    return entry_of


def plan_of(index_ref, least, sources, own_ref, plan_ref):
    lane = rows_of((1, 128), 1)
    low = jnp.zeros((1, 128), jnp.float32)
    high = jnp.zeros((1, 128), jnp.float32)
    top = jnp.zeros((1, 128), jnp.float32)
    tile = index_ref[0:1, :]
    here = jnp.zeros((1, 128), jnp.int32)
    for place, read in sources:
        ranges = read(80, 8)
        low = jnp.where(lane >> 4 == place, ranges[0:1], low)
        high = jnp.where(lane >> 4 == place, ranges[1:2], high)
        top = jnp.maximum(top, ranges[2:3])
        here = jnp.where(tile >> 4 == place, 1, here)
    used = (lane >> 4 > 0) & (lane >> 4 < index_ref[1:2, :]) & (here > 0)

    def picked(row):
        wide = jnp.take_along_axis(
            jnp.broadcast_to(row, (8, 128)),
            jnp.broadcast_to(tile, (8, 128)),
            axis=1,
            mode="promise_in_bounds",
        )
        return wide[0:1]

    gap = jnp.maximum(picked(low) - own_ref[81:82, :], own_ref[80:81, :] - picked(high))
    kind = jnp.where(used, jnp.where(gap >= FAR_GAP, 1 << 17, 1 << 16), 0)
    within = jnp.where(top - 0.99 >= least, 1, 0)
    row = rows_of((8, 128))
    plan = jnp.broadcast_to(tile * 32 + (lane & 15) + kind, (8, 128))
    plan_ref[...] = jnp.where(row == 0, plan, jnp.broadcast_to(within, (8, 128)))


def near_term(soft, scaled, offset, inside):
    inverse = lax.rsqrt(soft)
    distance = soft * inverse
    upper = distance + scaled
    gap = distance - scaled
    lower = jnp.minimum(jnp.maximum(offset, jnp.abs(gap)), upper)
    ratio = 1.0 / (lower * upper)
    difference = (upper - lower) * ratio
    total = (upper + lower) * ratio
    weight = gap * upper * inverse
    logs = jnp.log(lower * lower * ratio)
    term = difference * (4.0 - weight * total) + (inverse + inverse) * logs
    if inside:
        term += jnp.where(offset < -gap, 16.0 * (1.0 / offset - 1.0 / lower), 0.0)
    return term


def split_lists(steps_ref, near_ref, far_ref):
    near = jnp.int32(0)
    far = jnp.int32(0)
    for g in range(TILES):
        for k in range(1, 8):
            entry = steps_ref[0, TILES * k + g]
            near_ref[near] = entry
            far_ref[far] = entry
            near = near + ((entry >> 16) & 1)
            far = far + (entry >> 17)
    pad_list(near_ref, near)
    pad_list(far_ref, far)
    return near, far


def sum_pairs(left_ref, right_ref, blocks_ref, offsets_ref, acc_ref, buffers, lists, counts, within, own):
    def produce(w, g):
        return squares(left_ref, right_ref, g, w, 64)

    def consume_near(inside, diagonal):
        def consume(w, slot, buffer):
            scaled = blocks_ref[w, 3:4, :]
            for v in range(8):
                rows = slice(16 * v, 16 * v + 16)
                c = jnp.broadcast_to(scaled, (16, 128))
                if diagonal:
                    same = rows_of((16, 128)) + 16 * v == rows_of((16, 128), 1)
                    c = jnp.where(same, 0.0, c)
                term = near_term(buffer[rows, :], c, offsets_ref[slot, rows, :], inside)
                if diagonal:
                    acc_ref[slot, rows, :] = term
                else:
                    acc_ref[slot, rows, :] += term

        return consume

    def consume_far(w, slot, buffer):
        scaled = blocks_ref[w, 3:4, :]
        for v in range(8):
            rows = slice(16 * v, 16 * v + 16)
            soft = buffer[rows, :]
            inverse = lax.rsqrt(soft)
            gap = soft * inverse - scaled
            ratio = 1.0 / (soft - scaled * scaled)
            logs = jnp.log(gap * gap * ratio)
            acc_ref[slot, rows, :] += (4.0 * scaled) * ratio + (inverse + inverse) * logs

    def near_lists(inside):
        if own:
            run_list(TILES, own_entry, buffers[:4], produce, consume_near(inside, True))
        run_list(counts[0], entry_in(lists[0]), buffers[:4], produce, consume_near(inside, False))

    pl.when(within == 0)(lambda: near_lists(False))
    pl.when(within != 0)(lambda: near_lists(True))
    run_list(counts[1], entry_in(lists[1]), buffers, produce, consume_far)


def least_of(offset):
    return jnp.min(jnp.min(offset, axis=0, keepdims=True), axis=1, keepdims=True)


def born_own_kernel(
    slab_ref, index_ref, own_ref, other_ref, radii_ref,
    blocks_ref, left_ref, right_ref, offsets_ref, acc_ref, plan_ref,
    near_ref, far_ref, steps_ref, sem, *buffers,
):
    offset = radii_ref[...] - OFFSET
    sources = ((2, rows_in(own_ref)), (inner_slot(slab_ref[0]), rows_in(other_ref)))
    plan_of(index_ref, least_of(offset), sources, own_ref, plan_ref)
    copy = pltpu.make_async_copy(plan_ref, steps_ref, sem)
    copy.start()
    centre = (8 * slab_ref[0] + 4).astype(jnp.float32)
    for place, read in sources:
        fill_blocks(blocks_ref, read, place * TILES, centre)
        fill_right(right_ref, blocks_ref, place * TILES)
    copy.wait()
    counts = split_lists(steps_ref, near_ref, far_ref)
    fill_left(left_ref, blocks_ref)
    for g in range(TILES):
        offsets_ref[g] = column_of(offset[g : g + 1])
    offsets_ref[TILES] = offsets_ref[0]
    sum_pairs(
        left_ref, right_ref, blocks_ref, offsets_ref, acc_ref, buffers,
        (near_ref, far_ref), counts, steps_ref[1, 0], True,
    )


def born_rest_kernel(
    slab_ref, fill_ref, index_ref, own_ref, even_ref, odd_ref, radii_ref,
    left_ref, offsets_ref, blocks_in, right_in, acc_in,
    plan_ref, born_ref, send_ref, blocks_ref, right_ref, acc_ref,
    near_ref, far_ref, steps_ref, sem, sums_ref, *buffers,
):
    slab = slab_ref[0]
    sources = outer_slabs(slab, even_ref, odd_ref, ROWS)
    offset = radii_ref[...] - OFFSET
    plan_of(index_ref, least_of(offset), sources, own_ref, plan_ref)
    copy = pltpu.make_async_copy(plan_ref, steps_ref, sem)
    copy.start()
    centre = (8 * slab + 4).astype(jnp.float32)
    for i, (place, read) in enumerate(sources):
        if i == 1:
            copy.wait()
            counts = split_lists(steps_ref, near_ref, far_ref)
        fill_blocks(blocks_ref, read, place * TILES, centre)
        fill_right(right_ref, blocks_ref, place * TILES)
    sum_pairs(
        left_ref, right_ref, blocks_ref, offsets_ref, acc_ref, buffers,
        (near_ref, far_ref), counts, steps_ref[1, 0], False,
    )
    for g in range(TILES):
        sums_ref[g : g + 1, :] = jnp.sum(acc_ref[g].T, axis=0, keepdims=True)
    slot = rows_of((TILES, 128)) * 128 + rows_of((TILES, 128), 1)
    live = slot < fill_ref[0]
    radius = jnp.where(live, radii_ref[...], 1.5)
    inner = radius - OFFSET
    psi = 0.125 * sums_ref[...] * inner
    bending = jnp.tanh(psi - 0.8 * psi * psi + 4.85 * psi * psi * psi)
    born = 1.0 / (1.0 / inner - bending / radius)
    born_ref[...] = jnp.where(live, born, 0.0)
    send_ref[...] = jnp.where(live, born, 1.0)


def energy_list(steps_ref, list_ref):
    count = jnp.int32(0)
    for g in range(TILES):
        for k in range(1, 8):
            entry = steps_ref[0, TILES * k + g]
            list_ref[count] = entry
            count = count + jnp.minimum(entry >> 16, 1)
    pad_list(list_ref, count)
    return count


def sum_energy(left_ref, right_ref, blocks_ref, born_ref, column_ref, inverse_ref, acc_ref, buffers, entries, count, first):
    def produce(w, g):
        return squares(left_ref, right_ref, g, w, 48)

    def consume(w, slot, buffer):
        charge = blocks_ref[w, 4:5, :]
        partner = born_ref[pl.ds(w, 1), :]
        backward = 1.0 / partner
        for v in range(8):
            rows = slice(16 * v, 16 * v + 16)
            squared = buffer[rows, :]
            product = column_ref[slot, rows, :] * partner
            decay = jnp.exp2(squared * (inverse_ref[slot, rows, :] * backward))
            term = charge * lax.rsqrt(squared + product * decay)
            if first:
                acc_ref[slot, rows, :] = term
            else:
                acc_ref[slot, rows, :] += term

    run_list(count, entries, buffers, produce, consume)


def energy_own_kernel(
    slab_ref, plan_ref, blocks_ref, left_ref, right_ref, own_ref, other_ref,
    column_ref, inverse_ref, acc_ref,
    list_ref, steps_ref, born_ref, sem, *buffers,
):
    copy = pltpu.make_async_copy(plan_ref, steps_ref, sem)
    copy.start()
    born_ref[2 * TILES : 3 * TILES, :] = own_ref[...]
    born_ref[pl.ds(inner_slot(slab_ref[0]) * TILES, TILES), :] = other_ref[...]
    for g in range(TILES):
        if g == 6:
            copy.wait()
            count = energy_list(steps_ref, list_ref)
        column = column_of(own_ref[g : g + 1, :])
        column_ref[g] = column
        inverse_ref[g] = (-0.25 * LOG2E) / column
    column_ref[TILES] = column_ref[0]
    inverse_ref[TILES] = inverse_ref[0]
    shared = (left_ref, right_ref, blocks_ref, born_ref, column_ref, inverse_ref, acc_ref)
    sum_energy(*shared, buffers, own_entry, TILES, True)
    sum_energy(*shared, buffers, entry_in(list_ref), count, False)


def energy_rest_kernel(
    slab_ref, plan_ref, blocks_ref, left_ref, right_ref, even_ref, odd_ref,
    column_ref, inverse_ref, acc_in,
    energy_ref, share_ref, acc_ref,
    list_ref, steps_ref, born_ref, sem, charge_ref, *buffers,
):
    copy = pltpu.make_async_copy(plan_ref, steps_ref, sem)
    copy.start()
    for place, read in outer_slabs(slab_ref[0], even_ref, odd_ref, TILES):
        born_ref[pl.ds(place * TILES, TILES), :] = read(0, TILES)
    born_ref[2 * TILES : 3 * TILES, :] = jnp.ones((TILES, 128), jnp.float32)
    for g in range(TILES):
        charge_ref[g : g + 1, :] = blocks_ref[2 * TILES + g, 4:5, :]
    copy.wait()
    count = energy_list(steps_ref, list_ref)
    sum_energy(
        left_ref, right_ref, blocks_ref, born_ref, column_ref, inverse_ref, acc_ref, buffers,
        entry_in(list_ref), count, False,
    )
    for g in range(TILES):
        energy_ref[g : g + 1, :] = jnp.sum(acc_ref[g].T, axis=0, keepdims=True)
    energy = -0.5 * charge_ref[...] * energy_ref[...]
    energy_ref[...] = energy
    share = jnp.sum(jnp.sum(energy, axis=0, keepdims=True), axis=1, keepdims=True)
    share_ref[...] = jnp.broadcast_to(share[None], share_ref.shape)


def total_kernel(shares_ref, total_ref):
    total = shares_ref[0]
    for i in range(1, shares_ref.shape[0]):
        total = total + shares_ref[i]
    total_ref[0] = total[0, 0]


def shards(coords, charges, radii, screens, tile_lists, tile_counts, slab_fill):
    f32 = jnp.float32
    count = lax.axis_size(SLAB)
    smem = pl.BlockSpec(memory_space=pltpu.SMEM)
    vmem = pl.BlockSpec(memory_space=pltpu.VMEM)

    def near(*values):
        return tuple(pltpu.with_memory_space_constraint(value, pltpu.VMEM) for value in values)

    def call(kernel, name, outs, scalars, arrays, scratch, aliases=None, out_specs=None, flops=0):
        return pl.pallas_call(
            kernel,
            out_shape=outs,
            in_specs=[smem] * len(scalars) + [vmem] * len(arrays),
            out_specs=out_specs or (vmem,) * len(outs),
            scratch_shapes=scratch,
            input_output_aliases=aliases or {},
            cost_estimate=pl.CostEstimate(flops=flops, transcendentals=0, bytes_accessed=0),
            compiler_params=pltpu.CompilerParams(vmem_limit_bytes=20 << 20),
            name=name,
        )(*scalars, *arrays)

    stack = pltpu.VMEM((TILES + 1, 128, 128), f32)
    blocks_type = pltpu.VMEM((5 * TILES, 8, 128), f32)
    right_type = pltpu.VMEM((5 * TILES, 64, 128), jnp.bfloat16)
    left_type = pltpu.VMEM((TILES, 128, 64), jnp.bfloat16)
    plan_type = pltpu.VMEM((8, 128), jnp.int32)
    slab_type = pltpu.VMEM((TILES, 128), f32)
    entries = pltpu.SMEM((144,), jnp.int32)
    steps = pltpu.SMEM((8, 128), jnp.int32)
    squares = [pltpu.VMEM((128, 128), f32)] * 8
    sem = pltpu.SemaphoreType.DMA

    slab = lax.axis_index(SLAB).astype(jnp.int32)[None]
    charges, radii, screens = (v.reshape(TILES, 128) for v in (charges, radii, screens))
    lists, counts = tile_lists.T, tile_counts.reshape(1, TILES)
    coords, charges, radii, screens, lists, counts = (
        pltpu.with_memory_space_constraint(value, pltpu.HBM)
        for value in (coords, charges, radii, screens, lists, counts)
    )
    packed, index, kept = call(
        prep_kernel, "prep", (pltpu.VMEM((ROWS, 128), f32), plan_type, slab_type),
        (slab, slab_fill), (coords, charges, radii, screens, lists, counts), [],
    )
    other, even, odd = neighbours(packed)
    packed, other, even, odd, index, kept = near(packed, other, even, odd, index, kept)
    blocks, left, right, offsets, acc, own_plan = call(
        born_own_kernel, "born_own",
        (blocks_type, left_type, right_type, stack, stack, plan_type),
        (slab,), (index, packed, other, kept),
        [entries, entries, steps, sem] + squares, flops=1 << 27,
    )
    plan, born, send, blocks, right, acc = call(
        born_rest_kernel, "born_rest",
        (plan_type, slab_type, slab_type, blocks_type, right_type, stack),
        (slab, slab_fill),
        (index, packed, even, odd, kept, *near(left, offsets, blocks, right, acc)),
        [entries, entries, steps, sem, slab_type] + squares,
        aliases={9: 3, 10: 4, 11: 5},
    )
    born_other, born_even, born_odd = neighbours(send)
    column, inverse, acc = call(
        energy_own_kernel, "energy_own", (stack,) * 3,
        (slab,), near(own_plan, blocks, left, right, send, born_other),
        [entries, steps, pltpu.VMEM((5 * TILES, 128), f32), sem] + squares, flops=1 << 27,
    )
    energy, share, acc = call(
        energy_rest_kernel, "energy_rest",
        (slab_type, pltpu.VMEM((count, 1, 128), f32), stack),
        (slab,), near(plan, blocks, left, right, born_even, born_odd, column, inverse, acc),
        [entries, steps, pltpu.VMEM((5 * TILES, 128), f32), sem, slab_type] + squares,
        aliases={9: 2},
    )
    shares = lax.all_to_all(share, SLAB, 0, 0, tiled=True)
    (total,) = call(
        total_kernel, "total", (jax.ShapeDtypeStruct((1,), f32),), (), near(shares), [], out_specs=(smem,)
    )
    return (born.reshape(-1), energy.reshape(-1), total[0])


def solution(mesh):
    torus = Mesh(mesh.devices.reshape(4, 8, 4, 2), SLAB)
    placed = (P(None, SLAB), P(SLAB), P(SLAB), P(SLAB), P(SLAB, None), P(SLAB), P(SLAB))
    return jax.shard_map(
        shards, mesh=torus, in_specs=placed, out_specs=(P(SLAB), P(SLAB), P()), check_vma=False
    )
```

```python
import jax
import jax.numpy as jnp
from jax import lax
from jax.experimental import pallas as pl
from jax.experimental.pallas import tpu as pltpu
from jax.sharding import Mesh
from jax.sharding import PartitionSpec as P

SLAB = ("slab_0", "slab_1", "slab_2", "slab_3")
OFFSET = 0.09
LOG2E = 1.4426950408889634
TILES = 16
UNROLL = 8
FAR_GAP = 3.5
ROWS = 88


def chip_swap(count, odd):
    pairs = []
    for chip in range(count // 2):
        other = ((chip + odd) ^ 1) - odd
        for core in (0, 1):
            if 0 <= other < count // 2:
                pairs.append((2 * chip + core, 2 * other + core))
            else:
                pairs.append((2 * chip + core, 2 * chip + 1 - core))
    return pairs


def neighbours(value):
    count = lax.axis_size(SLAB)
    other = lax.ppermute(value, SLAB, [(i, i ^ 1) for i in range(count)])
    both = jnp.concatenate([value, other], axis=0)
    return [other] + [lax.ppermute(both, SLAB, chip_swap(count, odd)) for odd in (0, 1)]


def rows_in(ref):
    return lambda start, size: ref[pl.ds(start, size), :]


def inner_slot(slab):
    return jnp.where(slab % 2 == 0, 3, 1)


def outer_slabs(slab, even, odd, height):
    ahead = (slab // 2) % 2 == 0
    far = jnp.where(ahead, 4, 0)
    from_even = ahead == (slab % 2 == 1)

    def crossed(start, size):
        rows = pl.ds(height + start, size)
        return jnp.where(from_even, even[rows, :], odd[rows, :])

    return ((4 - inner_slot(slab), crossed), (far, rows_in(even)), (4 - far, rows_in(odd)))


def rows_of(shape, axis=0):
    return lax.broadcasted_iota(jnp.int32, shape, axis)


def prep_kernel(
    slab_ref, fill_ref, coords_ref, charges_ref, radii_ref, screens_ref, lists_ref, counts_ref,
    out_ref, index_ref, kept_ref,
):
    index_ref[...] = jnp.zeros((8, 128), jnp.int32)
    for k in range(8):
        lanes = slice(TILES * k, TILES * k + TILES)
        index_ref[0:1, lanes] = lists_ref[k : k + 1, :]
        index_ref[1:2, lanes] = counts_ref[...]
    kept_ref[...] = radii_ref[...]
    fill = fill_ref[0]
    middle = (8 * slab_ref[0] + 4).astype(jnp.float32)
    slot = rows_of((TILES, 128)) * 128 + rows_of((TILES, 128), 1)
    live = slot < fill
    scaled = jnp.where(live, screens_ref[...] * (radii_ref[...] - OFFSET), 0.0)
    charge = jnp.where(live, charges_ref[...], 0.0)
    home = jnp.where(rows_of((3, 128)) == 2, middle, 0.0)
    lane = rows_of((3, 128), 1)
    column = rows_of((1, 128), 1) % TILES
    low = jnp.zeros((1, 128), jnp.float32)
    high = jnp.zeros((1, 128), jnp.float32)
    for t in range(TILES):
        xyz = jnp.where(lane + t * 128 < fill, coords_ref[:, t * 128 : (t + 1) * 128], home)
        out_ref[5 * t : 5 * t + 3, :] = xyz
        out_ref[5 * t + 3 : 5 * t + 4, :] = scaled[t : t + 1]
        out_ref[5 * t + 4 : 5 * t + 5, :] = charge[t : t + 1]
        low = jnp.where(column == t, jnp.min(xyz[2:3], axis=1, keepdims=True), low)
        high = jnp.where(column == t, jnp.max(xyz[2:3], axis=1, keepdims=True), high)
    top = jnp.max(jnp.max(scaled, axis=0, keepdims=True), axis=1, keepdims=True)
    out_ref[80:81, :] = low
    out_ref[81:82, :] = high
    out_ref[82:83, :] = jnp.broadcast_to(top, (1, 128))
    out_ref[83:88, :] = jnp.zeros((5, 128), jnp.float32)


def parts_of(rows):
    first = rows.astype(jnp.bfloat16).astype(jnp.float32)
    rest = rows - first
    second = rest.astype(jnp.bfloat16).astype(jnp.float32)
    third = (rest - second).astype(jnp.bfloat16).astype(jnp.float32)
    return first, second, third


def fill_blocks(blocks_ref, read, base, centre):
    row = rows_of((8, 128))
    shift = jnp.where(row == 2, centre, 0.0)
    tail = jnp.where(row == 6, 1.0, 0.0)
    for t in range(TILES):
        block = read(5 * t, 8) - shift
        square = block * block
        norm = square[0:1] + square[1:2] + square[2:3]
        blocks_ref[base + t] = jnp.where(row < 5, block, jnp.where(row == 5, norm, tail))


def fill_right(right_ref, blocks_ref, base):
    last = jnp.where(rows_of((16, 128)) == 0, 1.0, 0.0)
    for t in range(TILES):
        b1, b2, b3 = parts_of(blocks_ref[base + t])
        stack = jnp.concatenate([b1, b2, b3, b1, b2, b1, last], axis=0)
        right_ref[base + t] = stack.astype(jnp.bfloat16)


def fill_left(left_ref, blocks_ref):
    row = rows_of((8, 128))
    last = jnp.where(rows_of((16, 128)) == 0, 1.0, 0.0)
    for g in range(TILES):
        block = blocks_ref[2 * TILES + g]
        norm = jnp.broadcast_to(block[5:6], (8, 128))
        left = jnp.where(
            row < 3, -2.0 * block, jnp.where(row == 5, 1.0, jnp.where(row == 6, norm, 0.0))
        )
        a1, a2, a3 = parts_of(left)
        stack = jnp.concatenate([a1, a1, a1, a2, a2, a3, last], axis=0)
        left_ref[g] = stack.T.astype(jnp.bfloat16)


def column_of(row):
    return jnp.broadcast_to(row, (128, 128)).T


def squares(left_ref, right_ref, g, w, depth):
    return jnp.dot(
        left_ref[g, :, :depth], right_ref[w, :depth, :], preferred_element_type=jnp.float32
    )


def run_list(count, entry_of, buffers, produce, consume):
    unroll = len(buffers)

    def fetch(base):
        for u, buffer in enumerate(buffers):
            w, slot = entry_of(base + u)
            buffer[...] = produce(w, jnp.minimum(slot, TILES - 1))

    fetch(0)

    @pl.loop(0, (count + unroll - 1) // unroll)
    def _(step):
        base = step * unroll
        for u, buffer in enumerate(buffers):
            w, slot = entry_of(base + u)
            consume(w, slot, buffer)
        fetch(base + unroll)


def own_entry(index):
    return 2 * TILES + jnp.minimum(index, TILES - 1), index


def pad_list(list_ref, count):
    for u in range(2 * UNROLL):
        list_ref[count + u] = 2 * TILES * 32 + TILES


def entry_in(list_ref):
    def entry_of(index):
        entry = list_ref[index]
        return (entry >> 5) & 127, entry & 31

    return entry_of


def plan_of(index_ref, least, sources, own_ref, plan_ref):
    lane = rows_of((1, 128), 1)
    low = jnp.zeros((1, 128), jnp.float32)
    high = jnp.zeros((1, 128), jnp.float32)
    top = jnp.zeros((1, 128), jnp.float32)
    tile = index_ref[0:1, :]
    here = jnp.zeros((1, 128), jnp.int32)
    for place, read in sources:
        ranges = read(80, 8)
        low = jnp.where(lane >> 4 == place, ranges[0:1], low)
        high = jnp.where(lane >> 4 == place, ranges[1:2], high)
        top = jnp.maximum(top, ranges[2:3])
        here = jnp.where(tile >> 4 == place, 1, here)
    used = (lane >> 4 > 0) & (lane >> 4 < index_ref[1:2, :]) & (here > 0)

    def picked(row):
        wide = jnp.take_along_axis(
            jnp.broadcast_to(row, (8, 128)),
            jnp.broadcast_to(tile, (8, 128)),
            axis=1,
            mode="promise_in_bounds",
        )
        return wide[0:1]

    gap = jnp.maximum(picked(low) - own_ref[81:82, :], own_ref[80:81, :] - picked(high))
    kind = jnp.where(used, jnp.where(gap >= FAR_GAP, 1 << 17, 1 << 16), 0)
    within = jnp.where(top - 0.99 >= least, 1, 0)
    row = rows_of((8, 128))
    plan = jnp.broadcast_to(tile * 32 + (lane & 15) + kind, (8, 128))
    plan_ref[...] = jnp.where(row == 0, plan, jnp.broadcast_to(within, (8, 128)))


def near_term(soft, scaled, offset, inside):
    inverse = lax.rsqrt(soft)
    distance = soft * inverse
    upper = distance + scaled
    gap = distance - scaled
    lower = jnp.minimum(jnp.maximum(offset, jnp.abs(gap)), upper)
    ratio = 1.0 / (lower * upper)
    difference = (upper - lower) * ratio
    total = (upper + lower) * ratio
    weight = gap * upper * inverse
    logs = jnp.log(lower * lower * ratio)
    term = difference * (4.0 - weight * total) + (inverse + inverse) * logs
    if inside:
        term += jnp.where(offset < -gap, 16.0 * (1.0 / offset - 1.0 / lower), 0.0)
    return term


def split_lists(steps_ref, near_ref, far_ref):
    near = jnp.int32(0)
    far = jnp.int32(0)
    for g in range(TILES):
        for k in range(1, 8):
            entry = steps_ref[0, TILES * k + g]
            near_ref[near] = entry
            far_ref[far] = entry
            near = near + ((entry >> 16) & 1)
            far = far + (entry >> 17)
    pad_list(near_ref, near)
    pad_list(far_ref, far)
    return near, far


def sum_pairs(left_ref, right_ref, blocks_ref, offsets_ref, acc_ref, buffers, lists, counts, within, own):
    def produce(w, g):
        return squares(left_ref, right_ref, g, w, 64)

    def consume_near(inside, diagonal):
        def consume(w, slot, buffer):
            scaled = blocks_ref[w, 3:4, :]
            for v in range(8):
                rows = slice(16 * v, 16 * v + 16)
                c = jnp.broadcast_to(scaled, (16, 128))
                if diagonal:
                    same = rows_of((16, 128)) + 16 * v == rows_of((16, 128), 1)
                    c = jnp.where(same, 0.0, c)
                term = near_term(buffer[rows, :], c, offsets_ref[slot, rows, :], inside)
                if diagonal:
                    acc_ref[slot, rows, :] = term
                else:
                    acc_ref[slot, rows, :] += term

        return consume

    def consume_far(w, slot, buffer):
        scaled = blocks_ref[w, 3:4, :]
        for v in range(8):
            rows = slice(16 * v, 16 * v + 16)
            soft = buffer[rows, :]
            inverse = lax.rsqrt(soft)
            gap = soft * inverse - scaled
            ratio = 1.0 / (soft - scaled * scaled)
            logs = jnp.log(gap * gap * ratio)
            acc_ref[slot, rows, :] += (4.0 * scaled) * ratio + (inverse + inverse) * logs

    def near_lists(inside):
        if own:
            run_list(TILES, own_entry, buffers[:4], produce, consume_near(inside, True))
        run_list(counts[0], entry_in(lists[0]), buffers[:4], produce, consume_near(inside, False))

    pl.when(within == 0)(lambda: near_lists(False))
    pl.when(within != 0)(lambda: near_lists(True))
    run_list(counts[1], entry_in(lists[1]), buffers, produce, consume_far)


def least_of(offset):
    return jnp.min(jnp.min(offset, axis=0, keepdims=True), axis=1, keepdims=True)


def born_own_kernel(
    slab_ref, index_ref, own_ref, other_ref, radii_ref,
    blocks_ref, left_ref, right_ref, offsets_ref, acc_ref, plan_ref,
    near_ref, far_ref, steps_ref, sem, *buffers,
):
    offset = radii_ref[...] - OFFSET
    sources = ((2, rows_in(own_ref)), (inner_slot(slab_ref[0]), rows_in(other_ref)))
    plan_of(index_ref, least_of(offset), sources, own_ref, plan_ref)
    copy = pltpu.make_async_copy(plan_ref, steps_ref, sem)
    copy.start()
    centre = (8 * slab_ref[0] + 4).astype(jnp.float32)
    for place, read in sources:
        fill_blocks(blocks_ref, read, place * TILES, centre)
        fill_right(right_ref, blocks_ref, place * TILES)
    copy.wait()
    counts = split_lists(steps_ref, near_ref, far_ref)
    fill_left(left_ref, blocks_ref)
    for g in range(TILES):
        offsets_ref[g] = column_of(offset[g : g + 1])
    offsets_ref[TILES] = offsets_ref[0]
    sum_pairs(
        left_ref, right_ref, blocks_ref, offsets_ref, acc_ref, buffers,
        (near_ref, far_ref), counts, steps_ref[1, 0], True,
    )


def born_rest_kernel(
    slab_ref, fill_ref, index_ref, own_ref, even_ref, odd_ref, radii_ref,
    left_ref, offsets_ref, blocks_in, right_in, acc_in,
    plan_ref, born_ref, send_ref, blocks_ref, right_ref, acc_ref,
    near_ref, far_ref, steps_ref, sem, sums_ref, *buffers,
):
    slab = slab_ref[0]
    sources = outer_slabs(slab, even_ref, odd_ref, ROWS)
    offset = radii_ref[...] - OFFSET
    plan_of(index_ref, least_of(offset), sources, own_ref, plan_ref)
    copy = pltpu.make_async_copy(plan_ref, steps_ref, sem)
    copy.start()
    centre = (8 * slab + 4).astype(jnp.float32)
    for i, (place, read) in enumerate(sources):
        if i == 1:
            copy.wait()
            counts = split_lists(steps_ref, near_ref, far_ref)
        fill_blocks(blocks_ref, read, place * TILES, centre)
        fill_right(right_ref, blocks_ref, place * TILES)
    sum_pairs(
        left_ref, right_ref, blocks_ref, offsets_ref, acc_ref, buffers,
        (near_ref, far_ref), counts, steps_ref[1, 0], False,
    )
    for g in range(TILES):
        sums_ref[g : g + 1, :] = jnp.sum(acc_ref[g].T, axis=0, keepdims=True)
    slot = rows_of((TILES, 128)) * 128 + rows_of((TILES, 128), 1)
    live = slot < fill_ref[0]
    radius = jnp.where(live, radii_ref[...], 1.5)
    inner = radius - OFFSET
    psi = 0.125 * sums_ref[...] * inner
    bending = jnp.tanh(psi - 0.8 * psi * psi + 4.85 * psi * psi * psi)
    born = 1.0 / (1.0 / inner - bending / radius)
    born_ref[...] = jnp.where(live, born, 0.0)
    send_ref[...] = jnp.where(live, born, 1.0)


def energy_list(steps_ref, list_ref):
    count = jnp.int32(0)
    for g in range(TILES):
        for k in range(1, 8):
            entry = steps_ref[0, TILES * k + g]
            list_ref[count] = entry
            count = count + jnp.minimum(entry >> 16, 1)
    pad_list(list_ref, count)
    return count


def sum_energy(left_ref, right_ref, blocks_ref, born_ref, column_ref, inverse_ref, acc_ref, buffers, entries, count, first):
    def produce(w, g):
        return squares(left_ref, right_ref, g, w, 48)

    def consume(w, slot, buffer):
        charge = blocks_ref[w, 4:5, :]
        partner = born_ref[pl.ds(w, 1), :]
        backward = 1.0 / partner
        for v in range(8):
            rows = slice(16 * v, 16 * v + 16)
            squared = buffer[rows, :]
            product = column_ref[slot, rows, :] * partner
            decay = jnp.exp2(squared * (inverse_ref[slot, rows, :] * backward))
            term = charge * lax.rsqrt(squared + product * decay)
            if first:
                acc_ref[slot, rows, :] = term
            else:
                acc_ref[slot, rows, :] += term

    run_list(count, entries, buffers, produce, consume)


def energy_own_kernel(
    slab_ref, plan_ref, blocks_ref, left_ref, right_ref, own_ref, other_ref, radii_ref,
    column_ref, inverse_ref, acc_ref, result_ref,
    list_ref, steps_ref, born_ref, sem, result_sem, *buffers,
):
    result = pltpu.make_async_copy(radii_ref, result_ref, result_sem)
    result.start()
    copy = pltpu.make_async_copy(plan_ref, steps_ref, sem)
    copy.start()
    born_ref[2 * TILES : 3 * TILES, :] = own_ref[...]
    born_ref[pl.ds(inner_slot(slab_ref[0]) * TILES, TILES), :] = other_ref[...]
    for g in range(TILES):
        if g == 6:
            copy.wait()
            count = energy_list(steps_ref, list_ref)
        column = column_of(own_ref[g : g + 1, :])
        column_ref[g] = column
        inverse_ref[g] = (-0.25 * LOG2E) / column
    column_ref[TILES] = column_ref[0]
    inverse_ref[TILES] = inverse_ref[0]
    shared = (left_ref, right_ref, blocks_ref, born_ref, column_ref, inverse_ref, acc_ref)
    sum_energy(*shared, buffers, own_entry, TILES, True)
    sum_energy(*shared, buffers, entry_in(list_ref), count, False)
    result.wait()


def energy_rest_kernel(
    slab_ref, plan_ref, blocks_ref, left_ref, right_ref, even_ref, odd_ref,
    column_ref, inverse_ref, acc_in,
    energy_ref, share_ref, acc_ref,
    list_ref, steps_ref, born_ref, sem, charge_ref, *buffers,
):
    copy = pltpu.make_async_copy(plan_ref, steps_ref, sem)
    copy.start()
    for place, read in outer_slabs(slab_ref[0], even_ref, odd_ref, TILES):
        born_ref[pl.ds(place * TILES, TILES), :] = read(0, TILES)
    born_ref[2 * TILES : 3 * TILES, :] = jnp.ones((TILES, 128), jnp.float32)
    for g in range(TILES):
        charge_ref[g : g + 1, :] = blocks_ref[2 * TILES + g, 4:5, :]
    copy.wait()
    count = energy_list(steps_ref, list_ref)
    sum_energy(
        left_ref, right_ref, blocks_ref, born_ref, column_ref, inverse_ref, acc_ref, buffers,
        entry_in(list_ref), count, False,
    )
    for g in range(TILES):
        energy_ref[g : g + 1, :] = jnp.sum(acc_ref[g].T, axis=0, keepdims=True)
    energy = -0.5 * charge_ref[...] * energy_ref[...]
    energy_ref[...] = energy
    share = jnp.sum(jnp.sum(energy, axis=0, keepdims=True), axis=1, keepdims=True)
    share_ref[...] = jnp.broadcast_to(share[None], share_ref.shape)


def total_kernel(shares_ref, energy_ref, total_ref, result_ref, sem):
    result = pltpu.make_async_copy(energy_ref, result_ref, sem)
    result.start()
    total = shares_ref[0]
    for i in range(1, shares_ref.shape[0]):
        total = total + shares_ref[i]
    total_ref[0] = total[0, 0]
    result.wait()


def shards(coords, charges, radii, screens, tile_lists, tile_counts, slab_fill):
    f32 = jnp.float32
    count = lax.axis_size(SLAB)
    smem = pl.BlockSpec(memory_space=pltpu.SMEM)
    vmem = pl.BlockSpec(memory_space=pltpu.VMEM)

    def near(*values):
        return tuple(pltpu.with_memory_space_constraint(value, pltpu.VMEM) for value in values)

    def call(kernel, name, outs, scalars, arrays, scratch, aliases=None, out_specs=None, flops=0):
        return pl.pallas_call(
            kernel,
            out_shape=outs,
            in_specs=[smem] * len(scalars) + [vmem] * len(arrays),
            out_specs=out_specs or (vmem,) * len(outs),
            scratch_shapes=scratch,
            input_output_aliases=aliases or {},
            cost_estimate=pl.CostEstimate(flops=flops, transcendentals=0, bytes_accessed=0),
            compiler_params=pltpu.CompilerParams(vmem_limit_bytes=20 << 20),
            name=name,
        )(*scalars, *arrays)

    stack = pltpu.VMEM((TILES + 1, 128, 128), f32)
    blocks_type = pltpu.VMEM((5 * TILES, 8, 128), f32)
    right_type = pltpu.VMEM((5 * TILES, 64, 128), jnp.bfloat16)
    left_type = pltpu.VMEM((TILES, 128, 64), jnp.bfloat16)
    plan_type = pltpu.VMEM((8, 128), jnp.int32)
    slab_type = pltpu.VMEM((TILES, 128), f32)
    result_type = pltpu.HBM((TILES, 128), f32)
    hbm = pl.BlockSpec(memory_space=pltpu.HBM)
    entries = pltpu.SMEM((144,), jnp.int32)
    steps = pltpu.SMEM((8, 128), jnp.int32)
    squares = [pltpu.VMEM((128, 128), f32)] * 8
    sem = pltpu.SemaphoreType.DMA

    slab = lax.axis_index(SLAB).astype(jnp.int32)[None]
    charges, radii, screens = (v.reshape(TILES, 128) for v in (charges, radii, screens))
    lists, counts = tile_lists.T, tile_counts.reshape(1, TILES)
    coords, charges, radii, screens, lists, counts = (
        pltpu.with_memory_space_constraint(value, pltpu.HBM)
        for value in (coords, charges, radii, screens, lists, counts)
    )
    packed, index, kept = call(
        prep_kernel, "prep", (pltpu.VMEM((ROWS, 128), f32), plan_type, slab_type),
        (slab, slab_fill), (coords, charges, radii, screens, lists, counts), [],
    )
    other, even, odd = neighbours(packed)
    packed, other, even, odd, index, kept = near(packed, other, even, odd, index, kept)
    blocks, left, right, offsets, acc, own_plan = call(
        born_own_kernel, "born_own",
        (blocks_type, left_type, right_type, stack, stack, plan_type),
        (slab,), (index, packed, other, kept),
        [entries, entries, steps, sem] + squares, flops=1 << 27,
    )
    plan, born, send, blocks, right, acc = call(
        born_rest_kernel, "born_rest",
        (plan_type, slab_type, slab_type, blocks_type, right_type, stack),
        (slab, slab_fill),
        (index, packed, even, odd, kept, *near(left, offsets, blocks, right, acc)),
        [entries, entries, steps, sem, slab_type] + squares,
        aliases={9: 3, 10: 4, 11: 5},
    )
    born_other, born_even, born_odd = neighbours(send)
    column, inverse, acc, born = call(
        energy_own_kernel, "energy_own", (stack, stack, stack, result_type),
        (slab,), near(own_plan, blocks, left, right, send, born_other, born),
        [entries, steps, pltpu.VMEM((5 * TILES, 128), f32), sem, sem] + squares,
        out_specs=(vmem, vmem, vmem, hbm), flops=1 << 27,
    )
    energy, share, acc = call(
        energy_rest_kernel, "energy_rest",
        (slab_type, pltpu.VMEM((count, 1, 128), f32), stack),
        (slab,), near(plan, blocks, left, right, born_even, born_odd, column, inverse, acc),
        [entries, steps, pltpu.VMEM((5 * TILES, 128), f32), sem, slab_type] + squares,
        aliases={9: 2},
    )
    shares = lax.all_to_all(share, SLAB, 0, 0, tiled=True)
    total, energy = call(
        total_kernel, "total", (jax.ShapeDtypeStruct((1,), f32), result_type), (),
        near(shares, energy), [sem], out_specs=(smem, hbm),
    )
    return (born.reshape(-1), energy.reshape(-1), total[0])


def solution(mesh):
    torus = Mesh(mesh.devices.reshape(4, 8, 4, 2), SLAB)
    placed = (P(None, SLAB), P(SLAB), P(SLAB), P(SLAB), P(SLAB, None), P(SLAB), P(SLAB))
    return jax.shard_map(
        shards, mesh=torus, in_specs=placed, out_specs=(P(SLAB), P(SLAB), P()), check_vma=False
    )
```

```python
import jax
import jax.numpy as jnp
from jax import lax
from jax.experimental import pallas as pl
from jax.experimental.pallas import tpu as pltpu
from jax.sharding import Mesh
from jax.sharding import PartitionSpec as P

SLAB = ("slab_0", "slab_1", "slab_2", "slab_3")
OFFSET = 0.09
LOG2E = 1.4426950408889634
TILES = 16
UNROLL = 8
FAR_GAP = 3.5
ROWS = 88


def chip_swap(count, odd):
    pairs = []
    for chip in range(count // 2):
        other = ((chip + odd) ^ 1) - odd
        for core in (0, 1):
            if 0 <= other < count // 2:
                pairs.append((2 * chip + core, 2 * other + core))
            else:
                pairs.append((2 * chip + core, 2 * chip + 1 - core))
    return pairs


def neighbours(value):
    count = lax.axis_size(SLAB)
    other = lax.ppermute(value, SLAB, [(i, i ^ 1) for i in range(count)])
    both = jnp.concatenate([value, other], axis=0)
    return [other] + [lax.ppermute(both, SLAB, chip_swap(count, odd)) for odd in (0, 1)]


def rows_in(ref):
    return lambda start, size: ref[pl.ds(start, size), :]


def inner_slot(slab):
    return jnp.where(slab % 2 == 0, 3, 1)


def outer_slabs(slab, even, odd, height):
    ahead = (slab // 2) % 2 == 0
    far = jnp.where(ahead, 4, 0)
    from_even = ahead == (slab % 2 == 1)

    def crossed(start, size):
        rows = pl.ds(height + start, size)
        return jnp.where(from_even, even[rows, :], odd[rows, :])

    return ((4 - inner_slot(slab), crossed), (far, rows_in(even)), (4 - far, rows_in(odd)))


def rows_of(shape, axis=0):
    return lax.broadcasted_iota(jnp.int32, shape, axis)


def prep_kernel(
    slab_ref, fill_ref, coords_ref, charges_ref, radii_ref, screens_ref, lists_ref, counts_ref,
    out_ref, index_ref, kept_ref,
):
    index_ref[...] = jnp.zeros((8, 128), jnp.int32)
    for k in range(8):
        lanes = slice(TILES * k, TILES * k + TILES)
        index_ref[0:1, lanes] = lists_ref[k : k + 1, :]
        index_ref[1:2, lanes] = counts_ref[...]
    kept_ref[...] = radii_ref[...]
    fill = fill_ref[0]
    middle = (8 * slab_ref[0] + 4).astype(jnp.float32)
    slot = rows_of((TILES, 128)) * 128 + rows_of((TILES, 128), 1)
    live = slot < fill
    scaled = jnp.where(live, screens_ref[...] * (radii_ref[...] - OFFSET), 0.0)
    charge = jnp.where(live, charges_ref[...], 0.0)
    home = jnp.where(rows_of((3, 128)) == 2, middle, 0.0)
    lane = rows_of((3, 128), 1)
    column = rows_of((1, 128), 1) % TILES
    low = jnp.zeros((1, 128), jnp.float32)
    high = jnp.zeros((1, 128), jnp.float32)
    for t in range(TILES):
        xyz = jnp.where(lane + t * 128 < fill, coords_ref[:, t * 128 : (t + 1) * 128], home)
        out_ref[5 * t : 5 * t + 3, :] = xyz
        out_ref[5 * t + 3 : 5 * t + 4, :] = scaled[t : t + 1]
        out_ref[5 * t + 4 : 5 * t + 5, :] = charge[t : t + 1]
        low = jnp.where(column == t, jnp.min(xyz[2:3], axis=1, keepdims=True), low)
        high = jnp.where(column == t, jnp.max(xyz[2:3], axis=1, keepdims=True), high)
    top = jnp.max(jnp.max(scaled, axis=0, keepdims=True), axis=1, keepdims=True)
    out_ref[80:81, :] = low
    out_ref[81:82, :] = high
    out_ref[82:83, :] = jnp.broadcast_to(top, (1, 128))
    out_ref[83:88, :] = jnp.zeros((5, 128), jnp.float32)


def parts_of(rows):
    first = rows.astype(jnp.bfloat16).astype(jnp.float32)
    rest = rows - first
    second = rest.astype(jnp.bfloat16).astype(jnp.float32)
    third = (rest - second).astype(jnp.bfloat16).astype(jnp.float32)
    return first, second, third


def fill_blocks(blocks_ref, read, base, centre):
    row = rows_of((8, 128))
    shift = jnp.where(row == 2, centre, 0.0)
    tail = jnp.where(row == 6, 1.0, 0.0)
    for t in range(TILES):
        block = read(5 * t, 8) - shift
        square = block * block
        norm = square[0:1] + square[1:2] + square[2:3]
        blocks_ref[base + t] = jnp.where(row < 5, block, jnp.where(row == 5, norm, tail))


def fill_right(right_ref, blocks_ref, base):
    last = jnp.where(rows_of((16, 128)) == 0, 1.0, 0.0)
    for t in range(TILES):
        b1, b2, b3 = parts_of(blocks_ref[base + t])
        stack = jnp.concatenate([b1, b2, b3, b1, b2, b1, last], axis=0)
        right_ref[base + t] = stack.astype(jnp.bfloat16)


def fill_left(left_ref, blocks_ref):
    row = rows_of((8, 128))
    last = jnp.where(rows_of((16, 128)) == 0, 1.0, 0.0)
    for g in range(TILES):
        block = blocks_ref[2 * TILES + g]
        norm = jnp.broadcast_to(block[5:6], (8, 128))
        left = jnp.where(
            row < 3, -2.0 * block, jnp.where(row == 5, 1.0, jnp.where(row == 6, norm, 0.0))
        )
        a1, a2, a3 = parts_of(left)
        stack = jnp.concatenate([a1, a1, a1, a2, a2, a3, last], axis=0)
        left_ref[g] = stack.T.astype(jnp.bfloat16)


def column_of(row):
    return jnp.broadcast_to(row, (128, 128)).T


def squares(left_ref, right_ref, g, w, depth):
    return jnp.dot(
        left_ref[g, :, :depth], right_ref[w, :depth, :], preferred_element_type=jnp.float32
    )


def run_list(count, entry_of, buffers, produce, consume):
    unroll = len(buffers)

    def fetch(base):
        for u, buffer in enumerate(buffers):
            w, slot = entry_of(base + u)
            buffer[...] = produce(w, jnp.minimum(slot, TILES - 1))

    fetch(0)

    @pl.loop(0, (count + unroll - 1) // unroll)
    def _(step):
        base = step * unroll
        for u, buffer in enumerate(buffers):
            w, slot = entry_of(base + u)
            consume(w, slot, buffer)
        fetch(base + unroll)


def own_entry(index):
    return 2 * TILES + jnp.minimum(index, TILES - 1), index


def pad_list(list_ref, count):
    for u in range(2 * UNROLL):
        list_ref[count + u] = 2 * TILES * 32 + TILES


def entry_in(list_ref):
    def entry_of(index):
        entry = list_ref[index]
        return (entry >> 5) & 127, entry & 31

    return entry_of


def plan_of(index_ref, least, sources, own_ref, plan_ref):
    lane = rows_of((1, 128), 1)
    low = jnp.zeros((1, 128), jnp.float32)
    high = jnp.zeros((1, 128), jnp.float32)
    top = jnp.zeros((1, 128), jnp.float32)
    tile = index_ref[0:1, :]
    here = jnp.zeros((1, 128), jnp.int32)
    for place, read in sources:
        ranges = read(80, 8)
        low = jnp.where(lane >> 4 == place, ranges[0:1], low)
        high = jnp.where(lane >> 4 == place, ranges[1:2], high)
        top = jnp.maximum(top, ranges[2:3])
        here = jnp.where(tile >> 4 == place, 1, here)
    used = (lane >> 4 > 0) & (lane >> 4 < index_ref[1:2, :]) & (here > 0)

    def picked(row):
        wide = jnp.take_along_axis(
            jnp.broadcast_to(row, (8, 128)),
            jnp.broadcast_to(tile, (8, 128)),
            axis=1,
            mode="promise_in_bounds",
        )
        return wide[0:1]

    gap = jnp.maximum(picked(low) - own_ref[81:82, :], own_ref[80:81, :] - picked(high))
    kind = jnp.where(used, jnp.where(gap >= FAR_GAP, 1 << 17, 1 << 16), 0)
    within = jnp.where(top - 0.99 >= least, 1, 0)
    row = rows_of((8, 128))
    plan = jnp.broadcast_to(tile * 32 + (lane & 15) + kind, (8, 128))
    plan_ref[...] = jnp.where(row == 0, plan, jnp.broadcast_to(within, (8, 128)))


def near_term(soft, scaled, offset, inside):
    inverse = lax.rsqrt(soft)
    distance = soft * inverse
    upper = distance + scaled
    gap = distance - scaled
    lower = jnp.minimum(jnp.maximum(offset, jnp.abs(gap)), upper)
    ratio = 1.0 / (lower * upper)
    difference = (upper - lower) * ratio
    total = (upper + lower) * ratio
    weight = gap * upper * inverse
    logs = jnp.log(lower * lower * ratio)
    term = difference * (2.0 - 0.5 * (weight * total)) + inverse * logs
    if inside:
        term += jnp.where(offset < -gap, 8.0 * (1.0 / offset - 1.0 / lower), 0.0)
    return term


def split_lists(steps_ref, near_ref, far_ref):
    near = jnp.int32(0)
    far = jnp.int32(0)
    for g in range(TILES):
        for k in range(1, 8):
            entry = steps_ref[0, TILES * k + g]
            near_ref[near] = entry
            far_ref[far] = entry
            near = near + ((entry >> 16) & 1)
            far = far + (entry >> 17)
    pad_list(near_ref, near)
    pad_list(far_ref, far)
    return near, far


def sum_pairs(left_ref, right_ref, blocks_ref, offsets_ref, acc_ref, buffers, lists, counts, within, own):
    def produce(w, g):
        return squares(left_ref, right_ref, g, w, 64)

    def consume_near(inside, diagonal):
        def consume(w, slot, buffer):
            scaled = blocks_ref[w, 3:4, :]
            for v in range(8):
                rows = slice(16 * v, 16 * v + 16)
                c = jnp.broadcast_to(scaled, (16, 128))
                if diagonal:
                    same = rows_of((16, 128)) + 16 * v == rows_of((16, 128), 1)
                    c = jnp.where(same, 0.0, c)
                term = near_term(buffer[rows, :], c, offsets_ref[slot, rows, :], inside)
                if diagonal:
                    acc_ref[slot, rows, :] = term
                else:
                    acc_ref[slot, rows, :] += term

        return consume

    def consume_far(w, slot, buffer):
        scaled = blocks_ref[w, 3:4, :]
        for v in range(8):
            rows = slice(16 * v, 16 * v + 16)
            soft = buffer[rows, :]
            inverse = lax.rsqrt(soft)
            gap = soft * inverse - scaled
            ratio = 1.0 / (soft - scaled * scaled)
            logs = jnp.log(gap * gap * ratio)
            acc_ref[slot, rows, :] += (2.0 * scaled) * ratio + inverse * logs

    def near_lists(inside):
        if own:
            run_list(TILES, own_entry, buffers, produce, consume_near(inside, True))
        run_list(counts[0], entry_in(lists[0]), buffers[:4], produce, consume_near(inside, False))

    pl.when(within == 0)(lambda: near_lists(False))
    pl.when(within != 0)(lambda: near_lists(True))
    run_list(counts[1], entry_in(lists[1]), buffers, produce, consume_far)


def least_of(offset):
    return jnp.min(jnp.min(offset, axis=0, keepdims=True), axis=1, keepdims=True)


def born_own_kernel(
    slab_ref, index_ref, own_ref, other_ref, radii_ref,
    blocks_ref, left_ref, right_ref, offsets_ref, acc_ref, plan_ref,
    near_ref, far_ref, steps_ref, sem, *buffers,
):
    offset = radii_ref[...] - OFFSET
    sources = ((2, rows_in(own_ref)), (inner_slot(slab_ref[0]), rows_in(other_ref)))
    plan_of(index_ref, least_of(offset), sources, own_ref, plan_ref)
    copy = pltpu.make_async_copy(plan_ref, steps_ref, sem)
    copy.start()
    centre = (8 * slab_ref[0] + 4).astype(jnp.float32)
    for place, read in sources:
        fill_blocks(blocks_ref, read, place * TILES, centre)
        fill_right(right_ref, blocks_ref, place * TILES)
    copy.wait()
    counts = split_lists(steps_ref, near_ref, far_ref)
    fill_left(left_ref, blocks_ref)
    for g in range(TILES):
        offsets_ref[g] = column_of(offset[g : g + 1])
    offsets_ref[TILES] = offsets_ref[0]
    sum_pairs(
        left_ref, right_ref, blocks_ref, offsets_ref, acc_ref, buffers,
        (near_ref, far_ref), counts, steps_ref[1, 0], True,
    )


def born_rest_kernel(
    slab_ref, fill_ref, index_ref, own_ref, even_ref, odd_ref, radii_ref,
    left_ref, offsets_ref, blocks_in, right_in, acc_in,
    plan_ref, born_ref, send_ref, blocks_ref, right_ref, acc_ref,
    near_ref, far_ref, steps_ref, sem, sums_ref, *buffers,
):
    slab = slab_ref[0]
    sources = outer_slabs(slab, even_ref, odd_ref, ROWS)
    offset = radii_ref[...] - OFFSET
    plan_of(index_ref, least_of(offset), sources, own_ref, plan_ref)
    copy = pltpu.make_async_copy(plan_ref, steps_ref, sem)
    copy.start()
    centre = (8 * slab + 4).astype(jnp.float32)
    for i, (place, read) in enumerate(sources):
        if i == 1:
            copy.wait()
            counts = split_lists(steps_ref, near_ref, far_ref)
        fill_blocks(blocks_ref, read, place * TILES, centre)
        fill_right(right_ref, blocks_ref, place * TILES)
    sum_pairs(
        left_ref, right_ref, blocks_ref, offsets_ref, acc_ref, buffers,
        (near_ref, far_ref), counts, steps_ref[1, 0], False,
    )
    for g in range(TILES):
        sums_ref[g : g + 1, :] = jnp.sum(acc_ref[g].T, axis=0, keepdims=True)
    slot = rows_of((TILES, 128)) * 128 + rows_of((TILES, 128), 1)
    live = slot < fill_ref[0]
    radius = jnp.where(live, radii_ref[...], 1.5)
    inner = radius - OFFSET
    psi = 0.25 * sums_ref[...] * inner
    bending = jnp.tanh(psi - 0.8 * psi * psi + 4.85 * psi * psi * psi)
    born = 1.0 / (1.0 / inner - bending / radius)
    born_ref[...] = jnp.where(live, born, 0.0)
    send_ref[...] = jnp.where(live, born, 1.0)


def energy_list(steps_ref, list_ref):
    count = jnp.int32(0)
    for g in range(TILES):
        for k in range(1, 8):
            entry = steps_ref[0, TILES * k + g]
            list_ref[count] = entry
            count = count + jnp.minimum(entry >> 16, 1)
    pad_list(list_ref, count)
    return count


def sum_energy(left_ref, right_ref, blocks_ref, born_ref, column_ref, inverse_ref, acc_ref, buffers, entries, count, first):
    def produce(w, g):
        return squares(left_ref, right_ref, g, w, 48)

    def consume(w, slot, buffer):
        charge = blocks_ref[w, 4:5, :]
        partner = born_ref[pl.ds(w, 1), :]
        backward = 1.0 / partner
        for v in range(8):
            rows = slice(16 * v, 16 * v + 16)
            squared = buffer[rows, :]
            product = column_ref[slot, rows, :] * partner
            decay = jnp.exp2(squared * (inverse_ref[slot, rows, :] * backward))
            term = charge * lax.rsqrt(squared + product * decay)
            if first:
                acc_ref[slot, rows, :] = term
            else:
                acc_ref[slot, rows, :] += term

    run_list(count, entries, buffers, produce, consume)


def energy_own_kernel(
    slab_ref, plan_ref, blocks_ref, left_ref, right_ref, own_ref, other_ref, radii_ref,
    column_ref, inverse_ref, acc_ref, result_ref,
    list_ref, steps_ref, born_ref, sem, result_sem, *buffers,
):
    result = pltpu.make_async_copy(radii_ref, result_ref, result_sem)
    result.start()
    copy = pltpu.make_async_copy(plan_ref, steps_ref, sem)
    copy.start()
    born_ref[2 * TILES : 3 * TILES, :] = own_ref[...]
    born_ref[pl.ds(inner_slot(slab_ref[0]) * TILES, TILES), :] = other_ref[...]
    for g in range(TILES):
        if g == 6:
            copy.wait()
            count = energy_list(steps_ref, list_ref)
        column = column_of(own_ref[g : g + 1, :])
        column_ref[g] = column
        inverse_ref[g] = (-0.25 * LOG2E) / column
    column_ref[TILES] = column_ref[0]
    inverse_ref[TILES] = inverse_ref[0]
    shared = (left_ref, right_ref, blocks_ref, born_ref, column_ref, inverse_ref, acc_ref)
    sum_energy(*shared, buffers, own_entry, TILES, True)
    sum_energy(*shared, buffers, entry_in(list_ref), count, False)
    result.wait()


def energy_rest_kernel(
    slab_ref, plan_ref, blocks_ref, left_ref, right_ref, even_ref, odd_ref,
    column_ref, inverse_ref, acc_in,
    energy_ref, share_ref, acc_ref,
    list_ref, steps_ref, born_ref, sem, charge_ref, *buffers,
):
    copy = pltpu.make_async_copy(plan_ref, steps_ref, sem)
    copy.start()
    for place, read in outer_slabs(slab_ref[0], even_ref, odd_ref, TILES):
        born_ref[pl.ds(place * TILES, TILES), :] = read(0, TILES)
    born_ref[2 * TILES : 3 * TILES, :] = jnp.ones((TILES, 128), jnp.float32)
    for g in range(TILES):
        charge_ref[g : g + 1, :] = blocks_ref[2 * TILES + g, 4:5, :]
    copy.wait()
    count = energy_list(steps_ref, list_ref)
    sum_energy(
        left_ref, right_ref, blocks_ref, born_ref, column_ref, inverse_ref, acc_ref, buffers,
        entry_in(list_ref), count, False,
    )
    for g in range(TILES):
        energy_ref[g : g + 1, :] = jnp.sum(acc_ref[g].T, axis=0, keepdims=True)
    energy = -0.5 * charge_ref[...] * energy_ref[...]
    energy_ref[...] = energy
    share = jnp.sum(jnp.sum(energy, axis=0, keepdims=True), axis=1, keepdims=True)
    share_ref[...] = jnp.broadcast_to(share[None], share_ref.shape)


def total_kernel(shares_ref, energy_ref, total_ref, result_ref, sem):
    result = pltpu.make_async_copy(energy_ref, result_ref, sem)
    result.start()
    total = shares_ref[0]
    for i in range(1, shares_ref.shape[0]):
        total = total + shares_ref[i]
    total_ref[0] = total[0, 0]
    result.wait()


def shards(coords, charges, radii, screens, tile_lists, tile_counts, slab_fill):
    f32 = jnp.float32
    count = lax.axis_size(SLAB)
    smem = pl.BlockSpec(memory_space=pltpu.SMEM)
    vmem = pl.BlockSpec(memory_space=pltpu.VMEM)

    def near(*values):
        return tuple(pltpu.with_memory_space_constraint(value, pltpu.VMEM) for value in values)

    def call(kernel, name, outs, scalars, arrays, scratch, aliases=None, out_specs=None, flops=0):
        return pl.pallas_call(
            kernel,
            out_shape=outs,
            in_specs=[smem] * len(scalars) + [vmem] * len(arrays),
            out_specs=out_specs or (vmem,) * len(outs),
            scratch_shapes=scratch,
            input_output_aliases=aliases or {},
            cost_estimate=pl.CostEstimate(flops=flops, transcendentals=0, bytes_accessed=0),
            compiler_params=pltpu.CompilerParams(vmem_limit_bytes=20 << 20),
            name=name,
        )(*scalars, *arrays)

    stack = pltpu.VMEM((TILES + 1, 128, 128), f32)
    blocks_type = pltpu.VMEM((5 * TILES, 8, 128), f32)
    right_type = pltpu.VMEM((5 * TILES, 64, 128), jnp.bfloat16)
    left_type = pltpu.VMEM((TILES, 128, 64), jnp.bfloat16)
    plan_type = pltpu.VMEM((8, 128), jnp.int32)
    slab_type = pltpu.VMEM((TILES, 128), f32)
    result_type = pltpu.HBM((TILES, 128), f32)
    hbm = pl.BlockSpec(memory_space=pltpu.HBM)
    entries = pltpu.SMEM((144,), jnp.int32)
    steps = pltpu.SMEM((8, 128), jnp.int32)
    squares = [pltpu.VMEM((128, 128), f32)] * 8
    sem = pltpu.SemaphoreType.DMA

    slab = lax.axis_index(SLAB).astype(jnp.int32)[None]
    charges, radii, screens = (v.reshape(TILES, 128) for v in (charges, radii, screens))
    lists, counts = tile_lists.T, tile_counts.reshape(1, TILES)
    coords, charges, radii, screens, lists, counts = (
        pltpu.with_memory_space_constraint(value, pltpu.HBM)
        for value in (coords, charges, radii, screens, lists, counts)
    )
    packed, index, kept = call(
        prep_kernel, "prep", (pltpu.VMEM((ROWS, 128), f32), plan_type, slab_type),
        (slab, slab_fill), (coords, charges, radii, screens, lists, counts), [],
    )
    other, even, odd = neighbours(packed)
    packed, other, even, odd, index, kept = near(packed, other, even, odd, index, kept)
    blocks, left, right, offsets, acc, own_plan = call(
        born_own_kernel, "born_own",
        (blocks_type, left_type, right_type, stack, stack, plan_type),
        (slab,), (index, packed, other, kept),
        [entries, entries, steps, sem] + squares, flops=1 << 27,
    )
    plan, born, send, blocks, right, acc = call(
        born_rest_kernel, "born_rest",
        (plan_type, slab_type, slab_type, blocks_type, right_type, stack),
        (slab, slab_fill),
        (index, packed, even, odd, kept, *near(left, offsets, blocks, right, acc)),
        [entries, entries, steps, sem, slab_type] + squares,
        aliases={9: 3, 10: 4, 11: 5},
    )
    born_other, born_even, born_odd = neighbours(send)
    column, inverse, acc, born = call(
        energy_own_kernel, "energy_own", (stack, stack, stack, result_type),
        (slab,), near(own_plan, blocks, left, right, send, born_other, born),
        [entries, steps, pltpu.VMEM((5 * TILES, 128), f32), sem, sem] + squares,
        out_specs=(vmem, vmem, vmem, hbm), flops=1 << 27,
    )
    energy, share, acc = call(
        energy_rest_kernel, "energy_rest",
        (slab_type, pltpu.VMEM((count, 1, 128), f32), stack),
        (slab,), near(plan, blocks, left, right, born_even, born_odd, column, inverse, acc),
        [entries, steps, pltpu.VMEM((5 * TILES, 128), f32), sem, slab_type] + squares,
        aliases={9: 2},
    )
    shares = lax.all_to_all(share, SLAB, 0, 0, tiled=True)
    total, energy = call(
        total_kernel, "total", (jax.ShapeDtypeStruct((1,), f32), result_type), (),
        near(shares, energy), [sem], out_specs=(smem, hbm),
    )
    return (born.reshape(-1), energy.reshape(-1), total[0])


def solution(mesh):
    torus = Mesh(mesh.devices.reshape(4, 8, 4, 2), SLAB)
    placed = (P(None, SLAB), P(SLAB), P(SLAB), P(SLAB), P(SLAB, None), P(SLAB), P(SLAB))
    return jax.shard_map(
        shards, mesh=torus, in_specs=placed, out_specs=(P(SLAB), P(SLAB), P()), check_vma=False
    )
```

```python
import jax
import jax.numpy as jnp
from jax import lax
from jax.experimental import pallas as pl
from jax.experimental.pallas import tpu as pltpu
from jax.sharding import Mesh
from jax.sharding import PartitionSpec as P

SLAB = ("slab_0", "slab_1", "slab_2", "slab_3")
OFFSET = 0.09
LOG2E = 1.4426950408889634
TILES = 16
UNROLL = 8
FAR_GAP = 3.5
ROWS = 88


def chip_swap(count, odd):
    pairs = []
    for chip in range(count // 2):
        other = ((chip + odd) ^ 1) - odd
        for core in (0, 1):
            if 0 <= other < count // 2:
                pairs.append((2 * chip + core, 2 * other + core))
            else:
                pairs.append((2 * chip + core, 2 * chip + 1 - core))
    return pairs


def neighbours(value):
    count = lax.axis_size(SLAB)
    other = lax.ppermute(value, SLAB, [(i, i ^ 1) for i in range(count)])
    both = jnp.concatenate([value, other], axis=0)
    return [other] + [lax.ppermute(both, SLAB, chip_swap(count, odd)) for odd in (0, 1)]


def rows_in(ref):
    return lambda start, size: ref[pl.ds(start, size), :]


def inner_slot(slab):
    return jnp.where(slab % 2 == 0, 3, 1)


def outer_slabs(slab, even, odd, height):
    ahead = (slab // 2) % 2 == 0
    far = jnp.where(ahead, 4, 0)
    from_even = ahead == (slab % 2 == 1)

    def crossed(start, size):
        rows = pl.ds(height + start, size)
        return jnp.where(from_even, even[rows, :], odd[rows, :])

    return ((4 - inner_slot(slab), crossed), (far, rows_in(even)), (4 - far, rows_in(odd)))


def rows_of(shape, axis=0):
    return lax.broadcasted_iota(jnp.int32, shape, axis)


def prep_kernel(
    slab_ref, fill_ref, coords_ref, charges_ref, radii_ref, screens_ref, lists_ref, counts_ref,
    out_ref, index_ref, kept_ref,
):
    index_ref[...] = jnp.zeros((8, 128), jnp.int32)
    for k in range(8):
        lanes = slice(TILES * k, TILES * k + TILES)
        index_ref[0:1, lanes] = lists_ref[k : k + 1, :]
        index_ref[1:2, lanes] = counts_ref[...]
    kept_ref[...] = radii_ref[...]
    fill = fill_ref[0]
    middle = (8 * slab_ref[0] + 4).astype(jnp.float32)
    slot = rows_of((TILES, 128)) * 128 + rows_of((TILES, 128), 1)
    live = slot < fill
    scaled = jnp.where(live, screens_ref[...] * (radii_ref[...] - OFFSET), 0.0)
    charge = jnp.where(live, charges_ref[...], 0.0)
    home = jnp.where(rows_of((3, 128)) == 2, middle, 0.0)
    lane = rows_of((3, 128), 1)
    column = rows_of((1, 128), 1) % TILES
    low = jnp.zeros((1, 128), jnp.float32)
    high = jnp.zeros((1, 128), jnp.float32)
    for t in range(TILES):
        xyz = jnp.where(lane + t * 128 < fill, coords_ref[:, t * 128 : (t + 1) * 128], home)
        out_ref[5 * t : 5 * t + 3, :] = xyz
        out_ref[5 * t + 3 : 5 * t + 4, :] = scaled[t : t + 1]
        out_ref[5 * t + 4 : 5 * t + 5, :] = charge[t : t + 1]
        low = jnp.where(column == t, jnp.min(xyz[2:3], axis=1, keepdims=True), low)
        high = jnp.where(column == t, jnp.max(xyz[2:3], axis=1, keepdims=True), high)
    top = jnp.max(jnp.max(scaled, axis=0, keepdims=True), axis=1, keepdims=True)
    out_ref[80:81, :] = low
    out_ref[81:82, :] = high
    out_ref[82:83, :] = jnp.broadcast_to(top, (1, 128))
    out_ref[83:88, :] = jnp.zeros((5, 128), jnp.float32)


def parts_of(rows):
    first = rows.astype(jnp.bfloat16).astype(jnp.float32)
    rest = rows - first
    second = rest.astype(jnp.bfloat16).astype(jnp.float32)
    third = (rest - second).astype(jnp.bfloat16).astype(jnp.float32)
    return first, second, third


def fill_blocks(blocks_ref, read, base, centre):
    row = rows_of((8, 128))
    shift = jnp.where(row == 2, centre, 0.0)
    tail = jnp.where(row == 6, 1.0, 0.0)
    for t in range(TILES):
        block = read(5 * t, 8) - shift
        square = block * block
        norm = square[0:1] + square[1:2] + square[2:3]
        blocks_ref[base + t] = jnp.where(row < 5, block, jnp.where(row == 5, norm, tail))


def fill_right(right_ref, blocks_ref, base):
    last = jnp.where(rows_of((16, 128)) == 0, 1.0, 0.0)
    for t in range(TILES):
        b1, b2, b3 = parts_of(blocks_ref[base + t])
        stack = jnp.concatenate([b1, b2, b3, b1, b2, b1, last], axis=0)
        right_ref[base + t] = stack.astype(jnp.bfloat16)


def fill_left(left_ref, blocks_ref):
    row = rows_of((8, 128))
    last = jnp.where(rows_of((16, 128)) == 0, 1.0, 0.0)
    for g in range(TILES):
        block = blocks_ref[2 * TILES + g]
        norm = jnp.broadcast_to(block[5:6], (8, 128))
        left = jnp.where(
            row < 3, -2.0 * block, jnp.where(row == 5, 1.0, jnp.where(row == 6, norm, 0.0))
        )
        a1, a2, a3 = parts_of(left)
        stack = jnp.concatenate([a1, a1, a1, a2, a2, a3, last], axis=0)
        left_ref[g] = stack.T.astype(jnp.bfloat16)


def column_of(row):
    return jnp.broadcast_to(row, (128, 128)).T


def squares(left_ref, right_ref, g, w, depth):
    return jnp.dot(
        left_ref[g, :, :depth], right_ref[w, :depth, :], preferred_element_type=jnp.float32
    )


def run_list(count, entry_of, buffers, produce, consume):
    unroll = len(buffers)

    def fetch(base):
        for u, buffer in enumerate(buffers):
            w, slot = entry_of(base + u)
            buffer[...] = produce(w, jnp.minimum(slot, TILES - 1))

    fetch(0)

    @pl.loop(0, (count + unroll - 1) // unroll)
    def _(step):
        base = step * unroll
        for u, buffer in enumerate(buffers):
            w, slot = entry_of(base + u)
            consume(w, slot, buffer)
        fetch(base + unroll)


def own_entry(index):
    return 2 * TILES + jnp.minimum(index, TILES - 1), index


def pad_list(list_ref, count):
    for u in range(2 * UNROLL):
        list_ref[count + u] = 2 * TILES * 32 + TILES


def entry_in(list_ref):
    def entry_of(index):
        entry = list_ref[index]
        return (entry >> 5) & 127, entry & 31

    return entry_of


def plan_of(index_ref, least, sources, own_ref, plan_ref):
    lane = rows_of((1, 128), 1)
    low = jnp.zeros((1, 128), jnp.float32)
    high = jnp.zeros((1, 128), jnp.float32)
    top = jnp.zeros((1, 128), jnp.float32)
    tile = index_ref[0:1, :]
    here = jnp.zeros((1, 128), jnp.int32)
    for place, read in sources:
        ranges = read(80, 8)
        low = jnp.where(lane >> 4 == place, ranges[0:1], low)
        high = jnp.where(lane >> 4 == place, ranges[1:2], high)
        top = jnp.maximum(top, ranges[2:3])
        here = jnp.where(tile >> 4 == place, 1, here)
    used = (lane >> 4 > 0) & (lane >> 4 < index_ref[1:2, :]) & (here > 0)

    def picked(row):
        wide = jnp.take_along_axis(
            jnp.broadcast_to(row, (8, 128)),
            jnp.broadcast_to(tile, (8, 128)),
            axis=1,
            mode="promise_in_bounds",
        )
        return wide[0:1]

    gap = jnp.maximum(picked(low) - own_ref[81:82, :], own_ref[80:81, :] - picked(high))
    kind = jnp.where(used, jnp.where(gap >= FAR_GAP, 1 << 17, 1 << 16), 0)
    within = jnp.where(top - 0.99 >= least, 1, 0)
    row = rows_of((8, 128))
    plan = jnp.broadcast_to(tile * 32 + (lane & 15) + kind, (8, 128))
    plan_ref[...] = jnp.where(row == 0, plan, jnp.broadcast_to(within, (8, 128)))


def near_term(soft, scaled, offset, inside):
    inverse = lax.rsqrt(soft)
    distance = soft * inverse
    upper = distance + scaled
    gap = distance - scaled
    lower = jnp.minimum(jnp.maximum(offset, jnp.abs(gap)), upper)
    ratio = 1.0 / (lower * upper)
    difference = (upper - lower) * ratio
    total = (upper + lower) * ratio
    weight = gap * upper * inverse
    logs = jnp.log(lower * lower * ratio)
    term = difference * (2.0 - 0.5 * (weight * total)) + inverse * logs
    if inside:
        term += jnp.where(offset < -gap, 8.0 * (1.0 / offset - 1.0 / lower), 0.0)
    return term


def split_lists(steps_ref, near_ref, far_ref):
    near = jnp.int32(0)
    far = jnp.int32(0)
    for g in range(TILES):
        for k in range(1, 8):
            entry = steps_ref[0, TILES * k + g]
            near_ref[near] = entry
            far_ref[far] = entry
            near = near + ((entry >> 16) & 1)
            far = far + (entry >> 17)
    pad_list(near_ref, near)
    pad_list(far_ref, far)
    return near, far


def sum_pairs(left_ref, right_ref, blocks_ref, offsets_ref, acc_ref, buffers, lists, counts, within, own):
    def produce(w, g):
        return squares(left_ref, right_ref, g, w, 64)

    def consume_near(inside, diagonal):
        def consume(w, slot, buffer):
            scaled = blocks_ref[w, 3:4, :]
            for v in range(8):
                rows = slice(16 * v, 16 * v + 16)
                c = jnp.broadcast_to(scaled, (16, 128))
                if diagonal:
                    same = rows_of((16, 128)) + 16 * v == rows_of((16, 128), 1)
                    c = jnp.where(same, 0.0, c)
                term = near_term(buffer[rows, :], c, offsets_ref[slot, rows, :], inside)
                if diagonal:
                    acc_ref[slot, rows, :] = term
                else:
                    acc_ref[slot, rows, :] += term

        return consume

    def consume_far(w, slot, buffer):
        scaled = blocks_ref[w, 3:4, :]
        for v in range(8):
            rows = slice(16 * v, 16 * v + 16)
            soft = buffer[rows, :]
            inverse = lax.rsqrt(soft)
            gap = soft * inverse - scaled
            ratio = 1.0 / (soft - scaled * scaled)
            logs = jnp.log(gap * gap * ratio)
            acc_ref[slot, rows, :] += (2.0 * scaled) * ratio + inverse * logs

    def near_lists(inside):
        if own:
            run_list(TILES, own_entry, buffers[:4], produce, consume_near(inside, True))
        run_list(counts[0], entry_in(lists[0]), buffers[:4], produce, consume_near(inside, False))

    pl.when(within == 0)(lambda: near_lists(False))
    pl.when(within != 0)(lambda: near_lists(True))
    run_list(counts[1], entry_in(lists[1]), buffers, produce, consume_far)


def least_of(offset):
    return jnp.min(jnp.min(offset, axis=0, keepdims=True), axis=1, keepdims=True)


def born_own_kernel(
    slab_ref, index_ref, own_ref, other_ref, radii_ref,
    blocks_ref, left_ref, right_ref, offsets_ref, acc_ref, plan_ref,
    near_ref, far_ref, steps_ref, sem, *buffers,
):
    offset = radii_ref[...] - OFFSET
    sources = ((2, rows_in(own_ref)), (inner_slot(slab_ref[0]), rows_in(other_ref)))
    plan_of(index_ref, least_of(offset), sources, own_ref, plan_ref)
    copy = pltpu.make_async_copy(plan_ref, steps_ref, sem)
    copy.start()
    centre = (8 * slab_ref[0] + 4).astype(jnp.float32)
    for place, read in sources:
        fill_blocks(blocks_ref, read, place * TILES, centre)
        fill_right(right_ref, blocks_ref, place * TILES)
    copy.wait()
    counts = split_lists(steps_ref, near_ref, far_ref)
    fill_left(left_ref, blocks_ref)
    for g in range(TILES):
        offsets_ref[g] = column_of(offset[g : g + 1])
    offsets_ref[TILES] = offsets_ref[0]
    sum_pairs(
        left_ref, right_ref, blocks_ref, offsets_ref, acc_ref, buffers,
        (near_ref, far_ref), counts, steps_ref[1, 0], True,
    )


def born_rest_kernel(
    slab_ref, fill_ref, index_ref, own_ref, even_ref, odd_ref, radii_ref,
    left_ref, offsets_ref, blocks_in, right_in, acc_in,
    plan_ref, born_ref, send_ref, blocks_ref, right_ref, acc_ref,
    near_ref, far_ref, steps_ref, sem, sums_ref, *buffers,
):
    slab = slab_ref[0]
    sources = outer_slabs(slab, even_ref, odd_ref, ROWS)
    offset = radii_ref[...] - OFFSET
    plan_of(index_ref, least_of(offset), sources, own_ref, plan_ref)
    copy = pltpu.make_async_copy(plan_ref, steps_ref, sem)
    copy.start()
    centre = (8 * slab + 4).astype(jnp.float32)
    for i, (place, read) in enumerate(sources):
        if i == 1:
            copy.wait()
            counts = split_lists(steps_ref, near_ref, far_ref)
        fill_blocks(blocks_ref, read, place * TILES, centre)
        fill_right(right_ref, blocks_ref, place * TILES)
    sum_pairs(
        left_ref, right_ref, blocks_ref, offsets_ref, acc_ref, buffers,
        (near_ref, far_ref), counts, steps_ref[1, 0], False,
    )
    for g in range(TILES):
        sums_ref[g : g + 1, :] = jnp.sum(acc_ref[g].T, axis=0, keepdims=True)
    slot = rows_of((TILES, 128)) * 128 + rows_of((TILES, 128), 1)
    live = slot < fill_ref[0]
    radius = jnp.where(live, radii_ref[...], 1.5)
    inner = radius - OFFSET
    psi = 0.25 * sums_ref[...] * inner
    bending = jnp.tanh(psi - 0.8 * psi * psi + 4.85 * psi * psi * psi)
    born = 1.0 / (1.0 / inner - bending / radius)
    born_ref[...] = jnp.where(live, born, 0.0)
    send_ref[...] = jnp.where(live, born, 1.0)


def energy_list(steps_ref, list_ref):
    count = jnp.int32(0)
    for g in range(TILES):
        for k in range(1, 8):
            entry = steps_ref[0, TILES * k + g]
            list_ref[count] = entry
            count = count + jnp.minimum(entry >> 16, 1)
    pad_list(list_ref, count)
    return count


def sum_energy(left_ref, right_ref, blocks_ref, born_ref, column_ref, inverse_ref, acc_ref, buffers, entries, count, first):
    def produce(w, g):
        return squares(left_ref, right_ref, g, w, 48)

    def consume(w, slot, buffer):
        charge = blocks_ref[w, 4:5, :]
        partner = born_ref[pl.ds(w, 1), :]
        backward = 1.0 / partner
        for v in range(8):
            rows = slice(16 * v, 16 * v + 16)
            squared = buffer[rows, :]
            product = column_ref[slot, rows, :] * partner
            decay = jnp.exp2(squared * (inverse_ref[slot, rows, :] * backward))
            term = charge * lax.rsqrt(squared + product * decay)
            if first:
                acc_ref[slot, rows, :] = term
            else:
                acc_ref[slot, rows, :] += term

    run_list(count, entries, buffers, produce, consume)


def energy_own_kernel(
    slab_ref, plan_ref, blocks_ref, left_ref, right_ref, own_ref, other_ref, radii_ref,
    column_ref, inverse_ref, acc_ref, result_ref,
    list_ref, steps_ref, born_ref, sem, result_sem, *buffers,
):
    result = pltpu.make_async_copy(radii_ref, result_ref, result_sem)
    result.start()
    copy = pltpu.make_async_copy(plan_ref, steps_ref, sem)
    copy.start()
    born_ref[2 * TILES : 3 * TILES, :] = own_ref[...]
    born_ref[pl.ds(inner_slot(slab_ref[0]) * TILES, TILES), :] = other_ref[...]
    for g in range(TILES):
        if g == 6:
            copy.wait()
            count = energy_list(steps_ref, list_ref)
        column = column_of(own_ref[g : g + 1, :])
        column_ref[g] = column
        inverse_ref[g] = (-0.25 * LOG2E) / column
    column_ref[TILES] = column_ref[0]
    inverse_ref[TILES] = inverse_ref[0]
    shared = (left_ref, right_ref, blocks_ref, born_ref, column_ref, inverse_ref, acc_ref)
    sum_energy(*shared, buffers, own_entry, TILES, True)
    sum_energy(*shared, buffers, entry_in(list_ref), count, False)
    result.wait()


def energy_rest_kernel(
    slab_ref, plan_ref, blocks_ref, left_ref, right_ref, even_ref, odd_ref,
    column_ref, inverse_ref, acc_in,
    energy_ref, share_ref, acc_ref,
    list_ref, steps_ref, born_ref, sem, charge_ref, *buffers,
):
    copy = pltpu.make_async_copy(plan_ref, steps_ref, sem)
    copy.start()
    for place, read in outer_slabs(slab_ref[0], even_ref, odd_ref, TILES):
        born_ref[pl.ds(place * TILES, TILES), :] = read(0, TILES)
    born_ref[2 * TILES : 3 * TILES, :] = jnp.ones((TILES, 128), jnp.float32)
    for g in range(TILES):
        charge_ref[g : g + 1, :] = blocks_ref[2 * TILES + g, 4:5, :]
    copy.wait()
    count = energy_list(steps_ref, list_ref)
    sum_energy(
        left_ref, right_ref, blocks_ref, born_ref, column_ref, inverse_ref, acc_ref, buffers,
        entry_in(list_ref), count, False,
    )
    for g in range(TILES):
        energy_ref[g : g + 1, :] = jnp.sum(acc_ref[g].T, axis=0, keepdims=True)
    energy = -0.5 * charge_ref[...] * energy_ref[...]
    energy_ref[...] = energy
    share = jnp.sum(jnp.sum(energy, axis=0, keepdims=True), axis=1, keepdims=True)
    share_ref[...] = jnp.broadcast_to(share[None], share_ref.shape)


def total_kernel(shares_ref, energy_ref, total_ref, result_ref, sem):
    result = pltpu.make_async_copy(energy_ref, result_ref, sem)
    result.start()
    total = shares_ref[0]
    for i in range(1, shares_ref.shape[0]):
        total = total + shares_ref[i]
    total_ref[0] = total[0, 0]
    result.wait()


def shards(coords, charges, radii, screens, tile_lists, tile_counts, slab_fill):
    f32 = jnp.float32
    count = lax.axis_size(SLAB)
    smem = pl.BlockSpec(memory_space=pltpu.SMEM)
    vmem = pl.BlockSpec(memory_space=pltpu.VMEM)

    def near(*values):
        return tuple(pltpu.with_memory_space_constraint(value, pltpu.VMEM) for value in values)

    def call(kernel, name, outs, scalars, arrays, scratch, aliases=None, out_specs=None, flops=0):
        return pl.pallas_call(
            kernel,
            out_shape=outs,
            in_specs=[smem] * len(scalars) + [vmem] * len(arrays),
            out_specs=out_specs or (vmem,) * len(outs),
            scratch_shapes=scratch,
            input_output_aliases=aliases or {},
            cost_estimate=pl.CostEstimate(flops=flops, transcendentals=0, bytes_accessed=0),
            compiler_params=pltpu.CompilerParams(vmem_limit_bytes=20 << 20),
            name=name,
        )(*scalars, *arrays)

    stack = pltpu.VMEM((TILES + 1, 128, 128), f32)
    blocks_type = pltpu.VMEM((5 * TILES, 8, 128), f32)
    right_type = pltpu.VMEM((5 * TILES, 64, 128), jnp.bfloat16)
    left_type = pltpu.VMEM((TILES, 128, 64), jnp.bfloat16)
    plan_type = pltpu.VMEM((8, 128), jnp.int32)
    slab_type = pltpu.VMEM((TILES, 128), f32)
    result_type = pltpu.HBM((TILES, 128), f32)
    hbm = pl.BlockSpec(memory_space=pltpu.HBM)
    entries = pltpu.SMEM((144,), jnp.int32)
    steps = pltpu.SMEM((8, 128), jnp.int32)
    squares = [pltpu.VMEM((128, 128), f32)] * 8
    sem = pltpu.SemaphoreType.DMA

    slab = lax.axis_index(SLAB).astype(jnp.int32)[None]
    charges, radii, screens = (v.reshape(TILES, 128) for v in (charges, radii, screens))
    lists, counts = tile_lists.T, tile_counts.reshape(1, TILES)
    coords, charges, radii, screens, lists, counts = (
        pltpu.with_memory_space_constraint(value, pltpu.HBM)
        for value in (coords, charges, radii, screens, lists, counts)
    )
    packed, index, kept = call(
        prep_kernel, "prep", (pltpu.VMEM((ROWS, 128), f32), plan_type, slab_type),
        (slab, slab_fill), (coords, charges, radii, screens, lists, counts), [],
    )
    other, even, odd = neighbours(packed)
    packed, other, even, odd, index, kept = near(packed, other, even, odd, index, kept)
    blocks, left, right, offsets, acc, own_plan = call(
        born_own_kernel, "born_own",
        (blocks_type, left_type, right_type, stack, stack, plan_type),
        (slab,), (index, packed, other, kept),
        [entries, entries, steps, sem] + squares, flops=1 << 27,
    )
    plan, born, send, blocks, right, acc = call(
        born_rest_kernel, "born_rest",
        (plan_type, slab_type, slab_type, blocks_type, right_type, stack),
        (slab, slab_fill),
        (index, packed, even, odd, kept, *near(left, offsets, blocks, right, acc)),
        [entries, entries, steps, sem, slab_type] + squares,
        aliases={9: 3, 10: 4, 11: 5},
    )
    born_other, born_even, born_odd = neighbours(send)
    column, inverse, acc, born = call(
        energy_own_kernel, "energy_own", (stack, stack, stack, result_type),
        (slab,), near(own_plan, blocks, left, right, send, born_other, born),
        [entries, steps, pltpu.VMEM((5 * TILES, 128), f32), sem, sem] + squares,
        out_specs=(vmem, vmem, vmem, hbm), flops=1 << 27,
    )
    energy, share, acc = call(
        energy_rest_kernel, "energy_rest",
        (slab_type, pltpu.VMEM((count, 1, 128), f32), stack),
        (slab,), near(plan, blocks, left, right, born_even, born_odd, column, inverse, acc),
        [entries, steps, pltpu.VMEM((5 * TILES, 128), f32), sem, slab_type] + squares,
        aliases={9: 2},
    )
    shares = lax.all_to_all(share, SLAB, 0, 0, tiled=True)
    total, energy = call(
        total_kernel, "total", (jax.ShapeDtypeStruct((1,), f32), result_type), (),
        near(shares, energy), [sem], out_specs=(smem, hbm),
    )
    return (born.reshape(-1), energy.reshape(-1), total[0])


def solution(mesh):
    torus = Mesh(mesh.devices.reshape(4, 8, 4, 2), SLAB)
    placed = (P(None, SLAB), P(SLAB), P(SLAB), P(SLAB), P(SLAB, None), P(SLAB), P(SLAB))
    return jax.shard_map(
        shards, mesh=torus, in_specs=placed, out_specs=(P(SLAB), P(SLAB), P()), check_vma=False
    )
```
